32 devices in a mesh: ctx: 4 (over x, core), head: 8 (over z, y).
Axes of the slice: x: 2, y: 2, z: 4, core: 2. Of those that a mesh axis runs over, the one named last changes fastest.
Arguments:
- layer_input: bfloat16 [1024, 8192], P('ctx'), may hold values from -6 to 6
- output_grad: bfloat16 [1024, 8192], P('ctx'), may hold values from -6 to 6
- routes: int32 [1024, 8], P('ctx'), may hold values from 0 to 31, all different within a row; in each aligned block of 256 rows (0 to 255, 256 to 511, ...) at most 128 rows name the same one
- route_gates: float32 [1024, 8], P('ctx'), may hold values from 0.05 to 0.3
- query_weight: bfloat16 [40, 8192, 128], P('head', 'ctx'), may hold values from -0.0625 to 0.0625
- output_weight: bfloat16 [40, 8192, 128], P('head', 'ctx'), may hold values from -0.0625 to 0.0625
- key_values: bfloat16 [8, 1024, 128], P('head', 'ctx'), may hold values from -96 to 96
Outputs:
- input_grad: bfloat16 [1024, 8192], P('ctx', 'head')
- keyvalue_grad: float32 [8, 1024, 128], P('head', 'ctx')
The draws below stay inside these ranges and needn't reach their ends.
Inputs may be any that keep to these rules, and one draw needn't show every extreme that they name: `routes`: each row names 8 different experts; in the 256 rows of one ctx block no expert is named more than 128 times, and some expert reaches 128.
All inputs are finite; a program needn't handle non-finite values.
Results may differ from the reference program's by a relative error of at most 0.015.
The reference program's roundings to bfloat16 on the way count: a program that leaves them out, or rounds other values in their place, can miss the bound.
Values may be sent and summed in bfloat16 or wider, within the bound.
A program may use at most 128 MiB of HBM per device.

```python
import math
import jax
import jax.numpy as jnp
import numpy as np
from jax import lax

D = 8192
HD = 128
TOP = 8
EXP_DEV = 4
TOK_DEV = 256
EXPERTS = 32
HEADS = 40
KVG = 4
CAP = 128
TOKENS = 1024
N_CTX = 4
N_HEAD = 8


def draw_key_values(key, part):
    normal_draw = jax.random.normal(key, (2 * KVG, TOKENS, HD), jnp.float32)
    normal_draw = jnp.clip(normal_draw, -4.0, 4.0)
    return normal_draw.astype(jnp.bfloat16)


def block_scale(own_key, extent, pieces, smallest, top_value):
    gain = 1.0
    for position, parts in pieces:
        draws = jax.random.uniform(jax.random.fold_in(jax.random.fold_in(own_key, 6), position), (parts,), jnp.float32, smallest / len(pieces), top_value / len(pieces))
        gain = gain * jnp.repeat(jnp.exp(draws), extent[position] // parts).reshape((-1,) + (1,) * (len(extent) - 1 - position))
    return gain


def assign_block(stream_key, own, number, rows, number_of, top, bound, skew):
    order = jax.random.permutation(stream_key, number_of)
    crowded, common = portions_of(number_of, rows * top, bound, skew, True), portions_of(number_of, rows * top, bound, skew, False)
    places = jnp.arange(number_of)

    def named(tallies, turn):
        used = int((tallies > 0).sum())
        fixed = max(1, used // 4)
        moved = fixed + (places - fixed + turn * (used - fixed)) % max(1, number_of - fixed)
        return jnp.zeros((number_of,), jnp.int32).at[order[jnp.where(places < fixed, places, moved)]].set(jnp.asarray(tallies, jnp.int32))

    tallies = jnp.where(number % 4 == 0, named(crowded, number // 4), named(common, number - number // 4 - 1))
    mixed = jax.random.permutation(jax.random.fold_in(own, 3), number_of)
    giver, receiver = mixed[0:number_of // 2 * 2:2], mixed[1:number_of // 2 * 2:2]
    margin = jnp.minimum(tallies[giver] - 1, bound - tallies[receiver]) // 2
    margin = jnp.where((giver == order[0]) | (receiver == order[0]) | (tallies[receiver] == 0), 0, jnp.maximum(margin, 0))
    moved = jax.random.randint(jax.random.fold_in(own, 4), (number_of // 2,), 0, 1 << 20) % (margin + 1)
    tallies = tallies.at[giver].add(-moved).at[receiver].add(moved)
    items = jnp.searchsorted(jnp.cumsum(tallies), jnp.arange(rows * top), side="right").astype(jnp.int32)
    listing = items.reshape(top, rows).T
    listing = listing[jax.random.permutation(jax.random.fold_in(own, 1), rows)]
    turn = jax.random.randint(jax.random.fold_in(own, 2), (rows, 1), 0, top)
    return jnp.take_along_axis(listing, (jnp.arange(top)[None, :] + turn) % top, axis=1)


def portions_of(number_of, total, most, lean, full):
    loads = [(1 << 20) // math.isqrt(standing ** lean) + 1 for standing in range(1, number_of + 1)]
    largest = most if full else min(most, max(-(-total // number_of), total * loads[0] // sum(loads)))
    least = 1 if total - largest >= number_of - 1 else 0
    counts, surplus = [largest] + [least] * (number_of - 1), total - largest - least * (number_of - 1)
    while surplus > 0:
        movable = [i for i in range(1, number_of) if counts[i] < largest] or [i for i in range(1, number_of) if counts[i] < most]
        whole, left = sum([loads[i] for i in movable]), surplus
        for i in movable:
            extra = min(most - counts[i], max(1, left * loads[i] // whole), surplus)
            counts[i] = counts[i] + extra
            surplus = surplus - extra
    return np.array(counts)


def scatter_about(rng, dims, deviation, limit, shards=(), kind=jnp.bfloat16):
    entries = deviation * jax.random.normal(rng, dims, jnp.float32)
    if shards:
        entries = entries * block_scale(rng, dims, shards, -0.22, 0.18)
    return jnp.clip(entries, -limit, limit).astype(kind)


def setup_inputs(seed: int = 0) -> dict:
    streams_of = jax.random.split(jax.random.key(seed), 8)
    layer_input = scatter_about(streams_of[0], (TOKENS, D), 1.0, 6.0, ((0, 4),))
    output_grad = scatter_about(streams_of[1], (TOKENS, D), 1.0, 6.0, ((0, 4),))
    routes_keys = jax.random.split(jax.random.fold_in(streams_of[2], 1), TOKENS // TOK_DEV)
    routes_turns = jax.random.permutation(jax.random.fold_in(streams_of[2], 3), TOKENS // TOK_DEV)
    routes = jax.vmap(lambda own, number: assign_block(jax.random.fold_in(streams_of[2], 2), own, number, TOK_DEV, EXPERTS, TOP, CAP, 2))(routes_keys, routes_turns).reshape((TOKENS, TOP))
    route_gates = jnp.clip(0.05 + 0.25 * jax.random.uniform(streams_of[3], (TOKENS, TOP), jnp.float32) ** block_scale(streams_of[3], (TOKENS, TOP), ((0, 4),), -0.2, 0.2), 0.05, 0.3)
    query_weight = scatter_about(streams_of[4], (HEADS, D, HD), D ** -0.5, 0.0625, ((0, 8), (1, 4)))
    output_weight = scatter_about(streams_of[5], (HEADS, D, HD), D ** -0.5, 0.0625, ((0, 8), (1, 4)))
    key_values = draw_key_values(jax.random.fold_in(streams_of[7], 71), 0)
    return dict(layer_input=layer_input, output_grad=output_grad, routes=routes, route_gates=route_gates, query_weight=query_weight, output_weight=output_weight, key_values=key_values)


PRECISE = lax.Precision.HIGHEST


def slot_table(route_rows, first_id, expert_count, slot_count):
    expert_ids = first_id + jnp.arange(expert_count, dtype=jnp.int32)
    matches = route_rows[:, :, None] == expert_ids[None, None, :]
    member = jnp.any(matches, axis=1).astype(jnp.int32)
    placed = jnp.cumsum(member, axis=0) - 1
    slot_map = (placed.T[:, None, :] == jnp.arange(slot_count, dtype=jnp.int32)[None, :, None]) & (member.T[:, None, :] == 1)
    return slot_map.astype(jnp.float32)


def expert_gate(route_rows, gate_rows, first_id, expert_count):
    expert_ids = first_id + jnp.arange(expert_count, dtype=jnp.int32)
    matches = route_rows[:, :, None] == expert_ids[None, None, :]
    return jnp.sum(jnp.where(matches, gate_rows[:, :, None], jnp.zeros_like(gate_rows)[:, :, None]), axis=1)


def attend(queries, query_place, key_rows, value_rows, key_place, head_grads):
    score_scale = queries.shape[1] ** -0.5
    scores = jnp.dot(queries, key_rows.T, preferred_element_type=jnp.float32) * score_scale
    scores = jnp.where(key_place[None, :] <= query_place[:, None], scores, -1e30)
    row_max = jnp.max(scores, axis=1, keepdims=True)
    raised = jnp.exp(scores - row_max)
    shares = raised / jnp.sum(raised, axis=1, keepdims=True)
    shares_low = shares.astype(jnp.bfloat16)
    outputs = jnp.dot(shares_low, value_rows, preferred_element_type=jnp.float32)
    share_grad = jnp.dot(head_grads, value_rows.T, preferred_element_type=jnp.float32)
    row_delta = jnp.sum(head_grads.astype(jnp.float32) * outputs, axis=1, keepdims=True)
    score_grad = (shares * (share_grad - row_delta) * score_scale).astype(jnp.bfloat16)
    query_grad = jnp.dot(score_grad, key_rows, preferred_element_type=jnp.float32).astype(jnp.bfloat16)
    key_grad = jnp.dot(score_grad.T, queries, preferred_element_type=jnp.float32)
    value_grad = jnp.dot(shares_low.T, head_grads, preferred_element_type=jnp.float32)
    return query_grad, key_grad, value_grad


def reference(layer_input, output_grad, routes, route_gates, query_weight, output_weight, key_values):
    per_block = EXP_DEV + 1
    key_place = jnp.arange(TOKENS, dtype=jnp.int32).astype(jnp.float32)
    place_blocks = key_place.reshape(N_CTX, TOK_DEV)
    input_blocks = layer_input.reshape(N_CTX, TOK_DEV, D).astype(jnp.float32)
    cotan_blocks = output_grad.reshape(N_CTX, TOK_DEV, D).astype(jnp.float32)
    route_blocks = routes.reshape(N_CTX, TOK_DEV, TOP)
    gate_blocks = route_gates.reshape(N_CTX, TOK_DEV, TOP)
    routed_rows = N_CTX * EXP_DEV * CAP

    def head_step(carry, head_index):
        input_acc, pair_acc = carry
        query_block = lax.dynamic_slice_in_dim(query_weight, head_index * per_block, per_block, 0).astype(jnp.float32)
        output_block = lax.dynamic_slice_in_dim(output_weight, head_index * per_block, per_block, 0).astype(jnp.float32)
        group_id = head_index // 2
        key_rows = lax.dynamic_index_in_dim(key_values, 2 * group_id, 0, keepdims=False)
        value_rows = lax.dynamic_index_in_dim(key_values, 2 * group_id + 1, 0, keepdims=False)
        first_id = head_index * EXP_DEV
        tables = jax.vmap(slot_table, in_axes=(0, None, None, None))(route_blocks, first_id, EXP_DEV, CAP)
        token_gates = jax.vmap(expert_gate, in_axes=(0, 0, None, None))(route_blocks, gate_blocks, first_id, EXP_DEV)
        picked_input = jnp.einsum('bjct,btd->bjcd', tables, input_blocks, precision=PRECISE).astype(jnp.bfloat16)
        routed_query = jnp.einsum('bjcd,jde->bjce', picked_input.astype(jnp.float32), query_block[:EXP_DEV], precision=PRECISE).astype(jnp.bfloat16)
        shared_query = jnp.einsum('btd,de->bte', input_blocks, query_block[EXP_DEV], precision=PRECISE).astype(jnp.bfloat16)
        picked_cotan = jnp.einsum('bjct,btd->bjcd', tables, cotan_blocks, precision=PRECISE).astype(jnp.bfloat16)
        slot_gate = jnp.einsum('bjct,btj->bjc', tables, token_gates, precision=PRECISE)
        routed_sum = jnp.einsum('bjcd,jde->bjce', picked_cotan.astype(jnp.float32), output_block[:EXP_DEV], precision=PRECISE)
        routed_cotan = (slot_gate[..., None] * routed_sum).astype(jnp.bfloat16)
        shared_cotan = jnp.einsum('btd,de->bte', cotan_blocks, output_block[EXP_DEV], precision=PRECISE).astype(jnp.bfloat16)
        routed_place = jnp.einsum('bjct,bt->bjc', tables, place_blocks, precision=PRECISE)
        queries = jnp.concatenate([routed_query.reshape(-1, HD), shared_query.reshape(-1, HD)], axis=0)
        query_place = jnp.concatenate([routed_place.reshape(-1), place_blocks.reshape(-1)], axis=0)
        head_grads = jnp.concatenate([routed_cotan.reshape(-1, HD), shared_cotan.reshape(-1, HD)], axis=0)
        query_grad, key_grad, value_grad = attend(queries, query_place, key_rows, value_rows, key_place, head_grads)
        routed_qgrad = query_grad[:routed_rows].reshape(N_CTX, EXP_DEV, CAP, HD).astype(jnp.float32)
        token_qgrad = jnp.einsum('bjct,bjce->btje', tables, routed_qgrad, precision=PRECISE).astype(jnp.bfloat16)
        shared_qgrad = query_grad[routed_rows:].reshape(N_CTX, TOK_DEV, 1, HD)
        every_qgrad = jnp.concatenate([token_qgrad, shared_qgrad], axis=2).reshape(TOKENS, per_block, HD)
        input_acc = input_acc + jnp.einsum('tje,jde->td', every_qgrad.astype(jnp.float32), query_block, precision=PRECISE)
        pair_acc = pair_acc.at[2 * group_id].add(key_grad).at[2 * group_id + 1].add(value_grad)
        return (input_acc, pair_acc), None

    initial = (jnp.zeros((TOKENS, D), jnp.float32), jnp.zeros((2 * KVG, TOKENS, HD), jnp.float32))
    (input_acc, pair_acc), ignored = lax.scan(head_step, initial, jnp.arange(N_HEAD, dtype=jnp.int32))
    return input_acc.astype(jnp.bfloat16), pair_acc
```

```python
import functools

import jax
import jax.numpy as jnp
from jax import lax
from jax.experimental import pallas as pl
from jax.experimental.pallas import tpu as pltpu
from jax.sharding import PartitionSpec as P

MESH = pl.DeviceIdType.MESH
ANY = pl.BlockSpec(memory_space=pl.ANY)
VMEM = pl.BlockSpec(memory_space=pltpu.VMEM)
DMA = pltpu.SemaphoreType.DMA
F32, BF16 = jnp.float32, jnp.bfloat16
SUBS = 4


def remote(source, target, send, recv, place):
    return pltpu.make_async_remote_copy(
        src_ref=source,
        dst_ref=target,
        send_sem=send,
        recv_sem=recv,
        device_id=place,
        device_id_type=MESH,
    )


def local(source, target, sem):
    return pltpu.make_async_copy(source, target, sem)


def greet(places):
    barrier = pltpu.get_barrier_semaphore()
    for place in places:
        pl.semaphore_signal(barrier, inc=1, device_id=place, device_id_type=MESH)
    pl.semaphore_wait(barrier, len(places))


def flip(index, bit):
    return index + bit - 2 * bit * ((index // bit) % 2)


def span(start, size):
    return pl.ds(pl.multiple_of(start, size), size)


def pairs(count):
    return [tuple(range(j, min(j + 2, count))) for j in range(0, count, 2)]


class Place:
    def __init__(self):
        self.ctx_count, self.head_count = lax.axis_size("ctx"), lax.axis_size("head")
        self.ctx, self.head = lax.axis_index("ctx"), lax.axis_index("head")
        self.chips = self.ctx_count // 2
        self.chip, self.core = self.ctx // 2, self.ctx % 2
        self.group = self.head_count // self.chips
        self.seat = self.head % self.group
        self.bits = [bit for bit in (1, 2) if bit < self.group]
        self.sibling = (self.ctx + 1 - 2 * self.core, self.head)

    def other(self, hop):
        return lax.rem(self.chip + hop, self.chips)

    def source(self, hop):
        return lax.rem(self.chip - hop + self.chips, self.chips)

    def across(self, hop):
        return (self.other(hop) * 2 + self.core, self.head)

    def beside(self, bit):
        return (self.ctx, flip(self.head, bit))

    def friends(self):
        hops = [self.across(hop) for hop in range(1, self.chips)]
        return hops + [self.beside(bit) for bit in self.bits] + [self.sibling]


class Spread:
    def __init__(self, place, located, count, sems):
        self.place, self.located, self.count = place, located, count
        self.direct_send, self.direct_recv, self.relay_send, self.relay_recv = sems
        self.direct, self.relay = {}, {}

    @staticmethod
    def sems(count):
        return [DMA((2, count))] * 2 + [DMA((count,))] * 2

    def start(self, n):
        for i, bit in enumerate(self.place.bits):
            block = self.located(n, self.place.seat)
            copy = remote(
                block,
                block,
                self.direct_send.at[i, n],
                self.direct_recv.at[i, n],
                self.place.beside(bit),
            )
            copy.start()
            self.direct[n, bit] = copy

    def pass_on(self, n):
        if len(self.place.bits) < 2:
            return
        came, onward = (2, 1) if n % 2 == 0 else (1, 2)
        self.direct[n, came].wait_recv()
        block = self.located(n, flip(self.place.seat, came))
        copy = remote(
            block, block, self.relay_send.at[n], self.relay_recv.at[n], self.place.beside(onward)
        )
        copy.start()
        self.relay[n] = copy

    def arrive(self, n):
        if len(self.place.bits) == 1:
            self.direct[n, 1].wait_recv()
        elif len(self.place.bits) == 2:
            self.direct[n, 1 if n % 2 == 0 else 2].wait_recv()
            self.relay[n].wait_recv()

    def finish(self):
        for copy in list(self.direct.values()) + list(self.relay.values()):
            copy.wait_send()


def contract(rows, weights, total, first):
    heads, depth, width = weights.shape
    step = min(512, depth)

    def body(i, carry):
        part = span(i * step, step)
        left = rows[:, part]
        for group in pairs(heads):
            right = jnp.concatenate([weights[j, part] for j in group], axis=1)
            columns = pl.ds(group[0] * width, len(group) * width)
            total[:, columns] += jnp.dot(left, right, preferred_element_type=F32)
        return carry

    if first:
        total[...] = jnp.zeros_like(total)
    lax.fori_loop(0, depth // step, body, 0)


def front_kernel(
    input_ref,
    cotan_ref,
    route_ref,
    gate_ref,
    query_ref,
    output_ref,
    pair_ref,
    q_out,
    da_out,
    weight_out,
    pair_out,
    mats,
    own,
    far,
    own_sum,
    far_sum,
    q_send_buf,
    q_got,
    da_send_buf,
    da_got,
    load_sem,
    weight_sem,
    x_send,
    x_recv,
    direct_send,
    direct_recv,
    relay_send,
    relay_recv,
    sum_send,
    sum_recv,
    pair_send,
    pair_recv,
    trade_send,
    trade_recv,
    share_send,
    share_recv,
):
    me = Place()
    chips, chip, core, seat, group = me.chips, me.chip, me.core, me.seat, me.group
    heads, depth, width = query_ref.shape
    tokens = input_ref.shape[0]
    half = 2 * depth
    piece = half // group
    acts, sources = (input_ref, cotan_ref), (query_ref, output_ref)
    rows = tokens // SUBS

    mine = span(core * depth, depth)
    loads = []
    for a in range(2):
        loads.append(local(sources[a], mats.at[a, :, mine], load_sem.at[a]))
        loads.append(local(acts[a].at[:, span(chip * half, half)], own.at[a], load_sem.at[2 + a]))
    for copy in loads:
        copy.start()
    diagonal = [(me.ctx, flip(flip(me.head, 1), 2))] if group == 4 else []
    greet(me.friends() + diagonal)

    order = [(a, hop, s) for a in range(2) for hop in range(1, chips) for s in range(SUBS)]

    def located(n, at):
        a, hop, s = order[n]
        return far.at[hop - 1, a, at, pl.ds(s * rows, rows)]

    crossing = []
    for n, (a, hop, s) in enumerate(order):
        begin = pl.multiple_of(me.other(hop) * half + seat * piece, piece)
        copy = remote(
            acts[a].at[pl.ds(s * rows, rows), pl.ds(begin, piece)],
            located(n, seat),
            x_send.at[n],
            x_recv.at[n],
            me.across(hop),
        )
        copy.start()
        crossing.append(copy)
    swaps = []
    for a in range(2):
        copy = remote(
            sources[a], mats.at[a, :, mine], weight_sem.at[a], weight_sem.at[2 + a], me.sibling
        )
        copy.start()
        swaps.append(copy)

    row = me.head % 2

    def key_block(which, at):
        return pair_out.at[which, span(at * tokens, tokens)]

    pair_copies = []
    for hop in range(1, chips):
        copy = remote(
            pair_ref.at[0],
            key_block(row, me.ctx),
            pair_send.at[hop],
            pair_recv.at[hop],
            me.across(hop),
        )
        copy.start()
        pair_copies.append(copy)
    keep = local(pair_ref.at[0], key_block(row, me.ctx), load_sem.at[4])
    keep.start()

    spread = Spread(me, located, len(order), (direct_send, direct_recv, relay_send, relay_recv))

    def own_slice(a, i):
        part = pl.ds(i * piece, piece)
        contract(own.at[a, :, part], mats.at[a, :, part], own_sum.at[a], i == 0)

    def far_slice(a, hop, at, first):
        part = span(at * piece, piece)
        contract(far.at[hop - 1, a, at], mats.at[a, :, part], far_sum.at[hop - 1, a], first)

    own_work = [(a, i) for a in range(2) for i in range(group)]
    seats = [seat] + [flip(seat, 1)] * (group > 1)
    if group == 4:
        seats += [flip(seat, 2), flip(flip(seat, 1), 2)]
    lag = 1
    for copy in loads:
        copy.wait()
    for copy in swaps:
        copy.wait_recv()
    for n in range(len(order)):
        crossing[n].wait_recv()
        spread.start(n)
        if n >= lag:
            spread.pass_on(n - lag)
        if n < len(own_work):
            own_slice(*own_work[n])
    for work in own_work[len(order) :]:
        own_slice(*work)

    sums = []

    def send_sum(a, hop):
        buffer, got = ((q_send_buf, q_got), (da_send_buf, da_got))[a]
        buffer[hop - 1] = far_sum[hop - 1, a].astype(buffer.dtype)
        copy = remote(
            buffer.at[hop - 1],
            got.at[hop - 1],
            sum_send.at[a, hop - 1],
            sum_recv.at[a, hop - 1],
            (me.source(hop) * 2 + core, me.head),
        )
        copy.start()
        sums.append(copy)

    def far_work(a):
        for hop in range(1, chips):
            for n, (b, by, s) in enumerate(order):
                if (b, by) == (a, hop):
                    spread.arrive(n)
            for i, at in enumerate(seats):
                far_slice(a, hop, at, i == 0)
            send_sum(a, hop)

    split = len(order) - lag
    far_work(0)
    for n in range(split, len(order)):
        spread.pass_on(n)

    part_columns = piece // 2
    trades = []
    for j in range(1, group):
        to = seat + 0
        for bit in (1, 2):
            if j & bit:
                to = flip(to, bit)
        copy = remote(
            mats.at[0, :, span(to * piece + core * part_columns, part_columns)],
            weight_out.at[seat, :, span(core * part_columns, part_columns)],
            trade_send.at[j],
            trade_recv.at[j],
            (me.ctx, me.head - seat + to),
        )
        copy.start()
        trades.append((j, copy))
    store = local(mats.at[0, :, span(seat * piece, piece)], weight_out.at[seat], load_sem.at[5])
    store.start()

    keep.wait()
    for copy in pair_copies:
        copy.wait_recv()
    pair_next = []
    for hop in range(chips):
        block = key_block(row, me.source(hop) * 2 + core)
        copy = remote(
            block, block, pair_send.at[chips + hop], pair_recv.at[chips + hop], me.beside(1)
        )
        copy.start()
        pair_next.append(copy)

    far_work(1)

    for copy in pair_next:
        copy.wait_recv()
    pair_last = []
    for hop in range(chips):
        for which in range(2):
            block = key_block(which, me.source(hop) * 2 + core)
            k = 2 * chips + 2 * hop + which
            copy = remote(block, block, pair_send.at[k], pair_recv.at[k], me.sibling)
            copy.start()
            pair_last.append(copy)

    ids = me.head * (heads - 1)
    for hop in range(1, chips):
        sums[hop - 1].wait_recv()
    for j in range(heads):
        columns = pl.ds(j * width, width)
        value = own_sum[0, :, columns]
        for hop in range(1, chips):
            value = value + q_got[hop - 1, :, columns]
        q_out[j] = value.astype(BF16)
    for hop in range(1, chips):
        sums[chips - 1 + hop - 1].wait_recv()
    for j in range(heads):
        columns = pl.ds(j * width, width)
        value = own_sum[1, :, columns]
        for hop in range(1, chips):
            value = value + da_got[hop - 1, :, columns].astype(F32)
        if j < heads - 1:
            named = route_ref[...] == ids + j
            value = value * jnp.sum(
                jnp.where(named, gate_ref[...], 0.0), axis=1, keepdims=True
            )
        da_out[j] = value.astype(BF16)

    shares = []
    for j, copy in trades:
        copy.wait_recv()
        came = seat + 0
        for bit in (1, 2):
            if j & bit:
                came = flip(came, bit)
        block = weight_out.at[came, :, span(core * part_columns, part_columns)]
        share = remote(block, block, share_send.at[j], share_recv.at[j], me.sibling)
        share.start()
        shares.append(share)
    store.wait()
    for copy in shares + pair_last:
        copy.wait()
    for copy in crossing + swaps + pair_copies + pair_next + sums + [copy for _, copy in trades]:
        copy.wait_send()
    spread.finish()


def front(layer_input, output_grad, routes, route_gates, query_weight, output_weight, key_values):
    ctx_count, head_count = lax.axis_size("ctx"), lax.axis_size("head")
    chips = ctx_count // 2
    group, hops = head_count // chips, chips - 1
    heads, depth, width = query_weight.shape
    tokens = layer_input.shape[0]
    half = 2 * depth
    piece = half // group
    count = 2 * hops * SUBS
    rows = jax.ShapeDtypeStruct((heads, tokens, width), BF16)
    return pl.pallas_call(
        front_kernel,
        out_shape=(
            rows,
            rows,
            jax.ShapeDtypeStruct((group, heads, piece, width), BF16),
            jax.ShapeDtypeStruct((2, tokens * ctx_count, width), BF16),
        ),
        in_specs=[ANY, ANY, VMEM, VMEM, ANY, ANY, VMEM],
        out_specs=(VMEM, VMEM, ANY, ANY),
        scratch_shapes=[
            pltpu.VMEM((2, heads, half, width), BF16),
            pltpu.VMEM((2, tokens, half), BF16),
            pltpu.VMEM((hops, 2, group, tokens, piece), BF16),
            pltpu.VMEM((2, tokens, heads * width), F32),
            pltpu.VMEM((hops, 2, tokens, heads * width), F32),
            pltpu.VMEM((hops, tokens, heads * width), F32),
            pltpu.VMEM((hops, tokens, heads * width), F32),
            pltpu.VMEM((hops, tokens, heads * width), BF16),
            pltpu.VMEM((hops, tokens, heads * width), BF16),
            DMA((6,)),
            DMA((4,)),
            DMA((count,)),
            DMA((count,)),
        ]
        + Spread.sems(count)
        + [DMA((2, hops))] * 2
        + [DMA((4 * chips,))] * 2
        + [DMA((group,))] * 4,
        compiler_params=pltpu.CompilerParams(
            collective_id=0, has_side_effects=True, vmem_limit_bytes=60 << 20
        ),
    )(
        layer_input,
        output_grad,
        routes,
        route_gates,
        query_weight,
        output_weight,
        key_values,
    )


def tail_kernel(
    dq_ref,
    weight_ref,
    grads_ref,
    land_out,
    grads_out,
    every,
    mats,
    block_buf,
    load_sem,
    x_send,
    x_recv,
    direct_send,
    direct_recv,
    relay_send,
    relay_recv,
    land_send,
    land_recv,
    grads_send,
    grads_recv,
):
    me = Place()
    chips, chip, core, seat, group = me.chips, me.chip, me.core, me.seat, me.group
    heads, tokens, width = dq_ref.shape
    piece = weight_ref.shape[2]
    family = me.head // group
    load = local(weight_ref, mats, load_sem.at[0])
    load.start()
    keep = local(dq_ref, every.at[chip, seat], load_sem.at[1])
    keep.start()

    steps = [(step, turn) for step in range(me.ctx_count) for turn in range(2) if step or turn]

    def partner(step, turn):
        return (
            lax.rem(me.ctx + step, me.ctx_count),
            me.head + turn * (1 - 2 * (me.head % 2)),
        )

    targets = [(me.other(hop) * 2 + core, chip * group + seat) for hop in range(chips)]
    givers = [(family * 2 + core, r * group + seat) for r in range(chips)]
    grads_places = [partner(step, turn) for step, turn in steps]
    barrier = pltpu.get_barrier_semaphore()
    sure = grads_places + me.friends()[:-1]
    for spot in sure + targets + givers:
        pl.semaphore_signal(barrier, inc=1, device_id=spot, device_id_type=MESH)
    pl.semaphore_wait(barrier, len(sure) + len(targets) + len(givers))

    order = [(hop, s) for hop in range(chips) for s in range(2)]
    rows = tokens // 2

    def located(n, at):
        hop, s = order[n]
        return every.at[me.source(hop), at, :, pl.ds(s * rows, rows)]

    spread = Spread(me, located, len(order), (direct_send, direct_recv, relay_send, relay_recv))
    crossing = {}
    for hop in range(1, chips):
        for s in range(2):
            n = order.index((hop, s))
            copy = remote(
                dq_ref.at[:, pl.ds(s * rows, rows)],
                every.at[chip, seat, :, pl.ds(s * rows, rows)],
                x_send.at[n],
                x_recv.at[n],
                me.across(hop),
            )
            copy.start()
            crossing[n] = copy
    keep.wait()
    for n, (hop, s) in enumerate(order):
        if hop:
            crossing[n].wait_recv()
        spread.start(n)
        if n >= 2:
            spread.pass_on(n - 2)
    for n in range(len(order) - 2, len(order)):
        spread.pass_on(n)

    grads_copies = []
    for n, spot in enumerate(grads_places):
        copy = remote(
            grads_ref.at[spot[1] % 2, spot[0]],
            grads_out.at[n],
            grads_send.at[n],
            grads_recv.at[n],
            spot,
        )
        copy.start()
        grads_copies.append(copy)
    load.wait()

    step = min(256, piece)
    flat = [(m, j) for m in range(group) for j in range(heads)]

    def multiply(hop):
        at = me.source(hop)

        def body(i, carry):
            part = span(i * step, step)
            total = jnp.zeros((tokens, step), F32)
            for k in range(0, len(flat), 2):
                both = flat[k : k + 2]
                left = jnp.concatenate([every[at, m, j] for m, j in both], axis=1)
                right = jnp.concatenate([mats[m, j, part] for m, j in both], axis=1)
                total += lax.dot_general(
                    left, right, (((1,), (1,)), ((), ())), preferred_element_type=F32
                )
            block_buf[hop, :, part] = total.astype(BF16)
            return carry

        lax.fori_loop(0, piece // step, body, 0)

    sent = {}
    stay = family == chip
    for hop in list(range(1, chips)) + [0]:
        for n, (by, s) in enumerate(order):
            if by == hop:
                spread.arrive(n)
        multiply(hop)
        spot = (me.source(hop) * 2 + core, chip * group + seat)
        copy = remote(
            block_buf.at[hop],
            land_out.at[family],
            land_send.at[hop],
            land_recv.at[family],
            spot,
        )
        sent[hop] = copy
        if hop:
            copy.start()
        else:
            pl.when(jnp.logical_not(stay))(copy.start)
            inside = local(block_buf.at[0], land_out.at[family], load_sem.at[2])
            pl.when(stay)(inside.start)

    for copy in grads_copies:
        copy.wait()
    for hop in range(1, chips):
        sent[hop].wait_send()
    pl.when(jnp.logical_not(stay))(sent[0].wait_send)
    pl.when(stay)(inside.wait)
    for r in range(chips):
        arrival = remote(
            block_buf.at[0], land_out.at[r], land_send.at[0], land_recv.at[r], me.sibling
        )
        pl.when(jnp.logical_not(jnp.logical_and(stay, family == r)))(arrival.wait_recv)
    for copy in crossing.values():
        copy.wait_send()
    spread.finish()


def tail(dq, weights, grads):
    ctx_count, head_count = lax.axis_size("ctx"), lax.axis_size("head")
    chips = ctx_count // 2
    heads, tokens, width = dq.shape
    group, _, piece, _ = weights.shape
    others = 2 * ctx_count - 1
    count = 2 * chips
    return pl.pallas_call(
        tail_kernel,
        out_shape=(
            jax.ShapeDtypeStruct((chips, tokens, piece), BF16),
            jax.ShapeDtypeStruct((others,) + grads.shape[2:], grads.dtype),
        ),
        in_specs=[VMEM, ANY, ANY],
        out_specs=(ANY, ANY),
        scratch_shapes=[
            pltpu.VMEM((chips, group, heads, tokens, width), BF16),
            pltpu.VMEM((group, heads, piece, width), BF16),
            pltpu.VMEM((chips, tokens, piece), BF16),
            DMA((3,)),
            DMA((count,)),
            DMA((count,)),
        ]
        + Spread.sems(count)
        + [DMA((chips,))] * 2
        + [DMA((others,))] * 2,
        compiler_params=pltpu.CompilerParams(
            collective_id=1, has_side_effects=True, vmem_limit_bytes=60 << 20
        ),
    )(dq, weights, grads)


def attend(queries, query_place, key_rows, value_rows, key_place, head_grads):
    score_scale = queries.shape[1] ** (-0.5)
    scores = jnp.dot(queries, key_rows.T, preferred_element_type=F32) * score_scale
    scores = jnp.where(key_place[None, :] <= query_place[:, None], scores, -1e30)
    row_max = jnp.max(scores, axis=1, keepdims=True)
    raised = jnp.exp(scores - row_max)
    shares = raised / jnp.sum(raised, axis=1, keepdims=True)
    shares_low = shares.astype(BF16)
    outputs = jnp.dot(shares_low, value_rows, preferred_element_type=F32)
    share_grad = jnp.dot(head_grads, value_rows.T, preferred_element_type=F32)
    row_delta = jnp.sum(head_grads.astype(F32) * outputs, axis=1, keepdims=True)
    score_grad = (shares * (share_grad - row_delta) * score_scale).astype(BF16)
    query_grad = jnp.dot(score_grad, key_rows, preferred_element_type=F32).astype(BF16)
    key_grad = jnp.dot(score_grad.T, queries, preferred_element_type=F32)
    value_grad = jnp.dot(shares_low.T, head_grads, preferred_element_type=F32)
    return (query_grad, key_grad, value_grad)


def per_device(
    layer_input, output_grad, routes, route_gates, query_weight, output_weight, key_values
):
    tokens = layer_input.shape[0]
    heads, _, width = query_weight.shape
    ctx_count = lax.axis_size("ctx")
    ctx_index, head_index = lax.axis_index("ctx"), lax.axis_index("head")
    queries, head_grads, weights, pair = front(
        layer_input, output_grad, routes, route_gates, query_weight, output_weight, key_values
    )
    token_place = ctx_index * tokens + jnp.arange(tokens, dtype=jnp.int32)
    query_place = jnp.tile(token_place, heads)
    key_place = jnp.arange(tokens * ctx_count, dtype=jnp.int32)
    query_grad, key_grad, value_grad = attend(
        queries.reshape(-1, width),
        query_place,
        pair[0],
        pair[1],
        key_place,
        head_grads.reshape(-1, width),
    )
    grads = jnp.stack([key_grad, value_grad]).astype(BF16)
    grads = grads.reshape(2, ctx_count, tokens, width)
    landed, grads_got = tail(query_grad.reshape(heads, tokens, width), weights, grads)
    input_grad = jnp.sum(landed.astype(F32), axis=0).astype(BF16)
    own_grads = grads[head_index % 2, ctx_index].astype(F32)
    kept_rows = own_grads + jnp.sum(grads_got.astype(F32), axis=0)
    return (input_grad, kept_rows[None])


def solution(mesh):
    in_specs = (
        P("ctx", None),
        P("ctx", None),
        P("ctx", None),
        P("ctx", None),
        P("head", "ctx", None),
        P("head", "ctx", None),
        P("head", "ctx", None),
    )
    out_specs = (P("ctx", "head"), P("head", "ctx", None))
    return jax.shard_map(
        per_device, mesh=mesh, in_specs=in_specs, out_specs=out_specs, check_vma=False
    )
```

```python
import functools

import jax
import jax.numpy as jnp
from jax import lax
from jax.experimental import pallas as pl
from jax.experimental.pallas import tpu as pltpu
from jax.sharding import PartitionSpec as P

MESH = pl.DeviceIdType.MESH
ANY = pl.BlockSpec(memory_space=pl.ANY)
VMEM = pl.BlockSpec(memory_space=pltpu.VMEM)
DMA = pltpu.SemaphoreType.DMA
F32, BF16 = jnp.float32, jnp.bfloat16
SUBS = 4
VMEM_BYTES = 67_043_328


def remote(source, target, send, recv, place):
    return pltpu.make_async_remote_copy(
        src_ref=source,
        dst_ref=target,
        send_sem=send,
        recv_sem=recv,
        device_id=place,
        device_id_type=MESH,
    )


def local(source, target, sem):
    return pltpu.make_async_copy(source, target, sem)


def greet(places):
    barrier = pltpu.get_barrier_semaphore()
    for place in places:
        pl.semaphore_signal(barrier, inc=1, device_id=place, device_id_type=MESH)
    pl.semaphore_wait(barrier, len(places))


def flip(index, bit):
    return index + bit - 2 * bit * ((index // bit) % 2)


def span(start, size):
    return pl.ds(pl.multiple_of(start, size), size)


def pairs(count):
    return [tuple(range(j, min(j + 2, count))) for j in range(0, count, 2)]


class Place:
    def __init__(self):
        self.ctx_count, self.head_count = lax.axis_size("ctx"), lax.axis_size("head")
        self.ctx, self.head = lax.axis_index("ctx"), lax.axis_index("head")
        self.chips = self.ctx_count // 2
        self.chip, self.core = self.ctx // 2, self.ctx % 2
        self.group = self.head_count // self.chips
        self.seat = self.head % self.group
        self.bits = [bit for bit in (1, 2) if bit < self.group]
        self.sibling = (self.ctx + 1 - 2 * self.core, self.head)

    def other(self, hop):
        return lax.rem(self.chip + hop, self.chips)

    def source(self, hop):
        return lax.rem(self.chip - hop + self.chips, self.chips)

    def across(self, hop):
        return (self.other(hop) * 2 + self.core, self.head)

    def beside(self, bit):
        return (self.ctx, flip(self.head, bit))

    def friends(self):
        hops = [self.across(hop) for hop in range(1, self.chips)]
        return hops + [self.beside(bit) for bit in self.bits] + [self.sibling]


class Spread:
    def __init__(self, place, located, count, sems):
        self.place, self.located, self.count = place, located, count
        self.direct_send, self.direct_recv, self.relay_send, self.relay_recv = sems
        self.direct, self.relay = {}, {}

    @staticmethod
    def sems(count):
        return [DMA((2, count))] * 2 + [DMA((count,))] * 2

    def start(self, n):
        for i, bit in enumerate(self.place.bits):
            block = self.located(n, self.place.seat)
            copy = remote(
                block,
                block,
                self.direct_send.at[i, n],
                self.direct_recv.at[i, n],
                self.place.beside(bit),
            )
            copy.start()
            self.direct[n, bit] = copy

    def pass_on(self, n):
        if len(self.place.bits) < 2:
            return
        came, onward = (2, 1) if n % 2 == 0 else (1, 2)
        self.direct[n, came].wait_recv()
        block = self.located(n, flip(self.place.seat, came))
        copy = remote(
            block, block, self.relay_send.at[n], self.relay_recv.at[n], self.place.beside(onward)
        )
        copy.start()
        self.relay[n] = copy

    def arrive(self, n):
        if len(self.place.bits) == 1:
            self.direct[n, 1].wait_recv()
        elif len(self.place.bits) == 2:
            self.direct[n, 1 if n % 2 == 0 else 2].wait_recv()
            self.relay[n].wait_recv()

    def finish(self):
        for copy in list(self.direct.values()) + list(self.relay.values()):
            copy.wait_send()


def contract(rows, weights, total, first):
    heads, depth, width = weights.shape
    step = min(512, depth)

    def body(i, carry):
        part = span(i * step, step)
        left = rows[:, part]
        for group in pairs(heads):
            right = jnp.concatenate([weights[j, part] for j in group], axis=1)
            columns = pl.ds(group[0] * width, len(group) * width)
            total[:, columns] += jnp.dot(left, right, preferred_element_type=F32)
        return carry

    if first:
        total[...] = jnp.zeros(total.shape, F32)
    lax.fori_loop(0, depth // step, body, 0)


def layer_kernel(
    input_ref,
    cotan_ref,
    route_ref,
    gate_ref,
    query_ref,
    output_ref,
    pair_ref,
    input_grad_out,
    kept_out,
    mats,
    own,
    far,
    own_sum,
    far_sum,
    q_got,
    da_low,
    da_got,
    queries,
    cotans,
    group_mats,
    keys,
    turned,
    turned_grads,
    grads_low,
    grads_got,
    every,
    made,
    hub,
    land,
    load_sem,
    weight_sem,
    x_send,
    x_recv,
    direct_send,
    direct_recv,
    relay_send,
    relay_recv,
    sum_send,
    sum_recv,
    pair_send,
    pair_recv,
    trade_send,
    trade_recv,
    share_send,
    share_recv,
    dq_send,
    dq_recv,
    dq_direct_send,
    dq_direct_recv,
    dq_relay_send,
    dq_relay_recv,
    grads_send,
    grads_recv,
    made_send,
    made_recv,
    land_send,
    land_recv,
):
    me = Place()
    chips, chip, core, seat, group = me.chips, me.chip, me.core, me.seat, me.group
    heads, depth, width = query_ref.shape
    tokens = input_ref.shape[0]
    window = tokens * me.ctx_count
    half = 2 * depth
    piece = half // group
    family = me.head // group
    acts, sources = (input_ref, cotan_ref), (query_ref, output_ref)
    rows = tokens // SUBS
    part_rows = tokens // 2

    mine = span(core * depth, depth)
    loads = []
    for a in range(2):
        loads.append(local(sources[a], mats.at[a, :, mine], load_sem.at[a]))
        loads.append(local(acts[a].at[:, span(chip * half, half)], own.at[a], load_sem.at[2 + a]))

    steps = [(step, turn) for step in range(me.ctx_count) for turn in range(2) if step or turn]
    grads_places = [
        (lax.rem(me.ctx + step, me.ctx_count), me.head + turn * (1 - 2 * (me.head % 2)))
        for step, turn in steps
    ]
    places = grads_places + [me.beside(bit) for bit in me.bits[1:]]
    if group == 4:
        places.append((me.ctx, flip(flip(me.head, 1), 2)))
    homes = [lax.rem(family + i, chips) for i in range(1, chips)]
    places += [(me.ctx, home * group + seat) for home in homes]
    greet(places)

    order = [(a, hop, s) for a in range(2) for hop in range(1, chips) for s in range(SUBS)]

    def located(n, at):
        a, hop, s = order[n]
        return far.at[hop - 1, a, at, pl.ds(s * rows, rows)]

    crossing = []
    for n, (a, hop, s) in enumerate(order):
        begin = pl.multiple_of(me.other(hop) * half + seat * piece, piece)
        copy = remote(
            acts[a].at[pl.ds(s * rows, rows), pl.ds(begin, piece)],
            located(n, seat),
            x_send.at[n],
            x_recv.at[n],
            me.across(hop),
        )
        copy.start()
        crossing.append(copy)
    for copy in loads:
        copy.start()
    swaps = []
    for a in range(2):
        copy = remote(
            sources[a], mats.at[a, :, mine], weight_sem.at[a], weight_sem.at[2 + a], me.sibling
        )
        copy.start()
        swaps.append(copy)

    row = me.head % 2

    def key_block(which, at):
        return keys.at[which, span(at * tokens, tokens)]

    pair_copies = []
    for hop in range(1, chips):
        copy = remote(
            pair_ref.at[0],
            key_block(row, me.ctx),
            pair_send.at[hop],
            pair_recv.at[hop],
            me.across(hop),
        )
        copy.start()
        pair_copies.append(copy)
    keep = local(pair_ref.at[0], key_block(row, me.ctx), load_sem.at[4])
    keep.start()

    spread = Spread(me, located, len(order), (direct_send, direct_recv, relay_send, relay_recv))

    def own_slice(a, i):
        part = pl.ds(i * piece, piece)
        contract(own.at[a, :, part], mats.at[a, :, part], own_sum.at[a], i == 0)

    seats = [seat] + [flip(seat, 1)] * (group > 1)
    if group == 4:
        seats += [flip(seat, 2), flip(flip(seat, 1), 2)]
    sums = {}

    def far_part(a, hop, p):
        block = pl.ds(p * part_rows, part_rows)
        for n, (b, by, s) in enumerate(order):
            if (b, by) == (a, hop) and s // (SUBS // 2) == p:
                spread.arrive(n)
        for i, at in enumerate(seats):
            part = span(at * piece, piece)
            contract(
                far.at[hop - 1, a, at, block],
                mats.at[a, :, part],
                far_sum.at[hop - 1, a, block],
                i == 0,
            )
        if a == 0:
            source, target = far_sum.at[hop - 1, 0, block], q_got.at[hop - 1, block]
        else:
            da_low[hop - 1, block] = far_sum[hop - 1, 1, block].astype(BF16)
            source, target = da_low.at[hop - 1, block], da_got.at[hop - 1, block]
        copy = remote(
            source,
            target,
            sum_send.at[a, hop - 1, p],
            sum_recv.at[a, hop - 1, p],
            (me.source(hop) * 2 + core, me.head),
        )
        copy.start()
        sums[a, hop, p] = copy

    own_work = [(a, i) for a in range(2) for i in range(group)]
    count = len(order)
    for n in range(count):
        crossing[n].wait_recv()
        spread.start(n)
        if n >= 1:
            spread.pass_on(n - 1)
        if n == 1:
            for copy in loads:
                copy.wait()
            for copy in swaps:
                copy.wait_recv()
        if n >= 2 and own_work:
            own_slice(*own_work.pop(0))
        if chips == 2 and n == count - 3:
            far_part(0, 1, 0)
    spread.pass_on(count - 1)

    part_columns = piece // 2
    ours = span(core * part_columns, part_columns)
    trades = []

    def seat_of(j):
        at = seat + 0
        for bit in (1, 2):
            if j & bit:
                at = flip(at, bit)
        return at

    for j in range(1, group):
        to = seat_of(j)
        copy = remote(
            mats.at[0, :, span(to * piece + core * part_columns, part_columns)],
            group_mats.at[seat, :, ours],
            trade_send.at[j],
            trade_recv.at[j],
            (me.ctx, me.head - seat + to),
        )
        copy.start()
        trades.append((j, copy))
    store = local(mats.at[0, :, span(seat * piece, piece)], group_mats.at[seat], load_sem.at[5])
    store.start()

    keep.wait()
    for copy in pair_copies:
        copy.wait_recv()
    pair_next = []
    for hop in range(chips):
        block = key_block(row, me.source(hop) * 2 + core)
        copy = remote(
            block, block, pair_send.at[chips + hop], pair_recv.at[chips + hop], me.beside(1)
        )
        copy.start()
        pair_next.append(copy)

    for work in own_work:
        own_slice(*work)
    for a in range(2):
        for p in range(2):
            for hop in range(1, chips):
                if (a, hop, p) not in sums:
                    far_part(a, hop, p)

    for copy in pair_next:
        copy.wait_recv()
    pair_last = []
    for hop in range(chips):
        for which in range(2):
            block = key_block(which, me.source(hop) * 2 + core)
            k = 2 * chips + 2 * hop + which
            copy = remote(block, block, pair_send.at[k], pair_recv.at[k], me.sibling)
            copy.start()
            pair_last.append(copy)

    lanes = []
    for j in range(heads - 1):
        named = route_ref[...] == me.head * (heads - 1) + j
        lanes.append(jnp.sum(jnp.where(named, gate_ref[...], 0.0), axis=0, keepdims=True))
    lanes.append(jnp.ones_like(lanes[0]))
    lanes += [jnp.zeros_like(lanes[0])] * (-heads % 8)
    token_gate = jnp.transpose(jnp.concatenate(lanes, axis=0))

    for hop in range(1, chips):
        for p in range(2):
            sums[0, hop, p].wait_recv()
    for j in range(heads):
        columns = pl.ds(j * width, width)
        value = own_sum[0, :, columns]
        for hop in range(1, chips):
            value = value + q_got[hop - 1, :, columns]
        queries[j] = value.astype(BF16)
    for copy in pair_last:
        copy.wait_recv()
    for which in range(2):
        for at in range(me.ctx_count):
            block = pl.ds(at * tokens, tokens)
            turned[which, :, block] = jnp.transpose(keys[which, block])
    for hop in range(1, chips):
        for p in range(2):
            sums[1, hop, p].wait_recv()
    for j in range(heads):
        columns = pl.ds(j * width, width)
        value = own_sum[1, :, columns]
        for hop in range(1, chips):
            value = value + da_got[hop - 1, :, columns].astype(F32)
        if j < heads - 1:
            value = value * token_gate[:, j : j + 1]
        cotans[j] = value.astype(BF16)

    units = [(hop, j) for hop in range(chips) for j in range(heads)]

    def unit(n, at):
        hop, j = units[n]
        return every.at[me.source(hop), at, j]

    dq_spread = Spread(
        me, unit, len(units), (dq_direct_send, dq_direct_recv, dq_relay_send, dq_relay_recv)
    )
    block_rows = min(tokens, max(16, 256 * 1024 // window))
    scale = width ** (-0.5)
    turned_grads[...] = jnp.zeros(turned_grads.shape, F32)

    def attend(j):
        def body(i, carry):
            block = span(i * block_rows, block_rows)
            query, cotan = queries[j, block], cotans[j, block]
            scores = jnp.dot(query, turned[0], preferred_element_type=F32) * scale
            first = me.ctx * tokens + i * block_rows
            place = first + lax.broadcasted_iota(jnp.int32, scores.shape, 0)
            scores = jnp.where(
                lax.broadcasted_iota(jnp.int32, scores.shape, 1) <= place, scores, -1e30
            )
            raised = jnp.exp(scores - jnp.max(scores, axis=1, keepdims=True))
            shares = raised / jnp.sum(raised, axis=1, keepdims=True)
            low = shares.astype(BF16)
            outputs = jnp.dot(low, keys[1], preferred_element_type=F32)
            share_grad = jnp.dot(cotan, turned[1], preferred_element_type=F32)
            delta = jnp.sum(cotan.astype(F32) * outputs, axis=1, keepdims=True)
            score_grad = (shares * (share_grad - delta) * scale).astype(BF16)
            every[chip, seat, j, block] = jnp.dot(
                score_grad, keys[0], preferred_element_type=F32
            ).astype(BF16)
            turned_grads[0] += jnp.dot(
                jnp.transpose(query), score_grad, preferred_element_type=F32
            )
            turned_grads[1] += jnp.dot(jnp.transpose(cotan), low, preferred_element_type=F32)
            return carry

        lax.fori_loop(0, tokens // block_rows, body, 0)

    dq_copies = {}
    for j in range(heads):
        attend(j)
        for hop in range(1, chips):
            n = units.index((hop, j))
            copy = remote(
                every.at[chip, seat, j],
                every.at[chip, seat, j],
                dq_send.at[n],
                dq_recv.at[n],
                me.across(hop),
            )
            copy.start()
            dq_copies[n] = copy
        dq_spread.start(j)
    for n in range(heads, len(units)):
        dq_copies[n].wait_recv()
        dq_spread.start(n)
        dq_spread.pass_on(n - heads)
    for n in range(len(units) - heads, len(units)):
        dq_spread.pass_on(n)

    for which in range(2):
        for at in range(me.ctx_count):
            block = pl.ds(at * tokens, tokens)
            grads_low[which, at] = jnp.transpose(turned_grads[which, :, block]).astype(BF16)
    grads_copies = []
    for n, spot in enumerate(grads_places):
        copy = remote(
            grads_low.at[spot[1] % 2, spot[0]],
            grads_got.at[n],
            grads_send.at[n],
            grads_recv.at[n],
            spot,
        )
        copy.start()
        grads_copies.append(copy)

    shares = []
    for j, copy in trades:
        copy.wait_recv()
        block = group_mats.at[seat_of(j), :, ours]
        share = remote(block, block, share_send.at[j], share_recv.at[j], me.sibling)
        share.start()
        shares.append(share)
    store.wait()
    for copy in shares:
        copy.wait_recv()

    chunks, chunk = made.shape[1], made.shape[3]
    flat = [(m, j) for m in range(group) for j in range(heads)]

    def made_copy(hop, i):
        return remote(
            made.at[hop - 1, i],
            hub.at[chips - hop, i],
            made_send.at[hop - 1, i],
            made_recv.at[chips - hop - 1, i],
            (me.source(hop) * 2 + core, me.head),
        )

    def land_copy(hop, i):
        return remote(
            hub.at[hop, i],
            land.at[family, i],
            land_send.at[hop, i],
            land_recv.at[family, i],
            (me.ctx, me.source(hop) * group + seat),
        )

    def moves(hop):
        return me.source(hop) != family

    def multiply(hop):
        at = me.source(hop)
        result = made.at[hop - 1] if hop else hub.at[0]

        def body(i, carry):
            part = span(i * chunk, chunk)
            total = jnp.zeros((tokens, chunk), F32)
            for k in range(0, len(flat), 2):
                both = flat[k : k + 2]
                left = jnp.concatenate([every[at, m, j] for m, j in both], axis=1)
                right = jnp.concatenate([group_mats[m, j, part] for m, j in both], axis=1)
                total += lax.dot_general(
                    left, right, (((1,), (1,)), ((), ())), preferred_element_type=F32
                )
            result[i] = total.astype(BF16)
            if hop:
                made_copy(hop, i).start()
            else:
                pl.when(moves(0))(land_copy(0, i).start)
            return carry

        lax.fori_loop(0, chunks, body, 0)

    for hop in list(range(1, chips)) + [0]:
        for n, (by, j) in enumerate(units):
            if by == hop:
                dq_spread.arrive(n)
        multiply(hop)
    for hop in range(1, chips):
        for i in range(chunks):
            made_copy(chips - hop, i).wait_recv()
            pl.when(moves(hop))(land_copy(hop, i).start)

    for copy in grads_copies:
        copy.wait()
    kept = grads_low[row, me.ctx].astype(F32)
    for n in range(len(grads_places)):
        kept = kept + grads_got[n].astype(F32)
    kept_out[0] = kept

    stay = lax.rem(chip - family + chips, chips)
    for i in range(chunks):
        total = hub[stay, i].astype(F32)
        for home in homes:
            arrival = remote(
                hub.at[0, i], land.at[home, i], land_send.at[0, i], land_recv.at[home, i], me.sibling
            )
            arrival.wait_recv()
            total = total + land[home, i].astype(F32)
        input_grad_out[:, pl.ds(i * chunk, chunk)] = total.astype(BF16)

    for hop in range(chips):
        for i in range(chunks):
            if hop:
                made_copy(hop, i).wait_send()
            pl.when(moves(hop))(land_copy(hop, i).wait_send)
    for copy in crossing + swaps + pair_copies + pair_next + pair_last + shares:
        copy.wait_send()
    for copy in list(sums.values()) + list(dq_copies.values()):
        copy.wait_send()
    for j, copy in trades:
        copy.wait_send()
    spread.finish()
    dq_spread.finish()


def per_device(
    layer_input, output_grad, routes, route_gates, query_weight, output_weight, key_values
):
    ctx_count, head_count = lax.axis_size("ctx"), lax.axis_size("head")
    chips = ctx_count // 2
    group, hops = head_count // chips, chips - 1
    heads, depth, width = query_weight.shape
    tokens = layer_input.shape[0]
    half = 2 * depth
    piece = half // group
    window = tokens * ctx_count
    others = 2 * ctx_count - 1
    count, units = 2 * hops * SUBS, chips * heads
    chunk = min(256, piece)
    chunks = piece // chunk
    return pl.pallas_call(
        layer_kernel,
        out_shape=(
            jax.ShapeDtypeStruct((tokens, piece), BF16),
            jax.ShapeDtypeStruct((1, tokens, width), F32),
        ),
        in_specs=[ANY, ANY, VMEM, VMEM, ANY, ANY, VMEM],
        out_specs=(VMEM, VMEM),
        scratch_shapes=[
            pltpu.VMEM((2, heads, half, width), BF16),
            pltpu.VMEM((2, tokens, half), BF16),
            pltpu.VMEM((hops, 2, group, tokens, piece), BF16),
            pltpu.VMEM((2, tokens, heads * width), F32),
            pltpu.VMEM((hops, 2, tokens, heads * width), F32),
            pltpu.VMEM((hops, tokens, heads * width), F32),
            pltpu.VMEM((hops, tokens, heads * width), BF16),
            pltpu.VMEM((hops, tokens, heads * width), BF16),
            pltpu.VMEM((heads, tokens, width), BF16),
            pltpu.VMEM((heads, tokens, width), BF16),
            pltpu.VMEM((group, heads, piece, width), BF16),
            pltpu.VMEM((2, window, width), BF16),
            pltpu.VMEM((2, width, window), BF16),
            pltpu.VMEM((2, width, window), F32),
            pltpu.VMEM((2, ctx_count, tokens, width), BF16),
            pltpu.VMEM((others, tokens, width), BF16),
            pltpu.VMEM((chips, group, heads, tokens, width), BF16),
            pltpu.VMEM((hops, chunks, tokens, chunk), BF16),
            pltpu.VMEM((chips, chunks, tokens, chunk), BF16),
            pltpu.VMEM((chips, chunks, tokens, chunk), BF16),
            DMA((6,)),
            DMA((4,)),
            DMA((count,)),
            DMA((count,)),
        ]
        + Spread.sems(count)
        + [DMA((2, hops, 2))] * 2
        + [DMA((4 * chips,))] * 2
        + [DMA((group,))] * 4
        + [DMA((units,))] * 2
        + Spread.sems(units)
        + [DMA((others,))] * 2
        + [DMA((hops, chunks))] * 2
        + [DMA((chips, chunks))] * 2,
        compiler_params=pltpu.CompilerParams(
            collective_id=0, has_side_effects=True, vmem_limit_bytes=VMEM_BYTES
        ),
    )(
        layer_input,
        output_grad,
        routes.T,
        route_gates.T,
        query_weight,
        output_weight,
        key_values,
    )


def solution(mesh):
    in_specs = (
        P("ctx", None),
        P("ctx", None),
        P("ctx", None),
        P("ctx", None),
        P("head", "ctx", None),
        P("head", "ctx", None),
        P("head", "ctx", None),
    )
    out_specs = (P("ctx", "head"), P("head", "ctx", None))
    return jax.shard_map(
        per_device, mesh=mesh, in_specs=in_specs, out_specs=out_specs, check_vma=False
    )
```

```python
import functools

import jax
import jax.numpy as jnp
from jax import lax
from jax.experimental import pallas as pl
from jax.experimental.pallas import tpu as pltpu
from jax.sharding import PartitionSpec as P

MESH = pl.DeviceIdType.MESH
ANY = pl.BlockSpec(memory_space=pl.ANY)
VMEM = pl.BlockSpec(memory_space=pltpu.VMEM)
DMA = pltpu.SemaphoreType.DMA
F32, BF16 = jnp.float32, jnp.bfloat16
SUBS = 4
VMEM_BYTES = 67_043_328


def remote(source, target, send, recv, place):
    return pltpu.make_async_remote_copy(
        src_ref=source,
        dst_ref=target,
        send_sem=send,
        recv_sem=recv,
        device_id=place,
        device_id_type=MESH,
    )


def local(source, target, sem):
    return pltpu.make_async_copy(source, target, sem)


def greet(places):
    barrier = pltpu.get_barrier_semaphore()
    for place in places:
        pl.semaphore_signal(barrier, inc=1, device_id=place, device_id_type=MESH)
    pl.semaphore_wait(barrier, len(places))


def flip(index, bit):
    return index + bit - 2 * bit * ((index // bit) % 2)


def span(start, size):
    return pl.ds(pl.multiple_of(start, size), size)


def pairs(count):
    return [tuple(range(j, min(j + 2, count))) for j in range(0, count, 2)]


class Place:
    def __init__(self):
        self.ctx_count, self.head_count = lax.axis_size("ctx"), lax.axis_size("head")
        self.ctx, self.head = lax.axis_index("ctx"), lax.axis_index("head")
        self.chips = self.ctx_count // 2
        self.chip, self.core = self.ctx // 2, self.ctx % 2
        self.group = self.head_count // self.chips
        self.seat = self.head % self.group
        self.bits = [bit for bit in (1, 2) if bit < self.group]
        self.sibling = (self.ctx + 1 - 2 * self.core, self.head)

    def other(self, hop):
        return lax.rem(self.chip + hop, self.chips)

    def source(self, hop):
        return lax.rem(self.chip - hop + self.chips, self.chips)

    def across(self, hop):
        return (self.other(hop) * 2 + self.core, self.head)

    def beside(self, bit):
        return (self.ctx, flip(self.head, bit))

    def friends(self):
        hops = [self.across(hop) for hop in range(1, self.chips)]
        return hops + [self.beside(bit) for bit in self.bits] + [self.sibling]


class Spread:
    def __init__(self, place, located, count, sems):
        self.place, self.located, self.count = place, located, count
        self.direct_send, self.direct_recv, self.relay_send, self.relay_recv = sems
        self.direct, self.relay = {}, {}

    @staticmethod
    def sems(count):
        return [DMA((2, count))] * 2 + [DMA((count,))] * 2

    def start(self, n):
        for i, bit in enumerate(self.place.bits):
            block = self.located(n, self.place.seat)
            copy = remote(
                block,
                block,
                self.direct_send.at[i, n],
                self.direct_recv.at[i, n],
                self.place.beside(bit),
            )
            copy.start()
            self.direct[n, bit] = copy

    def pass_on(self, n):
        if len(self.place.bits) < 2:
            return
        came, onward = (2, 1) if n % 2 == 0 else (1, 2)
        self.direct[n, came].wait_recv()
        block = self.located(n, flip(self.place.seat, came))
        copy = remote(
            block, block, self.relay_send.at[n], self.relay_recv.at[n], self.place.beside(onward)
        )
        copy.start()
        self.relay[n] = copy

    def arrive(self, n):
        if len(self.place.bits) == 1:
            self.direct[n, 1].wait_recv()
        elif len(self.place.bits) == 2:
            self.direct[n, 1 if n % 2 == 0 else 2].wait_recv()
            self.relay[n].wait_recv()

    def finish(self):
        for copy in list(self.direct.values()) + list(self.relay.values()):
            copy.wait_send()


def contract(rows, weights, total, first):
    heads, depth, width = weights.shape
    step = min(512, depth)

    def body(i, carry):
        part = span(i * step, step)
        left = rows[:, part]
        for group in pairs(heads):
            right = jnp.concatenate([weights[j, part] for j in group], axis=1)
            columns = pl.ds(group[0] * width, len(group) * width)
            total[:, columns] += jnp.dot(left, right, preferred_element_type=F32)
        return carry

    if first:
        total[...] = jnp.zeros(total.shape, F32)
    lax.fori_loop(0, depth // step, body, 0)


def layer_kernel(
    input_ref,
    cotan_ref,
    route_ref,
    gate_ref,
    query_ref,
    output_ref,
    pair_ref,
    input_grad_out,
    kept_out,
    mats,
    own,
    far,
    own_sum,
    far_sum,
    q_got,
    da_low,
    da_got,
    queries,
    cotans,
    group_mats,
    keys,
    turned,
    turned_grads,
    core_got,
    grads_low,
    chip_got,
    pair_low,
    pair_got,
    every,
    made,
    hub,
    land,
    load_sem,
    weight_sem,
    x_send,
    x_recv,
    direct_send,
    direct_recv,
    relay_send,
    relay_recv,
    sum_send,
    sum_recv,
    pair_send,
    pair_recv,
    trade_send,
    trade_recv,
    share_send,
    share_recv,
    dq_send,
    dq_recv,
    dq_direct_send,
    dq_direct_recv,
    dq_relay_send,
    dq_relay_recv,
    late_send,
    late_recv,
    core_send,
    core_recv,
    chip_send,
    chip_recv,
    last_send,
    last_recv,
    made_send,
    made_recv,
    land_send,
    land_recv,
):
    me = Place()
    chips, chip, core, seat, group = me.chips, me.chip, me.core, me.seat, me.group
    heads, depth, width = query_ref.shape
    tokens = input_ref.shape[0]
    window = tokens * me.ctx_count
    half = 2 * depth
    piece = half // group
    family = me.head // group
    acts, sources = (input_ref, cotan_ref), (query_ref, output_ref)
    rows = tokens // SUBS
    part_rows = tokens // 2

    mine = span(core * depth, depth)
    loads = []
    for a in range(2):
        loads.append(local(sources[a], mats.at[a, :, mine], load_sem.at[a]))
        loads.append(local(acts[a].at[:, span(chip * half, half)], own.at[a], load_sem.at[2 + a]))

    places = me.friends()
    if group == 4:
        places.append((me.ctx, flip(flip(me.head, 1), 2)))
    homes = [lax.rem(family + i, chips) for i in range(1, chips)]
    places += [(me.ctx, home * group + seat) for home in homes]
    greet(places)

    order = [(a, hop, s) for a in range(2) for hop in range(1, chips) for s in range(SUBS)]

    def located(n, at):
        a, hop, s = order[n]
        return far.at[hop - 1, a, at, pl.ds(s * rows, rows)]

    crossing = []
    for n, (a, hop, s) in enumerate(order):
        begin = pl.multiple_of(me.other(hop) * half + seat * piece, piece)
        copy = remote(
            acts[a].at[pl.ds(s * rows, rows), pl.ds(begin, piece)],
            located(n, seat),
            x_send.at[n],
            x_recv.at[n],
            me.across(hop),
        )
        copy.start()
        crossing.append(copy)
    for copy in loads:
        copy.start()
    swaps = []
    for a in range(2):
        copy = remote(
            sources[a], mats.at[a, :, mine], weight_sem.at[a], weight_sem.at[2 + a], me.sibling
        )
        copy.start()
        swaps.append(copy)

    row = me.head % 2

    def key_block(which, at):
        return keys.at[which, span(at * tokens, tokens)]

    pair_copies = []
    for hop in range(1, chips):
        copy = remote(
            pair_ref.at[0],
            key_block(row, me.ctx),
            pair_send.at[hop],
            pair_recv.at[hop],
            me.across(hop),
        )
        copy.start()
        pair_copies.append(copy)
    keep = local(pair_ref.at[0], key_block(row, me.ctx), load_sem.at[4])
    keep.start()

    spread = Spread(me, located, len(order), (direct_send, direct_recv, relay_send, relay_recv))

    def own_slice(a, i):
        part = pl.ds(i * piece, piece)
        contract(own.at[a, :, part], mats.at[a, :, part], own_sum.at[a], i == 0)

    seats = [seat] + [flip(seat, 1)] * (group > 1)
    if group == 4:
        seats += [flip(seat, 2), flip(flip(seat, 1), 2)]
    sums = {}

    def far_part(a, hop, p):
        block = pl.ds(p * part_rows, part_rows)
        for n, (b, by, s) in enumerate(order):
            if (b, by) == (a, hop) and s // (SUBS // 2) == p:
                spread.arrive(n)
        for i, at in enumerate(seats):
            part = span(at * piece, piece)
            contract(
                far.at[hop - 1, a, at, block],
                mats.at[a, :, part],
                far_sum.at[hop - 1, a, block],
                i == 0,
            )
        if a == 0:
            source, target = far_sum.at[hop - 1, 0, block], q_got.at[hop - 1, block]
        else:
            da_low[hop - 1, block] = far_sum[hop - 1, 1, block].astype(BF16)
            source, target = da_low.at[hop - 1, block], da_got.at[hop - 1, block]
        copy = remote(
            source,
            target,
            sum_send.at[a, hop - 1, p],
            sum_recv.at[a, hop - 1, p],
            (me.source(hop) * 2 + core, me.head),
        )
        copy.start()
        sums[a, hop, p] = copy

    own_work = [(a, i) for a in range(2) for i in range(group)]
    count = len(order)
    for n in range(count):
        crossing[n].wait_recv()
        spread.start(n)
        if n >= 1:
            spread.pass_on(n - 1)
        if n == 1:
            for copy in loads:
                copy.wait()
            for copy in swaps:
                copy.wait_recv()
        if n >= 2 and own_work:
            own_slice(*own_work.pop(0))
        if chips == 2 and n == count - 3:
            far_part(0, 1, 0)
    spread.pass_on(count - 1)

    part_columns = piece // 2
    ours = span(core * part_columns, part_columns)
    trades = []

    def seat_of(j):
        at = seat + 0
        for bit in (1, 2):
            if j & bit:
                at = flip(at, bit)
        return at

    for j in range(1, group):
        to = seat_of(j)
        copy = remote(
            mats.at[0, :, span(to * piece + core * part_columns, part_columns)],
            group_mats.at[seat, :, ours],
            trade_send.at[j],
            trade_recv.at[j],
            (me.ctx, me.head - seat + to),
        )
        copy.start()
        trades.append((j, copy))
    store = local(mats.at[0, :, span(seat * piece, piece)], group_mats.at[seat], load_sem.at[5])
    store.start()

    keep.wait()
    for copy in pair_copies:
        copy.wait_recv()
    pair_next = []
    for hop in range(chips):
        block = key_block(row, me.source(hop) * 2 + core)
        copy = remote(
            block, block, pair_send.at[chips + hop], pair_recv.at[chips + hop], me.beside(1)
        )
        copy.start()
        pair_next.append(copy)

    for work in own_work:
        own_slice(*work)
    for a in range(2):
        for p in range(2):
            for hop in range(1, chips):
                if (a, hop, p) not in sums:
                    far_part(a, hop, p)

    for copy in pair_next:
        copy.wait_recv()
    pair_last = []
    for hop in range(chips):
        for which in range(2):
            block = key_block(which, me.source(hop) * 2 + core)
            k = 2 * chips + 2 * hop + which
            copy = remote(block, block, pair_send.at[k], pair_recv.at[k], me.sibling)
            copy.start()
            pair_last.append(copy)

    lanes = []
    for j in range(heads - 1):
        named = route_ref[...] == me.head * (heads - 1) + j
        lanes.append(jnp.sum(jnp.where(named, gate_ref[...], 0.0), axis=0, keepdims=True))
    lanes.append(jnp.ones_like(lanes[0]))
    lanes += [jnp.zeros_like(lanes[0])] * (-heads % 8)
    token_gate = jnp.transpose(jnp.concatenate(lanes, axis=0))

    for hop in range(1, chips):
        for p in range(2):
            sums[0, hop, p].wait_recv()
    for j in range(heads):
        columns = pl.ds(j * width, width)
        value = own_sum[0, :, columns]
        for hop in range(1, chips):
            value = value + q_got[hop - 1, :, columns]
        queries[j] = value.astype(BF16)
    for copy in pair_last:
        copy.wait_recv()
    for which in range(2):
        for at in range(me.ctx_count):
            block = pl.ds(at * tokens, tokens)
            turned[which, :, block] = jnp.transpose(keys[which, block])
    for hop in range(1, chips):
        for p in range(2):
            sums[1, hop, p].wait_recv()
    for j in range(heads):
        columns = pl.ds(j * width, width)
        value = own_sum[1, :, columns]
        for hop in range(1, chips):
            value = value + da_got[hop - 1, :, columns].astype(F32)
        if j < heads - 1:
            value = value * token_gate[:, j : j + 1]
        cotans[j] = value.astype(BF16)

    late = 2 * heads // 5 if group == 4 else 0
    soon = heads - late
    units = [(0, j) for j in range(soon, heads)] + [(0, j) for j in range(soon)]
    units += [(hop, j) for hop in range(1, chips) for j in range(soon)]

    def unit(n, at):
        hop, j = units[n]
        return every.at[me.source(hop), at, j]

    dq_spread = Spread(
        me, unit, len(units), (dq_direct_send, dq_direct_recv, dq_relay_send, dq_relay_recv)
    )
    block_rows = min(tokens, max(16, 256 * 1024 // window))
    scale = width ** (-0.5)
    turned_grads[...] = jnp.zeros(turned_grads.shape, F32)

    def attend(j):
        def body(i, carry):
            block = span(i * block_rows, block_rows)
            query, cotan = queries[j, block], cotans[j, block]
            scores = jnp.dot(query, turned[0], preferred_element_type=F32) * scale
            first = me.ctx * tokens + i * block_rows
            place = first + lax.broadcasted_iota(jnp.int32, scores.shape, 0)
            scores = jnp.where(
                lax.broadcasted_iota(jnp.int32, scores.shape, 1) <= place, scores, -1e30
            )
            raised = jnp.exp(scores - jnp.max(scores, axis=1, keepdims=True))
            shares = raised / jnp.sum(raised, axis=1, keepdims=True)
            low = shares.astype(BF16)
            outputs = jnp.dot(low, keys[1], preferred_element_type=F32)
            share_grad = jnp.dot(cotan, turned[1], preferred_element_type=F32)
            delta = jnp.sum(cotan.astype(F32) * outputs, axis=1, keepdims=True)
            score_grad = (shares * (share_grad - delta) * scale).astype(BF16)
            every[chip, seat, j, block] = jnp.dot(
                score_grad, keys[0], preferred_element_type=F32
            ).astype(BF16)
            turned_grads[0] += jnp.dot(
                jnp.transpose(query), score_grad, preferred_element_type=F32
            )
            turned_grads[1] += jnp.dot(jnp.transpose(cotan), low, preferred_element_type=F32)
            return carry

        lax.fori_loop(0, tokens // block_rows, body, 0)

    dq_copies, late_copies = {}, []

    def late_send_on(j, k):
        for hop in range(1, chips):
            block = every.at[chip, seats[k], j]
            n = ((hop - 1) * late + j - soon) * group + k
            copy = remote(block, block, late_send.at[n], late_recv.at[n], me.across(hop))
            copy.start()
            late_copies.append(copy)

    for n in range(heads):
        j = units[n][1]
        attend(j)
        if j >= soon:
            late_send_on(j, 0)
        else:
            for hop in range(1, chips):
                m = units.index((hop, j))
                block = every.at[chip, seat, j]
                copy = remote(block, block, dq_send.at[m], dq_recv.at[m], me.across(hop))
                copy.start()
                dq_copies[m] = copy
        dq_spread.start(n)

    def column(at):
        return span(at * tokens, tokens)

    core_copies = []
    for hop in range(chips):
        spot = me.source(hop) * 2
        copy = remote(
            turned_grads.at[:, :, column(spot + 1 - core)],
            core_got.at[me.source(hop)],
            core_send.at[hop],
            core_recv.at[hop],
            me.sibling,
        )
        copy.start()
        core_copies.append(copy)
    kept_out[...] = jnp.zeros(kept_out.shape, F32)
    pair_low[...] = jnp.zeros(pair_low.shape, F32)
    for hop in range(chips):
        core_copies[hop].wait_recv()
        for which in range(2):
            both = (
                turned_grads[which, :, column(me.source(hop) * 2 + core)]
                + core_got[me.source(hop), which]
            )
            if hop:
                grads_low[hop - 1, which] = jnp.transpose(both).astype(BF16)
            else:
                kept_out[0] = jnp.where(row == which, jnp.transpose(both), kept_out[0])
                pair_low[...] = jnp.where(row == which, pair_low[...], jnp.transpose(both))
    chip_copies = []
    for hop in range(1, chips):
        copy = remote(
            grads_low.at[hop - 1],
            chip_got.at[hop - 1],
            chip_send.at[hop - 1],
            chip_recv.at[hop - 1],
            (me.source(hop) * 2 + core, me.head),
        )
        copy.start()
        chip_copies.append(copy)

    for n in range(late):
        dq_spread.pass_on(n)
    for n in range(heads, len(units)):
        dq_copies[n].wait_recv()
        dq_spread.start(n)
    for n in range(late, heads):
        dq_spread.pass_on(n)
    for n in range(late):
        dq_spread.arrive(n)
        for k in range(1, group):
            late_send_on(units[n][1], k)
    for n in range(heads, len(units)):
        dq_spread.pass_on(n)

    for hop in range(1, chips):
        chip_copies[hop - 1].wait_recv()
        for which in range(2):
            value = chip_got[hop - 1, which].astype(F32)
            kept_out[0] += jnp.where(row == which, value, 0.0)
            pair_low[...] += jnp.where(row == which, 0.0, value)
    last_low = grads_low.at[chips - 1, 0]
    last_low[...] = pair_low[...].astype(BF16)
    last = remote(last_low, pair_got, last_send.at[0], last_recv.at[0], me.beside(1))
    last.start()

    shares = []
    for j, copy in trades:
        copy.wait_recv()
        block = group_mats.at[seat_of(j), :, ours]
        share = remote(block, block, share_send.at[j], share_recv.at[j], me.sibling)
        share.start()
        shares.append(share)
    store.wait()
    for copy in shares:
        copy.wait_recv()

    chunks, chunk = made.shape[1], made.shape[3]
    flat = [(m, j) for m in range(group) for j in range(heads)]

    def made_copy(hop, i):
        return remote(
            made.at[hop - 1, i],
            hub.at[chips - hop, i],
            made_send.at[hop - 1, i],
            made_recv.at[chips - hop - 1, i],
            (me.source(hop) * 2 + core, me.head),
        )

    def land_copy(hop, i):
        return remote(
            hub.at[hop, i],
            land.at[family, i],
            land_send.at[hop, i],
            land_recv.at[family, i],
            (me.ctx, me.source(hop) * group + seat),
        )

    def moves(hop):
        return me.source(hop) != family

    def multiply(hop):
        at = me.source(hop)
        result = made.at[hop - 1] if hop else hub.at[0]

        def body(i, carry):
            part = span(i * chunk, chunk)
            total = jnp.zeros((tokens, chunk), F32)
            for k in range(0, len(flat), 2):
                both = flat[k : k + 2]
                left = jnp.concatenate([every[at, m, j] for m, j in both], axis=1)
                right = jnp.concatenate([group_mats[m, j, part] for m, j in both], axis=1)
                total += lax.dot_general(
                    left, right, (((1,), (1,)), ((), ())), preferred_element_type=F32
                )
            result[i] = total.astype(BF16)
            if hop:
                made_copy(hop, i).start()
            else:
                pl.when(moves(0))(land_copy(0, i).start)
            return carry

        lax.fori_loop(0, chunks, body, 0)

    for hop in range(chips):
        for n, (by, j) in enumerate(units):
            if by == hop and n >= late:
                dq_spread.arrive(n)
        if hop == 1:
            for copy in late_copies:
                copy.wait_recv()
        multiply(hop)
    for hop in range(1, chips):
        for i in range(chunks):
            made_copy(chips - hop, i).wait_recv()
            pl.when(moves(hop))(land_copy(hop, i).start)

    last.wait()
    kept_out[0] += pair_got[...].astype(F32)

    stay = lax.rem(chip - family + chips, chips)
    for i in range(chunks):
        total = hub[stay, i].astype(F32)
        for home in homes:
            arrival = remote(
                hub.at[0, i], land.at[home, i], land_send.at[0, i], land_recv.at[home, i], me.sibling
            )
            arrival.wait_recv()
            total = total + land[home, i].astype(F32)
        input_grad_out[:, pl.ds(i * chunk, chunk)] = total.astype(BF16)

    for hop in range(chips):
        for i in range(chunks):
            if hop:
                made_copy(hop, i).wait_send()
            pl.when(moves(hop))(land_copy(hop, i).wait_send)
    for copy in crossing + swaps + pair_copies + pair_next + pair_last + shares:
        copy.wait_send()
    for copy in core_copies + chip_copies:
        copy.wait_send()
    for copy in list(sums.values()) + list(dq_copies.values()) + late_copies:
        copy.wait_send()
    for j, copy in trades:
        copy.wait_send()
    spread.finish()
    dq_spread.finish()


def per_device(
    layer_input, output_grad, routes, route_gates, query_weight, output_weight, key_values
):
    ctx_count, head_count = lax.axis_size("ctx"), lax.axis_size("head")
    chips = ctx_count // 2
    group, hops = head_count // chips, chips - 1
    heads, depth, width = query_weight.shape
    tokens = layer_input.shape[0]
    half = 2 * depth
    piece = half // group
    window = tokens * ctx_count
    count, units = 2 * hops * SUBS, chips * heads
    chunk = min(256, piece)
    chunks = piece // chunk
    return pl.pallas_call(
        layer_kernel,
        out_shape=(
            jax.ShapeDtypeStruct((tokens, piece), BF16),
            jax.ShapeDtypeStruct((1, tokens, width), F32),
        ),
        in_specs=[ANY, ANY, VMEM, VMEM, ANY, ANY, VMEM],
        out_specs=(VMEM, VMEM),
        scratch_shapes=[
            pltpu.VMEM((2, heads, half, width), BF16),
            pltpu.VMEM((2, tokens, half), BF16),
            pltpu.VMEM((hops, 2, group, tokens, piece), BF16),
            pltpu.VMEM((2, tokens, heads * width), F32),
            pltpu.VMEM((hops, 2, tokens, heads * width), F32),
            pltpu.VMEM((hops, tokens, heads * width), F32),
            pltpu.VMEM((hops, tokens, heads * width), BF16),
            pltpu.VMEM((hops, tokens, heads * width), BF16),
            pltpu.VMEM((heads, tokens, width), BF16),
            pltpu.VMEM((heads, tokens, width), BF16),
            pltpu.VMEM((group, heads, piece, width), BF16),
            pltpu.VMEM((2, window, width), BF16),
            pltpu.VMEM((2, width, window), BF16),
            pltpu.VMEM((2, width, window), F32),
            pltpu.VMEM((chips, 2, width, tokens), F32),
            pltpu.VMEM((chips, 2, tokens, width), BF16),
            pltpu.VMEM((hops, 2, tokens, width), BF16),
            pltpu.VMEM((tokens, width), F32),
            pltpu.VMEM((tokens, width), BF16),
            pltpu.VMEM((chips, group, heads, tokens, width), BF16),
            pltpu.VMEM((hops, chunks, tokens, chunk), BF16),
            pltpu.VMEM((chips, chunks, tokens, chunk), BF16),
            pltpu.VMEM((chips, chunks, tokens, chunk), BF16),
            DMA((6,)),
            DMA((4,)),
            DMA((count,)),
            DMA((count,)),
        ]
        + Spread.sems(count)
        + [DMA((2, hops, 2))] * 2
        + [DMA((4 * chips,))] * 2
        + [DMA((group,))] * 4
        + [DMA((units,))] * 2
        + Spread.sems(units)
        + [DMA((hops * heads * group,))] * 2
        + [DMA((chips,))] * 4
        + [DMA((1,))] * 2
        + [DMA((hops, chunks))] * 2
        + [DMA((chips, chunks))] * 2,
        compiler_params=pltpu.CompilerParams(
            collective_id=0, has_side_effects=True, vmem_limit_bytes=VMEM_BYTES
        ),
    )(
        layer_input,
        output_grad,
        routes.T,
        route_gates.T,
        query_weight,
        output_weight,
        key_values,
    )


def solution(mesh):
    in_specs = (
        P("ctx", None),
        P("ctx", None),
        P("ctx", None),
        P("ctx", None),
        P("head", "ctx", None),
        P("head", "ctx", None),
        P("head", "ctx", None),
    )
    out_specs = (P("ctx", "head"), P("head", "ctx", None))
    return jax.shard_map(
        per_device, mesh=mesh, in_specs=in_specs, out_specs=out_specs, check_vma=False
    )
```

```python
import functools

import jax
import jax.numpy as jnp
from jax import lax
from jax.experimental import pallas as pl
from jax.experimental.pallas import tpu as pltpu
from jax.sharding import PartitionSpec as P

MESH = pl.DeviceIdType.MESH
ANY = pl.BlockSpec(memory_space=pl.ANY)
VMEM = pl.BlockSpec(memory_space=pltpu.VMEM)
DMA = pltpu.SemaphoreType.DMA
F32, BF16 = jnp.float32, jnp.bfloat16
SUBS = 4
VMEM_BYTES = 67_043_328


def remote(source, target, send, recv, place):
    return pltpu.make_async_remote_copy(
        src_ref=source,
        dst_ref=target,
        send_sem=send,
        recv_sem=recv,
        device_id=place,
        device_id_type=MESH,
    )


def local(source, target, sem):
    return pltpu.make_async_copy(source, target, sem)


def greet(places):
    barrier = pltpu.get_barrier_semaphore()
    for place in places:
        pl.semaphore_signal(barrier, inc=1, device_id=place, device_id_type=MESH)
    pl.semaphore_wait(barrier, len(places))


def flip(index, bit):
    return index + bit - 2 * bit * ((index // bit) % 2)


def span(start, size):
    return pl.ds(pl.multiple_of(start, size), size)


def pairs(count):
    return [tuple(range(j, min(j + 2, count))) for j in range(0, count, 2)]


class Place:
    def __init__(self):
        self.ctx_count, self.head_count = lax.axis_size("ctx"), lax.axis_size("head")
        self.ctx, self.head = lax.axis_index("ctx"), lax.axis_index("head")
        self.chips = self.ctx_count // 2
        self.chip, self.core = self.ctx // 2, self.ctx % 2
        self.group = self.head_count // self.chips
        self.seat = self.head % self.group
        self.bits = [bit for bit in (1, 2) if bit < self.group]
        self.sibling = (self.ctx + 1 - 2 * self.core, self.head)

    def other(self, hop):
        return lax.rem(self.chip + hop, self.chips)

    def source(self, hop):
        return lax.rem(self.chip - hop + self.chips, self.chips)

    def across(self, hop):
        return (self.other(hop) * 2 + self.core, self.head)

    def beside(self, bit):
        return (self.ctx, flip(self.head, bit))

    def friends(self):
        hops = [self.across(hop) for hop in range(1, self.chips)]
        return hops + [self.beside(bit) for bit in self.bits] + [self.sibling]


class Spread:
    def __init__(self, place, located, count, sems):
        self.place, self.located, self.count = place, located, count
        self.direct_send, self.direct_recv, self.relay_send, self.relay_recv = sems
        self.direct, self.relay = {}, {}

    @staticmethod
    def sems(count):
        return [DMA((2, count))] * 2 + [DMA((count,))] * 2

    def start(self, n):
        for i, bit in enumerate(self.place.bits):
            block = self.located(n, self.place.seat)
            copy = remote(
                block,
                block,
                self.direct_send.at[i, n],
                self.direct_recv.at[i, n],
                self.place.beside(bit),
            )
            copy.start()
            self.direct[n, bit] = copy

    def pass_on(self, n):
        if len(self.place.bits) < 2:
            return
        came, onward = (2, 1) if n % 2 == 0 else (1, 2)
        self.direct[n, came].wait_recv()
        block = self.located(n, flip(self.place.seat, came))
        copy = remote(
            block, block, self.relay_send.at[n], self.relay_recv.at[n], self.place.beside(onward)
        )
        copy.start()
        self.relay[n] = copy

    def arrive(self, n):
        if len(self.place.bits) == 1:
            self.direct[n, 1].wait_recv()
        elif len(self.place.bits) == 2:
            self.direct[n, 1 if n % 2 == 0 else 2].wait_recv()
            self.relay[n].wait_recv()

    def finish(self):
        for copy in list(self.direct.values()) + list(self.relay.values()):
            copy.wait_send()


def contract(rows, weights, total, first):
    heads, depth, width = weights.shape
    step = min(512, depth)

    def body(i, carry):
        part = span(i * step, step)
        left = rows[:, part]
        for group in pairs(heads):
            right = jnp.concatenate([weights[j, part] for j in group], axis=1)
            columns = pl.ds(group[0] * width, len(group) * width)
            total[:, columns] += jnp.dot(left, right, preferred_element_type=F32)
        return carry

    if first:
        total[...] = jnp.zeros(total.shape, F32)
    lax.fori_loop(0, depth // step, body, 0)


def layer_kernel(
    input_ref,
    cotan_ref,
    route_ref,
    gate_ref,
    query_ref,
    output_ref,
    pair_ref,
    input_grad_out,
    kept_out,
    mats,
    own,
    far,
    own_sum,
    far_sum,
    q_got,
    da_low,
    da_got,
    queries,
    cotans,
    group_mats,
    keys,
    turned,
    turned_grads,
    core_got,
    grads_low,
    chip_got,
    pair_low,
    pair_got,
    every,
    made,
    hub,
    land,
    load_sem,
    weight_sem,
    x_send,
    x_recv,
    direct_send,
    direct_recv,
    relay_send,
    relay_recv,
    sum_send,
    sum_recv,
    pair_send,
    pair_recv,
    trade_send,
    trade_recv,
    early_send,
    early_recv,
    share_send,
    share_recv,
    dq_send,
    dq_recv,
    dq_direct_send,
    dq_direct_recv,
    dq_relay_send,
    dq_relay_recv,
    late_send,
    late_recv,
    core_send,
    core_recv,
    chip_send,
    chip_recv,
    last_send,
    last_recv,
    made_send,
    made_recv,
    land_send,
    land_recv,
):
    me = Place()
    chips, chip, core, seat, group = me.chips, me.chip, me.core, me.seat, me.group
    heads, depth, width = query_ref.shape
    tokens = input_ref.shape[0]
    window = tokens * me.ctx_count
    half = 2 * depth
    piece = half // group
    family = me.head // group
    acts, sources = (input_ref, cotan_ref), (query_ref, output_ref)
    rows = tokens // SUBS
    part_rows = tokens // 2

    mine = span(core * depth, depth)
    loads = []
    for a in range(2):
        loads.append(local(sources[a], mats.at[a, :, mine], load_sem.at[a]))
        loads.append(local(acts[a].at[:, span(chip * half, half)], own.at[a], load_sem.at[2 + a]))

    places = me.friends()
    if group == 4:
        places.append((me.ctx, flip(flip(me.head, 1), 2)))
    homes = [lax.rem(family + i, chips) for i in range(1, chips)]
    places += [(me.ctx, home * group + seat) for home in homes]
    greet(places)

    order = [(a, hop, s) for a in range(2) for hop in range(1, chips) for s in range(SUBS)]

    def located(n, at):
        a, hop, s = order[n]
        return far.at[hop - 1, a, at, pl.ds(s * rows, rows)]

    crossing = []
    for n, (a, hop, s) in enumerate(order):
        begin = pl.multiple_of(me.other(hop) * half + seat * piece, piece)
        copy = remote(
            acts[a].at[pl.ds(s * rows, rows), pl.ds(begin, piece)],
            located(n, seat),
            x_send.at[n],
            x_recv.at[n],
            me.across(hop),
        )
        copy.start()
        crossing.append(copy)
    for copy in loads:
        copy.start()
    swaps = []
    for a in range(2):
        copy = remote(
            sources[a], mats.at[a, :, mine], weight_sem.at[a], weight_sem.at[2 + a], me.sibling
        )
        copy.start()
        swaps.append(copy)

    row = me.head % 2

    def key_block(which, at):
        return keys.at[which, span(at * tokens, tokens)]

    pair_copies = []
    for hop in range(1, chips):
        copy = remote(
            pair_ref.at[0],
            key_block(row, me.ctx),
            pair_send.at[hop],
            pair_recv.at[hop],
            me.across(hop),
        )
        copy.start()
        pair_copies.append(copy)
    keep = local(pair_ref.at[0], key_block(row, me.ctx), load_sem.at[4])
    keep.start()

    early = 1 if group == 4 else 0
    holder = core == seat // 2

    def ahead(bit):
        to = flip(seat, bit)
        begin = pl.multiple_of(to * piece - core * depth, piece)
        return remote(
            query_ref.at[pl.ds(0, early), pl.ds(begin, piece)],
            group_mats.at[seat, pl.ds(0, early)],
            early_send.at[bit],
            early_recv.at[bit],
            me.beside(bit),
        )

    def came_ahead(bit):
        return remote(
            group_mats.at[seat, pl.ds(0, early)],
            group_mats.at[flip(seat, bit), pl.ds(0, early)],
            early_send.at[bit],
            early_recv.at[bit],
            me.beside(bit),
        )

    def share_ahead(bit):
        block = group_mats.at[flip(seat, bit), pl.ds(0, early)]
        return remote(
            block, block, early_send.at[2 + bit], early_recv.at[2 + bit], me.sibling
        )

    def when_ahead(action):
        if early:
            pl.when(holder)(lambda: action(1))
            pl.when(jnp.logical_not(holder))(lambda: action(2))

    when_ahead(lambda bit: ahead(bit).start())

    spread = Spread(me, located, len(order), (direct_send, direct_recv, relay_send, relay_recv))

    def own_slice(a, i):
        part = pl.ds(i * piece, piece)
        contract(own.at[a, :, part], mats.at[a, :, part], own_sum.at[a], i == 0)

    seats = [seat] + [flip(seat, 1)] * (group > 1)
    if group == 4:
        seats += [flip(seat, 2), flip(flip(seat, 1), 2)]
    sums = {}

    def far_part(a, hop, p):
        block = pl.ds(p * part_rows, part_rows)
        for n, (b, by, s) in enumerate(order):
            if (b, by) == (a, hop) and s // (SUBS // 2) == p:
                spread.arrive(n)
        for i, at in enumerate(seats):
            part = span(at * piece, piece)
            contract(
                far.at[hop - 1, a, at, block],
                mats.at[a, :, part],
                far_sum.at[hop - 1, a, block],
                i == 0,
            )
        if a == 0:
            source, target = far_sum.at[hop - 1, 0, block], q_got.at[hop - 1, block]
        else:
            da_low[hop - 1, block] = far_sum[hop - 1, 1, block].astype(BF16)
            source, target = da_low.at[hop - 1, block], da_got.at[hop - 1, block]
        copy = remote(
            source,
            target,
            sum_send.at[a, hop - 1, p],
            sum_recv.at[a, hop - 1, p],
            (me.source(hop) * 2 + core, me.head),
        )
        copy.start()
        sums[a, hop, p] = copy

    own_work = [(a, i) for a in range(2) for i in range(group)]
    count = len(order)
    for n in range(count):
        crossing[n].wait_recv()
        spread.start(n)
        if n >= 1:
            spread.pass_on(n - 1)
        if n == 1:
            for copy in loads:
                copy.wait()
            for copy in swaps:
                copy.wait_recv()
        if n >= 2 and own_work:
            own_slice(*own_work.pop(0))
        if chips == 2 and n == count - 3:
            far_part(0, 1, 0)
        if chips == 2 and n == count - 1:
            far_part(0, 1, 1)
    spread.pass_on(count - 1)

    keep.wait()
    for copy in pair_copies:
        copy.wait_recv()
    pair_next = []
    for hop in range(chips):
        block = key_block(row, me.source(hop) * 2 + core)
        copy = remote(
            block, block, pair_send.at[chips + hop], pair_recv.at[chips + hop], me.beside(1)
        )
        copy.start()
        pair_next.append(copy)

    part_columns = piece // 2
    ours = span(core * part_columns, part_columns)
    trades = []

    def seat_of(j):
        at = seat + 0
        for bit in (1, 2):
            if j & bit:
                at = flip(at, bit)
        return at

    for j in range(1, group):
        to = seat_of(j)
        later = pl.ds(early if j < 3 else 0, heads - (early if j < 3 else 0))
        copy = remote(
            mats.at[0, later, span(to * piece + core * part_columns, part_columns)],
            group_mats.at[seat, later, ours],
            trade_send.at[j],
            trade_recv.at[j],
            (me.ctx, me.head - seat + to),
        )
        copy.start()
        trades.append((j, later, copy))
    store = local(mats.at[0, :, span(seat * piece, piece)], group_mats.at[seat], load_sem.at[5])
    store.start()

    for work in own_work:
        own_slice(*work)
    for a in range(2):
        for p in range(2):
            for hop in range(1, chips):
                if (a, hop, p) not in sums:
                    far_part(a, hop, p)

    for copy in pair_next:
        copy.wait_recv()
    pair_last = []
    for hop in range(chips):
        for which in range(2):
            block = key_block(which, me.source(hop) * 2 + core)
            k = 2 * chips + 2 * hop + which
            copy = remote(block, block, pair_send.at[k], pair_recv.at[k], me.sibling)
            copy.start()
            pair_last.append(copy)

    lanes = []
    for j in range(heads - 1):
        named = route_ref[...] == me.head * (heads - 1) + j
        lanes.append(jnp.sum(jnp.where(named, gate_ref[...], 0.0), axis=0, keepdims=True))
    lanes.append(jnp.ones_like(lanes[0]))
    lanes += [jnp.zeros_like(lanes[0])] * (-heads % 8)
    token_gate = jnp.transpose(jnp.concatenate(lanes, axis=0))

    for hop in range(1, chips):
        for p in range(2):
            sums[0, hop, p].wait_recv()
    for j in range(heads):
        columns = pl.ds(j * width, width)
        value = own_sum[0, :, columns]
        for hop in range(1, chips):
            value = value + q_got[hop - 1, :, columns]
        queries[j] = value.astype(BF16)
    for copy in pair_last:
        copy.wait_recv()
    for which in range(2):
        for at in range(me.ctx_count):
            block = pl.ds(at * tokens, tokens)
            turned[which, :, block] = jnp.transpose(keys[which, block])
    for hop in range(1, chips):
        for p in range(2):
            sums[1, hop, p].wait_recv()
    for j in range(heads):
        columns = pl.ds(j * width, width)
        value = own_sum[1, :, columns]
        for hop in range(1, chips):
            value = value + da_got[hop - 1, :, columns].astype(F32)
        if j < heads - 1:
            value = value * token_gate[:, j : j + 1]
        cotans[j] = value.astype(BF16)

    late = 2 * heads // 5 if group == 4 else 0
    soon = heads - late
    parts = 2
    lines = tokens // parts
    units, late_units, soon_units, far_units = [], [], [], []
    for t in range(parts):
        at = len(units)
        units += [(t, 0, j) for j in list(range(soon, heads)) + list(range(soon))]
        units += [(t, hop, j) for hop in range(1, chips) for j in range(soon)]
        late_units.append(range(at, at + late))
        soon_units.append(range(at + late, at + heads))
        far_units.append(range(at + heads, len(units)))

    def unit(n, at):
        t, hop, j = units[n]
        return every.at[me.source(hop), at, j, pl.ds(t * lines, lines)]

    dq_spread = Spread(
        me, unit, len(units), (dq_direct_send, dq_direct_recv, dq_relay_send, dq_relay_recv)
    )
    block_rows = min(lines, max(16, 256 * 1024 // window))
    scale = width ** (-0.5)
    turned_grads[...] = jnp.zeros(turned_grads.shape, F32)

    def attend(t, j):
        def body(i, carry):
            i = t * (lines // block_rows) + i
            block = span(i * block_rows, block_rows)
            query, cotan = queries[j, block], cotans[j, block]
            scores = jnp.dot(query, turned[0], preferred_element_type=F32) * scale
            first = me.ctx * tokens + i * block_rows
            place = first + lax.broadcasted_iota(jnp.int32, scores.shape, 0)
            scores = jnp.where(
                lax.broadcasted_iota(jnp.int32, scores.shape, 1) <= place, scores, -1e30
            )
            raised = jnp.exp(scores - jnp.max(scores, axis=1, keepdims=True))
            shares = raised / jnp.sum(raised, axis=1, keepdims=True)
            low = shares.astype(BF16)
            outputs = jnp.dot(low, keys[1], preferred_element_type=F32)
            share_grad = jnp.dot(cotan, turned[1], preferred_element_type=F32)
            delta = jnp.sum(cotan.astype(F32) * outputs, axis=1, keepdims=True)
            score_grad = (shares * (share_grad - delta) * scale).astype(BF16)
            every[chip, seat, j, block] = jnp.dot(
                score_grad, keys[0], preferred_element_type=F32
            ).astype(BF16)
            turned_grads[0] += jnp.dot(
                jnp.transpose(query), score_grad, preferred_element_type=F32
            )
            turned_grads[1] += jnp.dot(jnp.transpose(cotan), low, preferred_element_type=F32)
            return carry

        lax.fori_loop(0, lines // block_rows, body, 0)

    dq_copies, late_copies = {}, []

    def late_send_on(n, k):
        for hop in range(1, chips):
            block = unit(n, seats[k])
            m = ((hop - 1) * len(units) + n) * group + k
            copy = remote(block, block, late_send.at[m], late_recv.at[m], me.across(hop))
            copy.start()
            late_copies.append((units[n][0], copy))

    for t in range(parts):
        for n in list(late_units[t]) + list(soon_units[t]):
            j = units[n][2]
            attend(t, j)
            if j >= soon:
                late_send_on(n, 0)
            else:
                for hop in range(1, chips):
                    m = units.index((t, hop, j))
                    block = unit(n, seat)
                    copy = remote(block, block, dq_send.at[m], dq_recv.at[m], me.across(hop))
                    copy.start()
                    dq_copies[m] = copy
            if t == 0:
                dq_spread.start(n)

    def column(at):
        return span(at * tokens, tokens)

    core_copies = []
    for hop in range(chips):
        spot = me.source(hop) * 2
        copy = remote(
            turned_grads.at[:, :, column(spot + 1 - core)],
            core_got.at[me.source(hop)],
            core_send.at[hop],
            core_recv.at[hop],
            me.sibling,
        )
        copy.start()
        core_copies.append(copy)
    kept_out[...] = jnp.zeros(kept_out.shape, F32)
    pair_low[...] = jnp.zeros(pair_low.shape, F32)
    for hop in range(chips):
        core_copies[hop].wait_recv()
        for which in range(2):
            both = (
                turned_grads[which, :, column(me.source(hop) * 2 + core)]
                + core_got[me.source(hop), which]
            )
            if hop:
                grads_low[hop - 1, which] = jnp.transpose(both).astype(BF16)
            else:
                kept_out[0] = jnp.where(row == which, jnp.transpose(both), kept_out[0])
                pair_low[...] = jnp.where(row == which, pair_low[...], jnp.transpose(both))
    chip_copies = []
    for hop in range(1, chips):
        copy = remote(
            grads_low.at[hop - 1],
            chip_got.at[hop - 1],
            chip_send.at[hop - 1],
            chip_recv.at[hop - 1],
            (me.source(hop) * 2 + core, me.head),
        )
        copy.start()
        chip_copies.append(copy)

    for n in far_units[0]:
        dq_copies[n].wait_recv()
        dq_spread.start(n)
    shares = []
    for j, later, copy in trades:
        copy.wait_recv()
        block = group_mats.at[seat_of(j), later, ours]
        share = remote(block, block, share_send.at[j], share_recv.at[j], me.sibling)
        share.start()
        shares.append(share)
    if early:

        @pl.when(holder)
        def _():
            for bit in (1, 2):
                came_ahead(bit).wait_recv()
                share_ahead(bit).start()

    for n in list(late_units[0]) + list(soon_units[0]):
        dq_spread.pass_on(n)
    for n in late_units[1]:
        dq_spread.start(n)
    for n in far_units[0]:
        dq_spread.pass_on(n)
    for n in soon_units[1]:
        dq_spread.start(n)
    for n in far_units[1]:
        dq_copies[n].wait_recv()
        dq_spread.start(n)
    for n in late_units[0]:
        dq_spread.arrive(n)
        for k in range(1, group):
            late_send_on(n, k)

    for hop in range(1, chips):
        chip_copies[hop - 1].wait_recv()
        for which in range(2):
            value = chip_got[hop - 1, which].astype(F32)
            kept_out[0] += jnp.where(row == which, value, 0.0)
            pair_low[...] += jnp.where(row == which, 0.0, value)
    last_low = grads_low.at[chips - 1, 0]
    last_low[...] = pair_low[...].astype(BF16)
    last = remote(last_low, pair_got, last_send.at[0], last_recv.at[0], me.beside(1))

    store.wait()
    for copy in shares:
        copy.wait_recv()
    if early:

        @pl.when(jnp.logical_not(holder))
        def _():
            for bit in (1, 2):
                share_ahead(bit).wait_recv()

    chunk = made.shape[3]
    chunks = piece // chunk
    flat = [(m, j) for m in range(group) for j in range(heads)]

    def made_copy(hop, i):
        return remote(
            made.at[hop - 1, i],
            hub.at[chips - hop, i],
            made_send.at[hop - 1, i],
            made_recv.at[chips - hop - 1, i],
            (me.source(hop) * 2 + core, me.head),
        )

    def land_copy(hop, i):
        return remote(
            hub.at[hop, i],
            land.at[family, i],
            land_send.at[hop, i],
            land_recv.at[family, i],
            (me.ctx, me.source(hop) * group + seat),
        )

    def moves(hop):
        return me.source(hop) != family

    def multiply(t, hop):
        at = me.source(hop)
        block = pl.ds(t * lines, lines)
        result = made.at[hop - 1] if hop else hub.at[0]

        def body(i, carry):
            part = span(i * chunk, chunk)
            total = jnp.zeros((lines, chunk), F32)
            i = t * chunks + i
            for k in range(0, len(flat), 2):
                both = flat[k : k + 2]
                left = jnp.concatenate([every[at, m, j, block] for m, j in both], axis=1)
                right = jnp.concatenate([group_mats[m, j, part] for m, j in both], axis=1)
                total += lax.dot_general(
                    left, right, (((1,), (1,)), ((), ())), preferred_element_type=F32
                )
            result[i] = total.astype(BF16)
            if hop:
                made_copy(hop, i).start()
            else:
                pl.when(moves(0))(land_copy(0, i).start)
            return carry

        lax.fori_loop(0, chunks, body, 0)

    def pass_made(t):
        for hop in range(1, chips):
            for i in range(t * chunks, (t + 1) * chunks):
                made_copy(chips - hop, i).wait_recv()
                pl.when(moves(hop))(land_copy(hop, i).start)

    def finish_part(t):
        for n in soon_units[t]:
            dq_spread.arrive(n)
        multiply(t, 0)
        for n in far_units[t]:
            dq_spread.arrive(n)
        for when, copy in late_copies:
            if when == t:
                copy.wait_recv()
        for hop in range(1, chips):
            multiply(t, hop)

    finish_part(0)
    for n in range(len(units) // parts, len(units)):
        dq_spread.pass_on(n)
    for n in late_units[1]:
        dq_spread.arrive(n)
        for k in range(1, group):
            late_send_on(n, k)
    last.start()
    pass_made(0)
    finish_part(1)
    pass_made(1)

    last.wait()
    kept_out[0] += pair_got[...].astype(F32)

    stay = lax.rem(chip - family + chips, chips)
    for i in range(parts * chunks):
        total = hub[stay, i].astype(F32)
        for home in homes:
            arrival = remote(
                hub.at[0, i], land.at[home, i], land_send.at[0, i], land_recv.at[home, i], me.sibling
            )
            arrival.wait_recv()
            total = total + land[home, i].astype(F32)
        block = pl.ds(i // chunks * lines, lines)
        input_grad_out[block, pl.ds(i % chunks * chunk, chunk)] = total.astype(BF16)

    for hop in range(chips):
        for i in range(parts * chunks):
            if hop:
                made_copy(hop, i).wait_send()
            pl.when(moves(hop))(land_copy(hop, i).wait_send)
    for copy in crossing + swaps + pair_copies + pair_next + pair_last + shares:
        copy.wait_send()
    for copy in core_copies + chip_copies:
        copy.wait_send()
    for copy in list(sums.values()) + list(dq_copies.values()):
        copy.wait_send()
    for _, copy in late_copies:
        copy.wait_send()
    for _, _, copy in trades:
        copy.wait_send()
    when_ahead(lambda bit: ahead(bit).wait_send())
    if early:

        @pl.when(holder)
        def _():
            for bit in (1, 2):
                share_ahead(bit).wait_send()

    spread.finish()
    dq_spread.finish()


def per_device(
    layer_input, output_grad, routes, route_gates, query_weight, output_weight, key_values
):
    ctx_count, head_count = lax.axis_size("ctx"), lax.axis_size("head")
    chips = ctx_count // 2
    group, hops = head_count // chips, chips - 1
    heads, depth, width = query_weight.shape
    tokens = layer_input.shape[0]
    half = 2 * depth
    piece = half // group
    window = tokens * ctx_count
    count, units = 2 * hops * SUBS, 2 * chips * heads
    chunk = min(512, piece)
    chunks = 2 * piece // chunk
    lines = tokens // 2
    return pl.pallas_call(
        layer_kernel,
        out_shape=(
            jax.ShapeDtypeStruct((tokens, piece), BF16),
            jax.ShapeDtypeStruct((1, tokens, width), F32),
        ),
        in_specs=[ANY, ANY, VMEM, VMEM, ANY, ANY, VMEM],
        out_specs=(VMEM, VMEM),
        scratch_shapes=[
            pltpu.VMEM((2, heads, half, width), BF16),
            pltpu.VMEM((2, tokens, half), BF16),
            pltpu.VMEM((hops, 2, group, tokens, piece), BF16),
            pltpu.VMEM((2, tokens, heads * width), F32),
            pltpu.VMEM((hops, 2, tokens, heads * width), F32),
            pltpu.VMEM((hops, tokens, heads * width), F32),
            pltpu.VMEM((hops, tokens, heads * width), BF16),
            pltpu.VMEM((hops, tokens, heads * width), BF16),
            pltpu.VMEM((heads, tokens, width), BF16),
            pltpu.VMEM((heads, tokens, width), BF16),
            pltpu.VMEM((group, heads, piece, width), BF16),
            pltpu.VMEM((2, window, width), BF16),
            pltpu.VMEM((2, width, window), BF16),
            pltpu.VMEM((2, width, window), F32),
            pltpu.VMEM((chips, 2, width, tokens), F32),
            pltpu.VMEM((chips, 2, tokens, width), BF16),
            pltpu.VMEM((hops, 2, tokens, width), BF16),
            pltpu.VMEM((tokens, width), F32),
            pltpu.VMEM((tokens, width), BF16),
            pltpu.VMEM((chips, group, heads, tokens, width), BF16),
            pltpu.VMEM((hops, chunks, lines, chunk), BF16),
            pltpu.VMEM((chips, chunks, lines, chunk), BF16),
            pltpu.VMEM((chips, chunks, lines, chunk), BF16),
            DMA((6,)),
            DMA((4,)),
            DMA((count,)),
            DMA((count,)),
        ]
        + Spread.sems(count)
        + [DMA((2, hops, 2))] * 2
        + [DMA((4 * chips,))] * 2
        + [DMA((group,))] * 2
        + [DMA((5,))] * 2
        + [DMA((group,))] * 2
        + [DMA((units,))] * 2
        + Spread.sems(units)
        + [DMA((hops * units * group,))] * 2
        + [DMA((chips,))] * 4
        + [DMA((1,))] * 2
        + [DMA((hops, chunks))] * 2
        + [DMA((chips, chunks))] * 2,
        compiler_params=pltpu.CompilerParams(
            collective_id=0, has_side_effects=True, vmem_limit_bytes=VMEM_BYTES
        ),
    )(
        layer_input,
        output_grad,
        routes.T,
        route_gates.T,
        query_weight,
        output_weight,
        key_values,
    )


def solution(mesh):
    in_specs = (
        P("ctx", None),
        P("ctx", None),
        P("ctx", None),
        P("ctx", None),
        P("head", "ctx", None),
        P("head", "ctx", None),
        P("head", "ctx", None),
    )
    out_specs = (P("ctx", "head"), P("head", "ctx", None))
    return jax.shard_map(
        per_device, mesh=mesh, in_specs=in_specs, out_specs=out_specs, check_vma=False
    )
```

```python
import functools

import jax
import jax.numpy as jnp
from jax import lax
from jax.experimental import pallas as pl
from jax.experimental.pallas import tpu as pltpu
from jax.sharding import PartitionSpec as P

MESH = pl.DeviceIdType.MESH
ANY = pl.BlockSpec(memory_space=pl.ANY)
VMEM = pl.BlockSpec(memory_space=pltpu.VMEM)
DMA = pltpu.SemaphoreType.DMA
F32, BF16 = jnp.float32, jnp.bfloat16
SUBS = 4
STRAIGHT = 2
VMEM_BYTES = 67_043_328


def remote(source, target, send, recv, place):
    return pltpu.make_async_remote_copy(
        src_ref=source,
        dst_ref=target,
        send_sem=send,
        recv_sem=recv,
        device_id=place,
        device_id_type=MESH,
    )


def local(source, target, sem):
    return pltpu.make_async_copy(source, target, sem)


def greet(places):
    barrier = pltpu.get_barrier_semaphore()
    for place in places:
        pl.semaphore_signal(barrier, inc=1, device_id=place, device_id_type=MESH)
    pl.semaphore_wait(barrier, len(places))


def flip(index, bit):
    return index + bit - 2 * bit * ((index // bit) % 2)


def span(start, size):
    return pl.ds(pl.multiple_of(start, size), size)


def part_count(chips):
    return 4 if chips <= 2 else 2


def pairs(count):
    return [tuple(range(j, min(j + 2, count))) for j in range(0, count, 2)]


class Place:
    def __init__(self):
        self.ctx_count, self.head_count = lax.axis_size("ctx"), lax.axis_size("head")
        self.ctx, self.head = lax.axis_index("ctx"), lax.axis_index("head")
        self.chips = self.ctx_count // 2
        self.chip, self.core = self.ctx // 2, self.ctx % 2
        self.group = self.head_count // self.chips
        self.seat = self.head % self.group
        self.bits = [bit for bit in (1, 2) if bit < self.group]
        self.sibling = (self.ctx + 1 - 2 * self.core, self.head)

    def other(self, hop):
        return lax.rem(self.chip + hop, self.chips)

    def source(self, hop):
        return lax.rem(self.chip - hop + self.chips, self.chips)

    def across(self, hop):
        return (self.other(hop) * 2 + self.core, self.head)

    def beside(self, bit):
        return (self.ctx, flip(self.head, bit))

    def friends(self):
        hops = [self.across(hop) for hop in range(1, self.chips)]
        return hops + [self.beside(bit) for bit in self.bits] + [self.sibling]


class Spread:
    def __init__(self, place, located, sems, straight=()):
        self.place, self.located = place, located
        self.straight = dict(straight)
        self.direct_send, self.direct_recv, self.relay_send, self.relay_recv = sems
        self.direct, self.relay = {}, {}

    @staticmethod
    def sems(count):
        return [DMA((2, count))] * 2 + [DMA((count,))] * 2

    def start(self, n):
        for i, bit in enumerate(self.place.bits):
            block = self.located(n, self.place.seat)
            copy = remote(
                block,
                block,
                self.direct_send.at[i, n],
                self.direct_recv.at[i, n],
                self.place.beside(bit),
            )
            copy.start()
            self.direct[n, bit] = copy

    def pass_on(self, n):
        if len(self.place.bits) < 2 or n in self.straight:
            return
        came, onward = (2, 1) if n % 2 == 0 else (1, 2)
        self.direct[n, came].wait_recv()
        block = self.located(n, flip(self.place.seat, came))
        copy = remote(
            block, block, self.relay_send.at[n], self.relay_recv.at[n], self.place.beside(onward)
        )
        copy.start()
        self.relay[n] = copy

    def arrive(self, n):
        if n in self.straight:
            for bit in self.place.bits:
                self.direct[n, bit].wait_recv()
            self.straight[n].wait_recv()
        elif len(self.place.bits) == 1:
            self.direct[n, 1].wait_recv()
        elif len(self.place.bits) == 2:
            self.direct[n, 1 if n % 2 == 0 else 2].wait_recv()
            self.relay[n].wait_recv()

    def finish(self):
        for copy in list(self.direct.values()) + list(self.relay.values()):
            copy.wait_send()


def contract(rows, weights, total, first):
    heads, depth, width = weights.shape
    step = min(512, depth)

    def body(i, carry):
        part = span(i * step, step)
        left = rows[:, part]
        for group in pairs(heads):
            right = jnp.concatenate([weights[j, part] for j in group], axis=1)
            columns = pl.ds(group[0] * width, len(group) * width)
            total[:, columns] += jnp.dot(left, right, preferred_element_type=F32)
        return carry

    if first:
        total[...] = jnp.zeros(total.shape, F32)
    lax.fori_loop(0, depth // step, body, 0)


def layer_kernel(
    input_ref,
    cotan_ref,
    route_ref,
    gate_ref,
    query_ref,
    output_ref,
    pair_ref,
    input_grad_out,
    kept_out,
    mats,
    own,
    far,
    own_sum,
    far_sum,
    q_got,
    da_low,
    da_got,
    queries,
    cotans,
    group_mats,
    keys,
    turned,
    turned_grads,
    core_got,
    grads_low,
    chip_got,
    pair_low,
    pair_got,
    every,
    made,
    hub,
    land,
    load_sem,
    weight_sem,
    x_send,
    x_recv,
    straight_send,
    straight_recv,
    direct_send,
    direct_recv,
    relay_send,
    relay_recv,
    sum_send,
    sum_recv,
    pair_send,
    pair_recv,
    trade_send,
    trade_recv,
    early_send,
    early_recv,
    share_send,
    share_recv,
    dq_send,
    dq_recv,
    dq_direct_send,
    dq_direct_recv,
    dq_relay_send,
    dq_relay_recv,
    late_send,
    late_recv,
    core_send,
    core_recv,
    chip_send,
    chip_recv,
    last_send,
    last_recv,
    made_send,
    made_recv,
    land_send,
    land_recv,
):
    me = Place()
    chips, chip, core, seat, group = me.chips, me.chip, me.core, me.seat, me.group
    heads, depth, width = query_ref.shape
    tokens = input_ref.shape[0]
    window = tokens * me.ctx_count
    half = 2 * depth
    piece = half // group
    family = me.head // group
    acts, sources = (input_ref, cotan_ref), (query_ref, output_ref)
    rows = tokens // SUBS
    part_rows = tokens // 2

    mine = span(core * depth, depth)
    loads = []
    for a in range(2):
        loads.append(local(sources[a], mats.at[a, :, mine], load_sem.at[a]))
        loads.append(local(acts[a].at[:, span(chip * half, half)], own.at[a], load_sem.at[2 + a]))

    places = me.friends()
    if group == 4:
        places.append((me.ctx, flip(flip(me.head, 1), 2)))
    homes = [lax.rem(family + i, chips) for i in range(1, chips)]
    places += [(me.ctx, home * group + seat) for home in homes]
    greet(places)

    order = [(a, hop, s) for a in range(2) for hop in range(1, chips) for s in range(SUBS)]

    def located(n, at):
        a, hop, s = order[n]
        return far.at[hop - 1, a, at, pl.ds(s * rows, rows)]

    crossing = []
    for n, (a, hop, s) in enumerate(order):
        begin = pl.multiple_of(me.other(hop) * half + seat * piece, piece)
        copy = remote(
            acts[a].at[pl.ds(s * rows, rows), pl.ds(begin, piece)],
            located(n, seat),
            x_send.at[n],
            x_recv.at[n],
            me.across(hop),
        )
        copy.start()
        crossing.append(copy)
    straight = {}
    for n, (a, hop, s) in enumerate(order):
        if group == 4 and a == 1 and s >= SUBS - STRAIGHT:
            at = flip(flip(seat, 1), 2)
            begin = pl.multiple_of(me.other(hop) * half + at * piece, piece)
            copy = remote(
                acts[a].at[pl.ds(s * rows, rows), pl.ds(begin, piece)],
                located(n, at),
                straight_send.at[n],
                straight_recv.at[n],
                me.across(hop),
            )
            copy.start()
            straight[n] = copy
    for copy in loads:
        copy.start()
    swaps = []
    for a in range(2):
        copy = remote(
            sources[a], mats.at[a, :, mine], weight_sem.at[a], weight_sem.at[2 + a], me.sibling
        )
        copy.start()
        swaps.append(copy)

    row = me.head % 2

    def key_block(which, at):
        return keys.at[which, span(at * tokens, tokens)]

    pair_copies = []
    for hop in range(1, chips):
        copy = remote(
            pair_ref.at[0],
            key_block(row, me.ctx),
            pair_send.at[hop],
            pair_recv.at[hop],
            me.across(hop),
        )
        copy.start()
        pair_copies.append(copy)
    keep = local(pair_ref.at[0], key_block(row, me.ctx), load_sem.at[4])
    keep.start()

    early = 1 if group == 4 else 0
    holder = core == seat // 2

    def ahead(bit):
        to = flip(seat, bit)
        begin = pl.multiple_of(to * piece - core * depth, piece)
        return remote(
            query_ref.at[pl.ds(0, early), pl.ds(begin, piece)],
            group_mats.at[seat, pl.ds(0, early)],
            early_send.at[bit],
            early_recv.at[bit],
            me.beside(bit),
        )

    def came_ahead(bit):
        return remote(
            group_mats.at[seat, pl.ds(0, early)],
            group_mats.at[flip(seat, bit), pl.ds(0, early)],
            early_send.at[bit],
            early_recv.at[bit],
            me.beside(bit),
        )

    def share_ahead(bit):
        block = group_mats.at[flip(seat, bit), pl.ds(0, early)]
        return remote(
            block, block, early_send.at[2 + bit], early_recv.at[2 + bit], me.sibling
        )

    def when_ahead(action):
        if early:
            pl.when(holder)(lambda: action(1))
            pl.when(jnp.logical_not(holder))(lambda: action(2))

    when_ahead(lambda bit: ahead(bit).start())

    spread = Spread(
        me, located, (direct_send, direct_recv, relay_send, relay_recv), straight.items()
    )

    def own_slice(a, i):
        part = pl.ds(i * piece, piece)
        contract(own.at[a, :, part], mats.at[a, :, part], own_sum.at[a], i == 0)

    seats = [seat] + [flip(seat, 1)] * (group > 1)
    if group == 4:
        seats += [flip(seat, 2), flip(flip(seat, 1), 2)]
    sums = {}

    def far_part(a, hop, p):
        block = pl.ds(p * part_rows, part_rows)
        for n, (b, by, s) in enumerate(order):
            if (b, by) == (a, hop) and s // (SUBS // 2) == p:
                spread.arrive(n)
        for i, at in enumerate(seats):
            part = span(at * piece, piece)
            contract(
                far.at[hop - 1, a, at, block],
                mats.at[a, :, part],
                far_sum.at[hop - 1, a, block],
                i == 0,
            )
        if a == 0:
            source, target = far_sum.at[hop - 1, 0, block], q_got.at[hop - 1, block]
        else:
            da_low[hop - 1, block] = far_sum[hop - 1, 1, block].astype(BF16)
            source, target = da_low.at[hop - 1, block], da_got.at[hop - 1, block]
        copy = remote(
            source,
            target,
            sum_send.at[a, hop - 1, p],
            sum_recv.at[a, hop - 1, p],
            (me.source(hop) * 2 + core, me.head),
        )
        copy.start()
        sums[a, hop, p] = copy

    own_work = [(a, i) for a in range(2) for i in range(group)]
    count = len(order)
    for n in range(count):
        crossing[n].wait_recv()
        spread.start(n)
        if n >= 1:
            spread.pass_on(n - 1)
        if n == 1:
            for copy in loads:
                copy.wait()
            for copy in swaps:
                copy.wait_recv()
        if n >= 2 and own_work:
            own_slice(*own_work.pop(0))
        if chips == 2 and n == count - 3:
            far_part(0, 1, 0)
        if chips == 2 and n == count - 1:
            far_part(0, 1, 1)
    spread.pass_on(count - 1)

    keep.wait()
    for copy in pair_copies:
        copy.wait_recv()
    pair_next = []
    for hop in range(chips):
        block = key_block(row, me.source(hop) * 2 + core)
        copy = remote(
            block, block, pair_send.at[chips + hop], pair_recv.at[chips + hop], me.beside(1)
        )
        copy.start()
        pair_next.append(copy)

    part_columns = piece // 2
    ours = span(core * part_columns, part_columns)
    trades = []

    def seat_of(j):
        at = seat + 0
        for bit in (1, 2):
            if j & bit:
                at = flip(at, bit)
        return at

    for j in range(1, group):
        to = seat_of(j)
        later = pl.ds(early if j < 3 else 0, heads - (early if j < 3 else 0))
        copy = remote(
            mats.at[0, later, span(to * piece + core * part_columns, part_columns)],
            group_mats.at[seat, later, ours],
            trade_send.at[j],
            trade_recv.at[j],
            (me.ctx, me.head - seat + to),
        )
        copy.start()
        trades.append((j, later, copy))
    store = local(mats.at[0, :, span(seat * piece, piece)], group_mats.at[seat], load_sem.at[5])
    store.start()

    for work in own_work:
        own_slice(*work)
    for a in range(2):
        for p in range(2):
            for hop in range(1, chips):
                if (a, hop, p) not in sums:
                    far_part(a, hop, p)

    for copy in pair_next:
        copy.wait_recv()
    pair_last = []
    for hop in range(chips):
        for which in range(2):
            block = key_block(which, me.source(hop) * 2 + core)
            k = 2 * chips + 2 * hop + which
            copy = remote(block, block, pair_send.at[k], pair_recv.at[k], me.sibling)
            copy.start()
            pair_last.append(copy)

    lanes = []
    for j in range(heads - 1):
        named = route_ref[...] == me.head * (heads - 1) + j
        lanes.append(jnp.sum(jnp.where(named, gate_ref[...], 0.0), axis=0, keepdims=True))
    lanes.append(jnp.ones_like(lanes[0]))
    lanes += [jnp.zeros_like(lanes[0])] * (-heads % 8)
    token_gate = jnp.transpose(jnp.concatenate(lanes, axis=0))

    for hop in range(1, chips):
        for p in range(2):
            sums[0, hop, p].wait_recv()
    for j in range(heads):
        columns = pl.ds(j * width, width)
        value = own_sum[0, :, columns]
        for hop in range(1, chips):
            value = value + q_got[hop - 1, :, columns]
        queries[j] = value.astype(BF16)
    for copy in pair_last:
        copy.wait_recv()
    for which in range(2):
        for at in range(me.ctx_count):
            block = pl.ds(at * tokens, tokens)
            turned[which, :, block] = jnp.transpose(keys[which, block])
    for hop in range(1, chips):
        for p in range(2):
            sums[1, hop, p].wait_recv()
    for j in range(heads):
        columns = pl.ds(j * width, width)
        value = own_sum[1, :, columns]
        for hop in range(1, chips):
            value = value + da_got[hop - 1, :, columns].astype(F32)
        if j < heads - 1:
            value = value * token_gate[:, j : j + 1]
        cotans[j] = value.astype(BF16)

    late = 2 * heads // 5 if group == 4 else 0
    soon = heads - late
    parts = part_count(chips)
    lines = tokens // parts
    units, late_units, soon_units, far_units = [], [], [], []
    for t in range(parts):
        at = len(units)
        units += [(t, 0, j) for j in list(range(soon, heads)) + list(range(soon))]
        units += [(t, hop, j) for hop in range(1, chips) for j in range(soon)]
        late_units.append(range(at, at + late))
        soon_units.append(range(at + late, at + heads))
        far_units.append(range(at + heads, len(units)))

    def unit(n, at):
        t, hop, j = units[n]
        return every.at[me.source(hop), at, j, pl.ds(t * lines, lines)]

    dq_spread = Spread(
        me, unit, (dq_direct_send, dq_direct_recv, dq_relay_send, dq_relay_recv)
    )
    block_rows = min(part_rows, max(16, 256 * 1024 // window))
    scale = width ** (-0.5)
    turned_grads[...] = jnp.zeros(turned_grads.shape, F32)

    def attend(t, j):
        def body(i, carry):
            i = t * (part_rows // block_rows) + i
            block = span(i * block_rows, block_rows)
            query, cotan = queries[j, block], cotans[j, block]
            scores = jnp.dot(query, turned[0], preferred_element_type=F32) * scale
            first = me.ctx * tokens + i * block_rows
            place = first + lax.broadcasted_iota(jnp.int32, scores.shape, 0)
            scores = jnp.where(
                lax.broadcasted_iota(jnp.int32, scores.shape, 1) <= place, scores, -1e30
            )
            raised = jnp.exp(scores - jnp.max(scores, axis=1, keepdims=True))
            shares = raised / jnp.sum(raised, axis=1, keepdims=True)
            low = shares.astype(BF16)
            outputs = jnp.dot(low, keys[1], preferred_element_type=F32)
            share_grad = jnp.dot(cotan, turned[1], preferred_element_type=F32)
            delta = jnp.sum(cotan.astype(F32) * outputs, axis=1, keepdims=True)
            score_grad = (shares * (share_grad - delta) * scale).astype(BF16)
            every[chip, seat, j, block] = jnp.dot(
                score_grad, keys[0], preferred_element_type=F32
            ).astype(BF16)
            turned_grads[0] += jnp.dot(
                jnp.transpose(query), score_grad, preferred_element_type=F32
            )
            turned_grads[1] += jnp.dot(jnp.transpose(cotan), low, preferred_element_type=F32)
            return carry

        lax.fori_loop(0, part_rows // block_rows, body, 0)

    dq_copies, late_copies = {}, []

    def late_send_on(n, k):
        for hop in range(1, chips):
            block = unit(n, seats[k])
            m = len(late_copies)
            copy = remote(block, block, late_send.at[m], late_recv.at[m], me.across(hop))
            copy.start()
            late_copies.append((units[n][0], copy))

    def leave(n):
        t, _, j = units[n]
        if j >= soon:
            late_send_on(n, 0)
            return
        for hop in range(1, chips):
            m = units.index((t, hop, j))
            block = unit(n, seat)
            copy = remote(block, block, dq_send.at[m], dq_recv.at[m], me.across(hop))
            copy.start()
            dq_copies[m] = copy

    for p in range(2):
        for k in range(heads):
            ready = [list(late_units[t]) + list(soon_units[t]) for t in range(parts)]
            attend(p, units[ready[0][k]][2])
            for t in range(p * parts // 2, (p + 1) * parts // 2):
                leave(ready[t][k])
                if t == 0:
                    dq_spread.start(ready[t][k])

    def column(at):
        return span(at * tokens, tokens)

    core_copies = []
    for hop in range(chips):
        spot = me.source(hop) * 2
        copy = remote(
            turned_grads.at[:, :, column(spot + 1 - core)],
            core_got.at[me.source(hop)],
            core_send.at[hop],
            core_recv.at[hop],
            me.sibling,
        )
        copy.start()
        core_copies.append(copy)
    kept_out[...] = jnp.zeros(kept_out.shape, F32)
    pair_low[...] = jnp.zeros(pair_low.shape, F32)
    for hop in range(chips):
        core_copies[hop].wait_recv()
        for which in range(2):
            both = (
                turned_grads[which, :, column(me.source(hop) * 2 + core)]
                + core_got[me.source(hop), which]
            )
            if hop:
                grads_low[hop - 1, which] = jnp.transpose(both).astype(BF16)
            else:
                kept_out[0] = jnp.where(row == which, jnp.transpose(both), kept_out[0])
                pair_low[...] = jnp.where(row == which, pair_low[...], jnp.transpose(both))
    chip_copies = []
    for hop in range(1, chips):
        copy = remote(
            grads_low.at[hop - 1],
            chip_got.at[hop - 1],
            chip_send.at[hop - 1],
            chip_recv.at[hop - 1],
            (me.source(hop) * 2 + core, me.head),
        )
        copy.start()
        chip_copies.append(copy)

    for n in far_units[0]:
        dq_copies[n].wait_recv()
        dq_spread.start(n)
    shares = []
    for j, later, copy in trades:
        copy.wait_recv()
        block = group_mats.at[seat_of(j), later, ours]
        share = remote(block, block, share_send.at[j], share_recv.at[j], me.sibling)
        share.start()
        shares.append(share)
    if early:

        @pl.when(holder)
        def _():
            for bit in (1, 2):
                came_ahead(bit).wait_recv()
                share_ahead(bit).start()

    def hand_round(t):
        if t + 1 < parts:
            for n in list(late_units[t + 1]) + list(soon_units[t + 1]):
                dq_spread.start(n)
        for n in list(late_units[t]) + list(soon_units[t]):
            dq_spread.pass_on(n)
        if t + 1 < parts:
            for n in far_units[t + 1]:
                dq_copies[n].wait_recv()
                dq_spread.start(n)
        for n in far_units[t]:
            dq_spread.pass_on(n)
        for n in late_units[t]:
            dq_spread.arrive(n)
            for k in range(1, group):
                late_send_on(n, k)

    hand_round(0)

    for hop in range(1, chips):
        chip_copies[hop - 1].wait_recv()
        for which in range(2):
            value = chip_got[hop - 1, which].astype(F32)
            kept_out[0] += jnp.where(row == which, value, 0.0)
            pair_low[...] += jnp.where(row == which, 0.0, value)
    last_low = grads_low.at[chips - 1, 0]
    last_low[...] = pair_low[...].astype(BF16)
    last = remote(last_low, pair_got, last_send.at[0], last_recv.at[0], me.beside(1))

    store.wait()
    for copy in shares:
        copy.wait_recv()
    if early:

        @pl.when(jnp.logical_not(holder))
        def _():
            for bit in (1, 2):
                share_ahead(bit).wait_recv()

    step = min(512, piece) if chips <= 2 else min(256, piece)
    flat = [(m, j) for m in range(group) for j in range(heads)]

    def made_copy(hop, i):
        return remote(
            made.at[hop - 1, i],
            hub.at[chips - hop, i],
            made_send.at[hop - 1, i],
            made_recv.at[chips - hop - 1, i],
            (me.source(hop) * 2 + core, me.head),
        )

    def land_copy(hop, i):
        return remote(
            hub.at[hop, i],
            land.at[family, i],
            land_send.at[hop, i],
            land_recv.at[family, i],
            (me.ctx, me.source(hop) * group + seat),
        )

    def moves(hop):
        return me.source(hop) != family

    def multiply(t):
        block = pl.ds(t * lines, lines)

        def body(i, carry):
            part = span(i * step, step)
            total = jnp.zeros((chips * lines, step), F32)
            for k in range(0, len(flat), 2):
                both = flat[k : k + 2]
                left = jnp.concatenate(
                    [
                        jnp.concatenate([every[me.source(hop), m, j, block] for m, j in both], axis=1)
                        for hop in range(chips)
                    ],
                    axis=0,
                )
                right = jnp.concatenate([group_mats[m, j, part] for m, j in both], axis=1)
                total += lax.dot_general(
                    left, right, (((1,), (1,)), ((), ())), preferred_element_type=F32
                )
            for hop in range(chips):
                result = made.at[hop - 1] if hop else hub.at[0]
                result[t, :, part] = total[hop * lines : (hop + 1) * lines].astype(BF16)
            return carry

        lax.fori_loop(0, piece // step, body, 0)
        for hop in range(1, chips):
            made_copy(hop, t).start()
        pl.when(moves(0))(land_copy(0, t).start)

    def pass_made(t):
        for hop in range(1, chips):
            made_copy(chips - hop, t).wait_recv()
            pl.when(moves(hop))(land_copy(hop, t).start)

    def finish_part(t):
        for n in list(soon_units[t]) + list(far_units[t]):
            dq_spread.arrive(n)
        for when, copy in late_copies:
            if when == t:
                copy.wait_recv()
        multiply(t)

    for t in range(1, parts):
        hand_round(t)
        finish_part(t - 1)
        if t == 1:
            last.start()
        else:
            pass_made(t - 2)
    pass_made(parts - 2)
    finish_part(parts - 1)
    pass_made(parts - 1)

    last.wait()
    kept_out[0] += pair_got[...].astype(F32)

    stay = lax.rem(chip - family + chips, chips)
    for t in range(parts):
        total = hub[stay, t].astype(F32)
        for home in homes:
            arrival = remote(
                hub.at[0, t], land.at[home, t], land_send.at[0, t], land_recv.at[home, t], me.sibling
            )
            arrival.wait_recv()
            total = total + land[home, t].astype(F32)
        input_grad_out[pl.ds(t * lines, lines)] = total.astype(BF16)

    for hop in range(chips):
        for i in range(parts):
            if hop:
                made_copy(hop, i).wait_send()
            pl.when(moves(hop))(land_copy(hop, i).wait_send)
    for copy in crossing + swaps + pair_copies + pair_next + pair_last + shares:
        copy.wait_send()
    for copy in core_copies + chip_copies + list(straight.values()):
        copy.wait_send()
    for copy in list(sums.values()) + list(dq_copies.values()):
        copy.wait_send()
    for _, copy in late_copies:
        copy.wait_send()
    for _, _, copy in trades:
        copy.wait_send()
    when_ahead(lambda bit: ahead(bit).wait_send())
    if early:

        @pl.when(holder)
        def _():
            for bit in (1, 2):
                share_ahead(bit).wait_send()

    spread.finish()
    dq_spread.finish()


def per_device(
    layer_input, output_grad, routes, route_gates, query_weight, output_weight, key_values
):
    ctx_count, head_count = lax.axis_size("ctx"), lax.axis_size("head")
    chips = ctx_count // 2
    group, hops = head_count // chips, chips - 1
    heads, depth, width = query_weight.shape
    tokens = layer_input.shape[0]
    half = 2 * depth
    piece = half // group
    window = tokens * ctx_count
    count = 2 * hops * SUBS
    parts = part_count(chips)
    units, lines = parts * chips * heads, tokens // parts
    return pl.pallas_call(
        layer_kernel,
        out_shape=(
            jax.ShapeDtypeStruct((tokens, piece), BF16),
            jax.ShapeDtypeStruct((1, tokens, width), F32),
        ),
        in_specs=[ANY, ANY, VMEM, VMEM, ANY, ANY, VMEM],
        out_specs=(VMEM, VMEM),
        scratch_shapes=[
            pltpu.VMEM((2, heads, half, width), BF16),
            pltpu.VMEM((2, tokens, half), BF16),
            pltpu.VMEM((hops, 2, group, tokens, piece), BF16),
            pltpu.VMEM((2, tokens, heads * width), F32),
            pltpu.VMEM((hops, 2, tokens, heads * width), F32),
            pltpu.VMEM((hops, tokens, heads * width), F32),
            pltpu.VMEM((hops, tokens, heads * width), BF16),
            pltpu.VMEM((hops, tokens, heads * width), BF16),
            pltpu.VMEM((heads, tokens, width), BF16),
            pltpu.VMEM((heads, tokens, width), BF16),
            pltpu.VMEM((group, heads, piece, width), BF16),
            pltpu.VMEM((2, window, width), BF16),
            pltpu.VMEM((2, width, window), BF16),
            pltpu.VMEM((2, width, window), F32),
            pltpu.VMEM((chips, 2, width, tokens), F32),
            pltpu.VMEM((chips, 2, tokens, width), BF16),
            pltpu.VMEM((hops, 2, tokens, width), BF16),
            pltpu.VMEM((tokens, width), F32),
            pltpu.VMEM((tokens, width), BF16),
            pltpu.VMEM((chips, group, heads, tokens, width), BF16),
            pltpu.VMEM((hops, parts, lines, piece), BF16),
            pltpu.VMEM((chips, parts, lines, piece), BF16),
            pltpu.VMEM((chips, parts, lines, piece), BF16),
            DMA((6,)),
            DMA((4,)),
        ]
        + [DMA((count,))] * 4
        + Spread.sems(count)
        + [DMA((2, hops, 2))] * 2
        + [DMA((4 * chips,))] * 2
        + [DMA((group,))] * 2
        + [DMA((5,))] * 2
        + [DMA((group,))] * 2
        + [DMA((units,))] * 2
        + Spread.sems(units)
        + [DMA((hops * parts * heads * group,))] * 2
        + [DMA((chips,))] * 4
        + [DMA((1,))] * 2
        + [DMA((hops, parts))] * 2
        + [DMA((chips, parts))] * 2,
        compiler_params=pltpu.CompilerParams(
            collective_id=0, has_side_effects=True, vmem_limit_bytes=VMEM_BYTES
        ),
    )(
        layer_input,
        output_grad,
        routes.T,
        route_gates.T,
        query_weight,
        output_weight,
        key_values,
    )


def solution(mesh):
    in_specs = (
        P("ctx", None),
        P("ctx", None),
        P("ctx", None),
        P("ctx", None),
        P("head", "ctx", None),
        P("head", "ctx", None),
        P("head", "ctx", None),
    )
    out_specs = (P("ctx", "head"), P("head", "ctx", None))
    return jax.shard_map(
        per_device, mesh=mesh, in_specs=in_specs, out_specs=out_specs, check_vma=False
    )
```

```python
import functools

import jax
import jax.numpy as jnp
from jax import lax
from jax.experimental import pallas as pl
from jax.experimental.pallas import tpu as pltpu
from jax.sharding import PartitionSpec as P

MESH = pl.DeviceIdType.MESH
ANY = pl.BlockSpec(memory_space=pl.ANY)
VMEM = pl.BlockSpec(memory_space=pltpu.VMEM)
DMA = pltpu.SemaphoreType.DMA
F32, BF16 = jnp.float32, jnp.bfloat16
SUBS = 4
STRAIGHT = 2
VMEM_BYTES = 67_043_328


def remote(source, target, send, recv, place):
    return pltpu.make_async_remote_copy(
        src_ref=source,
        dst_ref=target,
        send_sem=send,
        recv_sem=recv,
        device_id=place,
        device_id_type=MESH,
    )


def local(source, target, sem):
    return pltpu.make_async_copy(source, target, sem)


def greet(places):
    barrier = pltpu.get_barrier_semaphore()
    for place in places:
        pl.semaphore_signal(barrier, inc=1, device_id=place, device_id_type=MESH)
    pl.semaphore_wait(barrier, len(places))


def flip(index, bit):
    return index + bit - 2 * bit * ((index // bit) % 2)


def span(start, size):
    return pl.ds(pl.multiple_of(start, size), size)


def late_heads(heads, group):
    return 2 * heads // 5 if group == 4 else 0


def part_count(chips):
    return 4 if chips <= 2 else 2


def pairs(count):
    return [tuple(range(j, min(j + 2, count))) for j in range(0, count, 2)]


class Place:
    def __init__(self):
        self.ctx_count, self.head_count = lax.axis_size("ctx"), lax.axis_size("head")
        self.ctx, self.head = lax.axis_index("ctx"), lax.axis_index("head")
        self.chips = self.ctx_count // 2
        self.chip, self.core = self.ctx // 2, self.ctx % 2
        self.group = self.head_count // self.chips
        self.seat = self.head % self.group
        self.bits = [bit for bit in (1, 2) if bit < self.group]
        self.sibling = (self.ctx + 1 - 2 * self.core, self.head)

    def other(self, hop):
        return lax.rem(self.chip + hop, self.chips)

    def source(self, hop):
        return lax.rem(self.chip - hop + self.chips, self.chips)

    def across(self, hop):
        return (self.other(hop) * 2 + self.core, self.head)

    def beside(self, bit):
        return (self.ctx, flip(self.head, bit))

    def friends(self):
        hops = [self.across(hop) for hop in range(1, self.chips)]
        return hops + [self.beside(bit) for bit in self.bits] + [self.sibling]


class Spread:
    def __init__(self, place, located, sems, straight=()):
        self.place, self.located = place, located
        self.straight = dict(straight)
        self.direct_send, self.direct_recv, self.relay_send, self.relay_recv = sems
        self.direct, self.relay = {}, {}

    @staticmethod
    def sems(count):
        return [DMA((2, count))] * 2 + [DMA((count,))] * 2

    def start(self, n):
        for i, bit in enumerate(self.place.bits):
            block = self.located(n, self.place.seat)
            copy = remote(
                block,
                block,
                self.direct_send.at[i, n],
                self.direct_recv.at[i, n],
                self.place.beside(bit),
            )
            copy.start()
            self.direct[n, bit] = copy

    def pass_on(self, n):
        if len(self.place.bits) < 2 or n in self.straight:
            return
        came, onward = (2, 1) if n % 2 == 0 else (1, 2)
        self.direct[n, came].wait_recv()
        block = self.located(n, flip(self.place.seat, came))
        copy = remote(
            block, block, self.relay_send.at[n], self.relay_recv.at[n], self.place.beside(onward)
        )
        copy.start()
        self.relay[n] = copy

    def arrive(self, n):
        if n in self.straight:
            for bit in self.place.bits:
                self.direct[n, bit].wait_recv()
            self.straight[n].wait_recv()
        elif len(self.place.bits) == 1:
            self.direct[n, 1].wait_recv()
        elif len(self.place.bits) == 2:
            self.direct[n, 1 if n % 2 == 0 else 2].wait_recv()
            self.relay[n].wait_recv()

    def finish(self):
        for copy in list(self.direct.values()) + list(self.relay.values()):
            copy.wait_send()


def contract(rows, weights, total, first):
    heads, depth, width = weights.shape
    step = min(512, depth)

    def body(i, carry):
        part = span(i * step, step)
        left = rows[:, part]
        for group in pairs(heads):
            right = jnp.concatenate([weights[j, part] for j in group], axis=1)
            columns = pl.ds(group[0] * width, len(group) * width)
            total[:, columns] += jnp.dot(left, right, preferred_element_type=F32)
        return carry

    if first:
        total[...] = jnp.zeros(total.shape, F32)
    lax.fori_loop(0, depth // step, body, 0)


def layer_kernel(
    input_ref,
    cotan_ref,
    route_ref,
    gate_ref,
    query_ref,
    output_ref,
    pair_ref,
    input_grad_out,
    kept_out,
    mats,
    own,
    far,
    own_sum,
    far_sum,
    q_got,
    da_low,
    da_got,
    queries,
    cotans,
    group_mats,
    keys,
    turned,
    turned_grads,
    core_got,
    grads_low,
    chip_got,
    pair_low,
    pair_got,
    every,
    made,
    hub,
    land,
    load_sem,
    weight_sem,
    x_send,
    x_recv,
    straight_send,
    straight_recv,
    direct_send,
    direct_recv,
    relay_send,
    relay_recv,
    sum_send,
    sum_recv,
    pair_send,
    pair_recv,
    trade_send,
    trade_recv,
    early_send,
    early_recv,
    share_send,
    share_recv,
    dq_send,
    dq_recv,
    dq_direct_send,
    dq_direct_recv,
    dq_relay_send,
    dq_relay_recv,
    late_send,
    late_recv,
    core_send,
    core_recv,
    chip_send,
    chip_recv,
    last_send,
    last_recv,
    made_send,
    made_recv,
    land_send,
    land_recv,
):
    me = Place()
    chips, chip, core, seat, group = me.chips, me.chip, me.core, me.seat, me.group
    heads, depth, width = query_ref.shape
    tokens = input_ref.shape[0]
    window = tokens * me.ctx_count
    half = 2 * depth
    piece = half // group
    family = me.head // group
    acts, sources = (input_ref, cotan_ref), (query_ref, output_ref)
    rows = tokens // SUBS
    part_rows = tokens // 2

    mine = span(core * depth, depth)
    loads = []
    for a in range(2):
        loads.append(local(sources[a], mats.at[a, :, mine], load_sem.at[a]))
        loads.append(local(acts[a].at[:, span(chip * half, half)], own.at[a], load_sem.at[2 + a]))

    places = me.friends()
    if group == 4:
        places.append((me.ctx, flip(flip(me.head, 1), 2)))
    homes = [lax.rem(family + i, chips) for i in range(1, chips)]
    places += [(me.ctx, home * group + seat) for home in homes]
    greet(places)

    order = [(a, hop, s) for a in range(2) for hop in range(1, chips) for s in range(SUBS)]

    def located(n, at):
        a, hop, s = order[n]
        return far.at[hop - 1, a, at, pl.ds(s * rows, rows)]

    crossing = []
    for n, (a, hop, s) in enumerate(order):
        begin = pl.multiple_of(me.other(hop) * half + seat * piece, piece)
        copy = remote(
            acts[a].at[pl.ds(s * rows, rows), pl.ds(begin, piece)],
            located(n, seat),
            x_send.at[n],
            x_recv.at[n],
            me.across(hop),
        )
        copy.start()
        crossing.append(copy)
    straight = {}
    for n, (a, hop, s) in enumerate(order):
        if group == 4 and a == 1 and s >= SUBS - STRAIGHT:
            at = flip(flip(seat, 1), 2)
            begin = pl.multiple_of(me.other(hop) * half + at * piece, piece)
            copy = remote(
                acts[a].at[pl.ds(s * rows, rows), pl.ds(begin, piece)],
                located(n, at),
                straight_send.at[len(straight)],
                straight_recv.at[len(straight)],
                me.across(hop),
            )
            copy.start()
            straight[n] = copy
    for copy in loads:
        copy.start()
    swaps = []
    for a in range(2):
        copy = remote(
            sources[a], mats.at[a, :, mine], weight_sem.at[a], weight_sem.at[2 + a], me.sibling
        )
        copy.start()
        swaps.append(copy)

    row = me.head % 2

    def key_block(which, at):
        return keys.at[which, span(at * tokens, tokens)]

    pair_copies = []
    for hop in range(1, chips):
        copy = remote(
            pair_ref.at[0],
            key_block(row, me.ctx),
            pair_send.at[hop],
            pair_recv.at[hop],
            me.across(hop),
        )
        copy.start()
        pair_copies.append(copy)
    keep = local(pair_ref.at[0], key_block(row, me.ctx), load_sem.at[4])
    keep.start()

    early = 1 if group == 4 else 0
    holder = core == seat // 2

    def ahead(bit):
        to = flip(seat, bit)
        begin = pl.multiple_of(to * piece - core * depth, piece)
        return remote(
            query_ref.at[pl.ds(0, early), pl.ds(begin, piece)],
            group_mats.at[seat, pl.ds(0, early)],
            early_send.at[bit],
            early_recv.at[bit],
            me.beside(bit),
        )

    def came_ahead(bit):
        return remote(
            group_mats.at[seat, pl.ds(0, early)],
            group_mats.at[flip(seat, bit), pl.ds(0, early)],
            early_send.at[bit],
            early_recv.at[bit],
            me.beside(bit),
        )

    def share_ahead(bit):
        block = group_mats.at[flip(seat, bit), pl.ds(0, early)]
        return remote(
            block, block, early_send.at[2 + bit], early_recv.at[2 + bit], me.sibling
        )

    def when_ahead(action):
        if early:
            pl.when(holder)(lambda: action(1))
            pl.when(jnp.logical_not(holder))(lambda: action(2))

    when_ahead(lambda bit: ahead(bit).start())

    spread = Spread(
        me, located, (direct_send, direct_recv, relay_send, relay_recv), straight.items()
    )

    def own_slice(a, i):
        part = pl.ds(i * piece, piece)
        contract(own.at[a, :, part], mats.at[a, :, part], own_sum.at[a], i == 0)

    seats = [seat] + [flip(seat, 1)] * (group > 1)
    if group == 4:
        seats += [flip(seat, 2), flip(flip(seat, 1), 2)]
    sums = {}

    def far_part(a, hop, p):
        block = pl.ds(p * part_rows, part_rows)
        for n, (b, by, s) in enumerate(order):
            if (b, by) == (a, hop) and s // (SUBS // 2) == p:
                spread.arrive(n)
        for i, at in enumerate(seats):
            part = span(at * piece, piece)
            contract(
                far.at[hop - 1, a, at, block],
                mats.at[a, :, part],
                far_sum.at[hop - 1, a, block],
                i == 0,
            )
        if a == 0:
            source, target = far_sum.at[hop - 1, 0, block], q_got.at[hop - 1, block]
        else:
            da_low[hop - 1, block] = far_sum[hop - 1, 1, block].astype(BF16)
            source, target = da_low.at[hop - 1, block], da_got.at[hop - 1, block]
        copy = remote(
            source,
            target,
            sum_send.at[a, hop - 1, p],
            sum_recv.at[a, hop - 1, p],
            (me.source(hop) * 2 + core, me.head),
        )
        copy.start()
        sums[a, hop, p] = copy

    own_work = [(a, i) for a in range(2) for i in range(group)]
    count = len(order)
    for n in range(count):
        crossing[n].wait_recv()
        spread.start(n)
        if n >= 1:
            spread.pass_on(n - 1)
        if n == 1:
            for copy in loads:
                copy.wait()
            for copy in swaps:
                copy.wait_recv()
        if n >= 2 and own_work:
            own_slice(*own_work.pop(0))
        if chips == 2 and n == count - 3:
            far_part(0, 1, 0)
        if chips == 2 and n == count - 1:
            far_part(0, 1, 1)
    spread.pass_on(count - 1)

    keep.wait()
    for copy in pair_copies:
        copy.wait_recv()
    pair_next = []
    for hop in range(chips):
        block = key_block(row, me.source(hop) * 2 + core)
        copy = remote(
            block, block, pair_send.at[chips + hop], pair_recv.at[chips + hop], me.beside(1)
        )
        copy.start()
        pair_next.append(copy)

    part_columns = piece // 2
    ours = span(core * part_columns, part_columns)
    trades = []

    def seat_of(j):
        at = seat + 0
        for bit in (1, 2):
            if j & bit:
                at = flip(at, bit)
        return at

    for j in range(1, group):
        to = seat_of(j)
        later = pl.ds(early if j < 3 else 0, heads - (early if j < 3 else 0))
        copy = remote(
            mats.at[0, later, span(to * piece + core * part_columns, part_columns)],
            group_mats.at[seat, later, ours],
            trade_send.at[j],
            trade_recv.at[j],
            (me.ctx, me.head - seat + to),
        )
        copy.start()
        trades.append((j, later, copy))
    store = local(mats.at[0, :, span(seat * piece, piece)], group_mats.at[seat], load_sem.at[5])
    store.start()

    for work in own_work:
        own_slice(*work)
    for a in range(2):
        for p in range(2):
            for hop in range(1, chips):
                if (a, hop, p) not in sums:
                    far_part(a, hop, p)

    for copy in pair_next:
        copy.wait_recv()
    pair_last = []
    for hop in range(chips):
        for which in range(2):
            block = key_block(which, me.source(hop) * 2 + core)
            k = 2 * chips + 2 * hop + which
            copy = remote(block, block, pair_send.at[k], pair_recv.at[k], me.sibling)
            copy.start()
            pair_last.append(copy)

    lanes = []
    for j in range(heads - 1):
        named = route_ref[...] == me.head * (heads - 1) + j
        lanes.append(jnp.sum(jnp.where(named, gate_ref[...], 0.0), axis=0, keepdims=True))
    lanes.append(jnp.ones_like(lanes[0]))
    lanes += [jnp.zeros_like(lanes[0])] * (-heads % 8)
    token_gate = jnp.transpose(jnp.concatenate(lanes, axis=0))

    for hop in range(1, chips):
        for p in range(2):
            sums[0, hop, p].wait_recv()
    for j in range(heads):
        columns = pl.ds(j * width, width)
        value = own_sum[0, :, columns]
        for hop in range(1, chips):
            value = value + q_got[hop - 1, :, columns]
        queries[j] = value.astype(BF16)
    for copy in pair_last:
        copy.wait_recv()
    for which in range(2):
        for at in range(me.ctx_count):
            block = pl.ds(at * tokens, tokens)
            turned[which, :, block] = jnp.transpose(keys[which, block])
    for hop in range(1, chips):
        for p in range(2):
            sums[1, hop, p].wait_recv()
    for j in range(heads):
        columns = pl.ds(j * width, width)
        value = own_sum[1, :, columns]
        for hop in range(1, chips):
            value = value + da_got[hop - 1, :, columns].astype(F32)
        if j < heads - 1:
            value = value * token_gate[:, j : j + 1]
        cotans[j] = value.astype(BF16)

    late = late_heads(heads, group)
    soon = heads - late
    parts = part_count(chips)
    lines = tokens // parts
    units, late_units, soon_units, far_units = [], [], [], []
    for t in range(parts):
        late_units.append(range(len(units), len(units) + (late > 0)))
        units += [(t, 0, pl.ds(soon, late))] * (late > 0)
        soon_units.append(range(len(units), len(units) + 1))
        units.append((t, 0, pl.ds(0, soon)))
        far_units.append(range(len(units), len(units) + chips - 1))
        units += [(t, hop, pl.ds(0, soon)) for hop in range(1, chips)]

    def unit(n, at):
        t, hop, which = units[n]
        return every.at[me.source(hop), at, which, pl.ds(t * lines, lines)]

    dq_spread = Spread(
        me, unit, (dq_direct_send, dq_direct_recv, dq_relay_send, dq_relay_recv)
    )
    block_rows = min(part_rows, max(16, 256 * 1024 // window))
    scale = width ** (-0.5)
    turned_grads[...] = jnp.zeros(turned_grads.shape, F32)

    def attend(t, j):
        def body(i, carry):
            i = t * (part_rows // block_rows) + i
            block = span(i * block_rows, block_rows)
            query, cotan = queries[j, block], cotans[j, block]
            scores = jnp.dot(query, turned[0], preferred_element_type=F32) * scale
            first = me.ctx * tokens + i * block_rows
            place = first + lax.broadcasted_iota(jnp.int32, scores.shape, 0)
            scores = jnp.where(
                lax.broadcasted_iota(jnp.int32, scores.shape, 1) <= place, scores, -1e30
            )
            raised = jnp.exp(scores - jnp.max(scores, axis=1, keepdims=True))
            shares = raised / jnp.sum(raised, axis=1, keepdims=True)
            low = shares.astype(BF16)
            outputs = jnp.dot(low, keys[1], preferred_element_type=F32)
            share_grad = jnp.dot(cotan, turned[1], preferred_element_type=F32)
            delta = jnp.sum(cotan.astype(F32) * outputs, axis=1, keepdims=True)
            score_grad = (shares * (share_grad - delta) * scale).astype(BF16)
            every[chip, seat, j, block] = jnp.dot(
                score_grad, keys[0], preferred_element_type=F32
            ).astype(BF16)
            turned_grads[0] += jnp.dot(
                jnp.transpose(query), score_grad, preferred_element_type=F32
            )
            turned_grads[1] += jnp.dot(jnp.transpose(cotan), low, preferred_element_type=F32)
            return carry

        lax.fori_loop(0, part_rows // block_rows, body, 0)

    dq_copies, late_copies = {}, []

    def late_send_on(n, k):
        for hop in range(1, chips):
            block = unit(n, seats[k])
            m = len(late_copies)
            copy = remote(block, block, late_send.at[m], late_recv.at[m], me.across(hop))
            copy.start()
            late_copies.append((units[n][0], copy))

    for p in range(2):
        these = range(p * parts // 2, (p + 1) * parts // 2)
        for j in range(soon, heads):
            attend(p, j)
        for t in these:
            for n in late_units[t]:
                late_send_on(n, 0)
                if t < 2:
                    dq_spread.start(n)
        for j in range(soon):
            attend(p, j)
        for t in these:
            for n in soon_units[t]:
                if t == 0:
                    dq_spread.start(n)
                for hop in range(1, chips):
                    m = far_units[t][hop - 1]
                    block = unit(n, seat)
                    k = t * (chips - 1) + hop - 1
                    copy = remote(block, block, dq_send.at[k], dq_recv.at[k], me.across(hop))
                    copy.start()
                    dq_copies[m] = copy

    def column(at):
        return span(at * tokens, tokens)

    core_copies = []
    for hop in range(chips):
        spot = me.source(hop) * 2
        copy = remote(
            turned_grads.at[:, :, column(spot + 1 - core)],
            core_got.at[me.source(hop)],
            core_send.at[hop],
            core_recv.at[hop],
            me.sibling,
        )
        copy.start()
        core_copies.append(copy)
    kept_out[...] = jnp.zeros(kept_out.shape, F32)
    pair_low[...] = jnp.zeros(pair_low.shape, F32)
    for hop in range(chips):
        core_copies[hop].wait_recv()
        for which in range(2):
            both = (
                turned_grads[which, :, column(me.source(hop) * 2 + core)]
                + core_got[me.source(hop), which]
            )
            if hop:
                grads_low[hop - 1, which] = jnp.transpose(both).astype(BF16)
            else:
                kept_out[0] = jnp.where(row == which, jnp.transpose(both), kept_out[0])
                pair_low[...] = jnp.where(row == which, pair_low[...], jnp.transpose(both))
    chip_copies = []
    for hop in range(1, chips):
        copy = remote(
            grads_low.at[hop - 1],
            chip_got.at[hop - 1],
            chip_send.at[hop - 1],
            chip_recv.at[hop - 1],
            (me.source(hop) * 2 + core, me.head),
        )
        copy.start()
        chip_copies.append(copy)

    for n in far_units[0]:
        dq_copies[n].wait_recv()
        dq_spread.start(n)
    shares = []
    for j, later, copy in trades:
        copy.wait_recv()
        block = group_mats.at[seat_of(j), later, ours]
        share = remote(block, block, share_send.at[j], share_recv.at[j], me.sibling)
        share.start()
        shares.append(share)
    if early:

        @pl.when(holder)
        def _():
            for bit in (1, 2):
                came_ahead(bit).wait_recv()
                share_ahead(bit).start()

    def start_rest(t):
        for n in soon_units[t]:
            dq_spread.start(n)
        for n in far_units[t]:
            dq_copies[n].wait_recv()
            dq_spread.start(n)

    def hand_round(t):
        for n in late_units[t]:
            dq_spread.pass_on(n)
        if t + 1 < parts:
            start_rest(t + 1)
        for n in list(soon_units[t]) + list(far_units[t]):
            dq_spread.pass_on(n)
        if t + 2 < parts:
            for n in late_units[t + 2]:
                dq_spread.start(n)
        for n in late_units[t]:
            dq_spread.arrive(n)
            for k in range(1, group):
                late_send_on(n, k)

    hand_round(0)

    for hop in range(1, chips):
        chip_copies[hop - 1].wait_recv()
        for which in range(2):
            value = chip_got[hop - 1, which].astype(F32)
            kept_out[0] += jnp.where(row == which, value, 0.0)
            pair_low[...] += jnp.where(row == which, 0.0, value)
    last_low = grads_low.at[chips - 1, 0]
    last_low[...] = pair_low[...].astype(BF16)
    last = remote(last_low, pair_got, last_send.at[0], last_recv.at[0], me.beside(1))

    store.wait()
    for copy in shares:
        copy.wait_recv()
    if early:

        @pl.when(jnp.logical_not(holder))
        def _():
            for bit in (1, 2):
                share_ahead(bit).wait_recv()

    step = min(512, piece) if chips <= 2 else min(256, piece)
    flat = [(m, j) for m in range(group) for j in range(heads)]

    def made_copy(hop, i):
        return remote(
            made.at[hop - 1, i],
            hub.at[chips - hop, i],
            made_send.at[hop - 1, i],
            made_recv.at[chips - hop - 1, i],
            (me.source(hop) * 2 + core, me.head),
        )

    def land_copy(hop, i):
        return remote(
            hub.at[hop, i],
            land.at[family, i],
            land_send.at[hop, i],
            land_recv.at[family, i],
            (me.ctx, me.source(hop) * group + seat),
        )

    def moves(hop):
        return me.source(hop) != family

    def multiply(t):
        block = pl.ds(t * lines, lines)

        def body(i, carry):
            part = span(i * step, step)
            total = jnp.zeros((chips * lines, step), F32)
            for k in range(0, len(flat), 2):
                both = flat[k : k + 2]
                left = jnp.concatenate(
                    [
                        jnp.concatenate([every[me.source(hop), m, j, block] for m, j in both], axis=1)
                        for hop in range(chips)
                    ],
                    axis=0,
                )
                right = jnp.concatenate([group_mats[m, j, part] for m, j in both], axis=1)
                total += lax.dot_general(
                    left, right, (((1,), (1,)), ((), ())), preferred_element_type=F32
                )
            for hop in range(chips):
                result = made.at[hop - 1] if hop else hub.at[0]
                result[t, :, part] = total[hop * lines : (hop + 1) * lines].astype(BF16)
            return carry

        lax.fori_loop(0, piece // step, body, 0)
        for hop in range(1, chips):
            made_copy(hop, t).start()
        pl.when(moves(0))(land_copy(0, t).start)

    def pass_made(t):
        for hop in range(1, chips):
            made_copy(chips - hop, t).wait_recv()
            pl.when(moves(hop))(land_copy(hop, t).start)

    def finish_part(t):
        for n in list(soon_units[t]) + list(far_units[t]):
            dq_spread.arrive(n)
        for when, copy in late_copies:
            if when == t:
                copy.wait_recv()
        multiply(t)

    for t in range(1, parts):
        hand_round(t)
        finish_part(t - 1)
        if t == 1:
            last.start()
        else:
            pass_made(t - 2)
    pass_made(parts - 2)
    finish_part(parts - 1)
    pass_made(parts - 1)

    last.wait()
    kept_out[0] += pair_got[...].astype(F32)

    stay = lax.rem(chip - family + chips, chips)
    for t in range(parts):
        total = hub[stay, t].astype(F32)
        for home in homes:
            arrival = remote(
                hub.at[0, t], land.at[home, t], land_send.at[0, t], land_recv.at[home, t], me.sibling
            )
            arrival.wait_recv()
            total = total + land[home, t].astype(F32)
        input_grad_out[pl.ds(t * lines, lines)] = total.astype(BF16)

    for hop in range(chips):
        for i in range(parts):
            if hop:
                made_copy(hop, i).wait_send()
            pl.when(moves(hop))(land_copy(hop, i).wait_send)
    for copy in crossing + swaps + pair_copies + pair_next + pair_last + shares:
        copy.wait_send()
    for copy in core_copies + chip_copies + list(straight.values()):
        copy.wait_send()
    for copy in list(sums.values()) + list(dq_copies.values()):
        copy.wait_send()
    for _, copy in late_copies:
        copy.wait_send()
    for _, _, copy in trades:
        copy.wait_send()
    when_ahead(lambda bit: ahead(bit).wait_send())
    if early:

        @pl.when(holder)
        def _():
            for bit in (1, 2):
                share_ahead(bit).wait_send()

    spread.finish()
    dq_spread.finish()


def per_device(
    layer_input, output_grad, routes, route_gates, query_weight, output_weight, key_values
):
    ctx_count, head_count = lax.axis_size("ctx"), lax.axis_size("head")
    chips = ctx_count // 2
    group, hops = head_count // chips, chips - 1
    heads, depth, width = query_weight.shape
    tokens = layer_input.shape[0]
    half = 2 * depth
    piece = half // group
    window = tokens * ctx_count
    count = 2 * hops * SUBS
    parts = part_count(chips)
    late = late_heads(heads, group)
    units, lines = parts * (chips + (late > 0)), tokens // parts
    return pl.pallas_call(
        layer_kernel,
        out_shape=(
            jax.ShapeDtypeStruct((tokens, piece), BF16),
            jax.ShapeDtypeStruct((1, tokens, width), F32),
        ),
        in_specs=[ANY, ANY, VMEM, VMEM, ANY, ANY, VMEM],
        out_specs=(VMEM, VMEM),
        scratch_shapes=[
            pltpu.VMEM((2, heads, half, width), BF16),
            pltpu.VMEM((2, tokens, half), BF16),
            pltpu.VMEM((hops, 2, group, tokens, piece), BF16),
            pltpu.VMEM((2, tokens, heads * width), F32),
            pltpu.VMEM((hops, 2, tokens, heads * width), F32),
            pltpu.VMEM((hops, tokens, heads * width), F32),
            pltpu.VMEM((hops, tokens, heads * width), BF16),
            pltpu.VMEM((hops, tokens, heads * width), BF16),
            pltpu.VMEM((heads, tokens, width), BF16),
            pltpu.VMEM((heads, tokens, width), BF16),
            pltpu.VMEM((group, heads, piece, width), BF16),
            pltpu.VMEM((2, window, width), BF16),
            pltpu.VMEM((2, width, window), BF16),
            pltpu.VMEM((2, width, window), F32),
            pltpu.VMEM((chips, 2, width, tokens), F32),
            pltpu.VMEM((chips, 2, tokens, width), BF16),
            pltpu.VMEM((hops, 2, tokens, width), BF16),
            pltpu.VMEM((tokens, width), F32),
            pltpu.VMEM((tokens, width), BF16),
            pltpu.VMEM((chips, group, heads, tokens, width), BF16),
            pltpu.VMEM((hops, parts, lines, piece), BF16),
            pltpu.VMEM((chips, parts, lines, piece), BF16),
            pltpu.VMEM((chips, parts, lines, piece), BF16),
            DMA((6,)),
            DMA((4,)),
        ]
        + [DMA((count,))] * 2
        + [DMA((hops * STRAIGHT,))] * 2
        + Spread.sems(count)
        + [DMA((2, hops, 2))] * 2
        + [DMA((4 * chips,))] * 2
        + [DMA((group,))] * 2
        + [DMA((5,))] * 2
        + [DMA((group,))] * 2
        + [DMA((parts * hops,))] * 2
        + Spread.sems(units)
        + [DMA((max(1, hops * parts * group * (late > 0)),))] * 2
        + [DMA((chips,))] * 2
        + [DMA((hops,))] * 2
        + [DMA((1,))] * 2
        + [DMA((hops, parts))] * 2
        + [DMA((chips, parts))] * 2,
        compiler_params=pltpu.CompilerParams(
            collective_id=0, has_side_effects=True, vmem_limit_bytes=VMEM_BYTES
        ),
    )(
        layer_input,
        output_grad,
        routes.T,
        route_gates.T,
        query_weight,
        output_weight,
        key_values,
    )


def solution(mesh):
    in_specs = (
        P("ctx", None),
        P("ctx", None),
        P("ctx", None),
        P("ctx", None),
        P("head", "ctx", None),
        P("head", "ctx", None),
        P("head", "ctx", None),
    )
    out_specs = (P("ctx", "head"), P("head", "ctx", None))
    return jax.shard_map(
        per_device, mesh=mesh, in_specs=in_specs, out_specs=out_specs, check_vma=False
    )
```

```python
import functools

import jax
import jax.numpy as jnp
from jax import lax
from jax.experimental import pallas as pl
from jax.experimental.pallas import tpu as pltpu
from jax.sharding import PartitionSpec as P

MESH = pl.DeviceIdType.MESH
ANY = pl.BlockSpec(memory_space=pl.ANY)
VMEM = pl.BlockSpec(memory_space=pltpu.VMEM)
DMA = pltpu.SemaphoreType.DMA
F32, BF16 = jnp.float32, jnp.bfloat16
SUBS = 4
STRAIGHT = 2
VMEM_BYTES = 67_043_328


def remote(source, target, send, recv, place):
    return pltpu.make_async_remote_copy(
        src_ref=source,
        dst_ref=target,
        send_sem=send,
        recv_sem=recv,
        device_id=place,
        device_id_type=MESH,
    )


def local(source, target, sem):
    return pltpu.make_async_copy(source, target, sem)


def greet(places):
    barrier = pltpu.get_barrier_semaphore()
    for place in places:
        pl.semaphore_signal(barrier, inc=1, device_id=place, device_id_type=MESH)
    pl.semaphore_wait(barrier, len(places))


def flip(index, bit):
    return index + bit - 2 * bit * ((index // bit) % 2)


def span(start, size):
    return pl.ds(pl.multiple_of(start, size), size)


def late_heads(heads, group):
    return 2 * heads // 5 if group == 4 else 0


def part_count(chips):
    return 4 if chips <= 2 else 2


def pairs(count):
    return [tuple(range(j, min(j + 2, count))) for j in range(0, count, 2)]


class Place:
    def __init__(self):
        self.ctx_count, self.head_count = lax.axis_size("ctx"), lax.axis_size("head")
        self.ctx, self.head = lax.axis_index("ctx"), lax.axis_index("head")
        self.chips = self.ctx_count // 2
        self.chip, self.core = self.ctx // 2, self.ctx % 2
        self.group = self.head_count // self.chips
        self.seat = self.head % self.group
        self.bits = [bit for bit in (1, 2) if bit < self.group]
        self.sibling = (self.ctx + 1 - 2 * self.core, self.head)

    def other(self, hop):
        return lax.rem(self.chip + hop, self.chips)

    def source(self, hop):
        return lax.rem(self.chip - hop + self.chips, self.chips)

    def across(self, hop):
        return (self.other(hop) * 2 + self.core, self.head)

    def beside(self, bit):
        return (self.ctx, flip(self.head, bit))

    def friends(self):
        hops = [self.across(hop) for hop in range(1, self.chips)]
        return hops + [self.beside(bit) for bit in self.bits] + [self.sibling]


class Spread:
    def __init__(self, place, located, sems, straight=()):
        self.place, self.located = place, located
        self.straight = dict(straight)
        self.direct_send, self.direct_recv, self.relay_send, self.relay_recv = sems
        self.direct, self.relay = {}, {}

    @staticmethod
    def sems(count):
        return [DMA((2, count))] * 2 + [DMA((count,))] * 2

    def start(self, n):
        for i, bit in enumerate(self.place.bits):
            block = self.located(n, self.place.seat)
            copy = remote(
                block,
                block,
                self.direct_send.at[i, n],
                self.direct_recv.at[i, n],
                self.place.beside(bit),
            )
            copy.start()
            self.direct[n, bit] = copy

    def pass_on(self, n):
        if len(self.place.bits) < 2 or n in self.straight:
            return
        came, onward = (2, 1) if n % 2 == 0 else (1, 2)
        self.direct[n, came].wait_recv()
        block = self.located(n, flip(self.place.seat, came))
        copy = remote(
            block, block, self.relay_send.at[n], self.relay_recv.at[n], self.place.beside(onward)
        )
        copy.start()
        self.relay[n] = copy

    def arrive(self, n):
        if n in self.straight:
            for bit in self.place.bits:
                self.direct[n, bit].wait_recv()
            self.straight[n].wait_recv()
        elif len(self.place.bits) == 1:
            self.direct[n, 1].wait_recv()
        elif len(self.place.bits) == 2:
            self.direct[n, 1 if n % 2 == 0 else 2].wait_recv()
            self.relay[n].wait_recv()

    def finish(self):
        for copy in list(self.direct.values()) + list(self.relay.values()):
            copy.wait_send()


def contract(rows, weights, total, first):
    heads, depth, width = weights.shape
    step = min(512, depth)

    def body(i, carry):
        part = span(i * step, step)
        left = rows[:, part]
        for group in pairs(heads):
            right = jnp.concatenate([weights[j, part] for j in group], axis=1)
            columns = pl.ds(group[0] * width, len(group) * width)
            total[:, columns] += jnp.dot(left, right, preferred_element_type=F32)
        return carry

    if first:
        total[...] = jnp.zeros(total.shape, F32)
    lax.fori_loop(0, depth // step, body, 0)


def layer_kernel(
    input_ref,
    cotan_ref,
    route_ref,
    gate_ref,
    query_ref,
    output_ref,
    pair_ref,
    input_grad_out,
    kept_out,
    mats,
    own,
    far,
    own_sum,
    far_sum,
    q_got,
    da_low,
    da_got,
    queries,
    cotans,
    group_mats,
    keys,
    turned,
    turned_grads,
    core_got,
    grads_low,
    chip_got,
    pair_low,
    pair_got,
    every,
    made,
    hub,
    land,
    load_sem,
    weight_sem,
    x_send,
    x_recv,
    straight_send,
    straight_recv,
    direct_send,
    direct_recv,
    relay_send,
    relay_recv,
    sum_send,
    sum_recv,
    pair_send,
    pair_recv,
    trade_send,
    trade_recv,
    early_send,
    early_recv,
    share_send,
    share_recv,
    dq_send,
    dq_recv,
    dq_direct_send,
    dq_direct_recv,
    dq_relay_send,
    dq_relay_recv,
    late_send,
    late_recv,
    core_send,
    core_recv,
    chip_send,
    chip_recv,
    last_send,
    last_recv,
    made_send,
    made_recv,
    land_send,
    land_recv,
):
    me = Place()
    chips, chip, core, seat, group = me.chips, me.chip, me.core, me.seat, me.group
    heads, depth, width = query_ref.shape
    tokens = input_ref.shape[0]
    window = tokens * me.ctx_count
    half = 2 * depth
    piece = half // group
    family = me.head // group
    acts, sources = (input_ref, cotan_ref), (query_ref, output_ref)
    rows = tokens // SUBS
    part_rows = tokens // 2

    mine = span(core * depth, depth)
    loads = []
    for a in range(2):
        loads.append(local(sources[a], mats.at[a, :, mine], load_sem.at[a]))
        loads.append(local(acts[a].at[:, span(chip * half, half)], own.at[a], load_sem.at[2 + a]))

    places = me.friends()
    if group == 4:
        places.append((me.ctx, flip(flip(me.head, 1), 2)))
    homes = [lax.rem(family + i, chips) for i in range(1, chips)]
    places += [(me.ctx, home * group + seat) for home in homes]
    greet(places)

    order = [(a, hop, s) for a in range(2) for hop in range(1, chips) for s in range(SUBS)]

    def located(n, at):
        a, hop, s = order[n]
        return far.at[hop - 1, a, at, pl.ds(s * rows, rows)]

    crossing = []
    for n, (a, hop, s) in enumerate(order):
        begin = pl.multiple_of(me.other(hop) * half + seat * piece, piece)
        copy = remote(
            acts[a].at[pl.ds(s * rows, rows), pl.ds(begin, piece)],
            located(n, seat),
            x_send.at[n],
            x_recv.at[n],
            me.across(hop),
        )
        copy.start()
        crossing.append(copy)
    straight = {}
    for n, (a, hop, s) in enumerate(order):
        if group == 4 and a == 1 and s >= SUBS - STRAIGHT:
            at = flip(flip(seat, 1), 2)
            begin = pl.multiple_of(me.other(hop) * half + at * piece, piece)
            copy = remote(
                acts[a].at[pl.ds(s * rows, rows), pl.ds(begin, piece)],
                located(n, at),
                straight_send.at[len(straight)],
                straight_recv.at[len(straight)],
                me.across(hop),
            )
            copy.start()
            straight[n] = copy
    for copy in loads:
        copy.start()
    swaps = []
    for a in range(2):
        copy = remote(
            sources[a], mats.at[a, :, mine], weight_sem.at[a], weight_sem.at[2 + a], me.sibling
        )
        copy.start()
        swaps.append(copy)

    row = me.head % 2

    def key_block(which, at):
        return keys.at[which, span(at * tokens, tokens)]

    pair_copies = []
    for hop in range(1, chips):
        copy = remote(
            pair_ref.at[0],
            key_block(row, me.ctx),
            pair_send.at[hop],
            pair_recv.at[hop],
            me.across(hop),
        )
        copy.start()
        pair_copies.append(copy)
    keep = local(pair_ref.at[0], key_block(row, me.ctx), load_sem.at[4])
    keep.start()

    early = 1 if group == 4 else 0
    holder = core == seat // 2

    def ahead(bit):
        to = flip(seat, bit)
        begin = pl.multiple_of(to * piece - core * depth, piece)
        return remote(
            query_ref.at[pl.ds(0, early), pl.ds(begin, piece)],
            group_mats.at[seat, pl.ds(0, early)],
            early_send.at[bit],
            early_recv.at[bit],
            me.beside(bit),
        )

    def came_ahead(bit):
        return remote(
            group_mats.at[seat, pl.ds(0, early)],
            group_mats.at[flip(seat, bit), pl.ds(0, early)],
            early_send.at[bit],
            early_recv.at[bit],
            me.beside(bit),
        )

    def share_ahead(bit):
        block = group_mats.at[flip(seat, bit), pl.ds(0, early)]
        return remote(
            block, block, early_send.at[2 + bit], early_recv.at[2 + bit], me.sibling
        )

    def when_ahead(action):
        if early:
            pl.when(holder)(lambda: action(1))
            pl.when(jnp.logical_not(holder))(lambda: action(2))

    when_ahead(lambda bit: ahead(bit).start())

    spread = Spread(
        me, located, (direct_send, direct_recv, relay_send, relay_recv), straight.items()
    )

    def own_slice(a, i):
        part = pl.ds(i * piece, piece)
        contract(own.at[a, :, part], mats.at[a, :, part], own_sum.at[a], i == 0)

    seats = [seat] + [flip(seat, 1)] * (group > 1)
    if group == 4:
        seats += [flip(seat, 2), flip(flip(seat, 1), 2)]
    sums = {}

    def far_part(a, hop, p):
        block = pl.ds(p * part_rows, part_rows)
        for n, (b, by, s) in enumerate(order):
            if (b, by) == (a, hop) and s // (SUBS // 2) == p:
                spread.arrive(n)
        for i, at in enumerate(seats):
            part = span(at * piece, piece)
            contract(
                far.at[hop - 1, a, at, block],
                mats.at[a, :, part],
                far_sum.at[hop - 1, a, block],
                i == 0,
            )
        if a == 0:
            source, target = far_sum.at[hop - 1, 0, block], q_got.at[hop - 1, block]
        else:
            da_low[hop - 1, block] = far_sum[hop - 1, 1, block].astype(BF16)
            source, target = da_low.at[hop - 1, block], da_got.at[hop - 1, block]
        copy = remote(
            source,
            target,
            sum_send.at[a, hop - 1, p],
            sum_recv.at[a, hop - 1, p],
            (me.source(hop) * 2 + core, me.head),
        )
        copy.start()
        sums[a, hop, p] = copy

    own_work = [(a, i) for a in range(2) for i in range(group)]
    count = len(order)
    for n in range(count):
        crossing[n].wait_recv()
        spread.start(n)
        if n >= 1:
            spread.pass_on(n - 1)
        if n == 1:
            for copy in loads:
                copy.wait()
            for copy in swaps:
                copy.wait_recv()
        if n >= 2 and own_work:
            own_slice(*own_work.pop(0))
        if chips == 2 and n == count - 3:
            far_part(0, 1, 0)
        if chips == 2 and n == count - 1:
            far_part(0, 1, 1)
    spread.pass_on(count - 1)

    keep.wait()
    for copy in pair_copies:
        copy.wait_recv()
    pair_next = []
    for hop in range(chips):
        block = key_block(row, me.source(hop) * 2 + core)
        copy = remote(
            block, block, pair_send.at[chips + hop], pair_recv.at[chips + hop], me.beside(1)
        )
        copy.start()
        pair_next.append(copy)

    part_columns = piece // 2
    ours = span(core * part_columns, part_columns)
    trades = []

    def seat_of(j):
        at = seat + 0
        for bit in (1, 2):
            if j & bit:
                at = flip(at, bit)
        return at

    held_back = late_heads(heads, group)

    def trade(j, later, k):
        to = seat_of(j)
        copy = remote(
            mats.at[0, later, span(to * piece + core * part_columns, part_columns)],
            group_mats.at[seat, later, ours],
            trade_send.at[k],
            trade_recv.at[k],
            (me.ctx, me.head - seat + to),
        )
        copy.start()
        trades.append((j, later, copy))

    for j in range(1, group):
        skip = early if j < 3 else 0
        trade(j, pl.ds(skip, heads - skip - (held_back if j == 3 else 0)), j)

    def trade_rest():
        if held_back:
            trade(3, pl.ds(heads - held_back, held_back), 0)

    store = local(mats.at[0, :, span(seat * piece, piece)], group_mats.at[seat], load_sem.at[5])
    store.start()

    for work in own_work:
        own_slice(*work)
    for a in range(2):
        for p in range(2):
            for hop in range(1, chips):
                if (a, hop, p) not in sums:
                    far_part(a, hop, p)

    for copy in pair_next:
        copy.wait_recv()
    pair_last = []
    for hop in range(chips):
        for which in range(2):
            block = key_block(which, me.source(hop) * 2 + core)
            k = 2 * chips + 2 * hop + which
            copy = remote(block, block, pair_send.at[k], pair_recv.at[k], me.sibling)
            copy.start()
            pair_last.append(copy)

    lanes = []
    for j in range(heads - 1):
        named = route_ref[...] == me.head * (heads - 1) + j
        lanes.append(jnp.sum(jnp.where(named, gate_ref[...], 0.0), axis=0, keepdims=True))
    lanes.append(jnp.ones_like(lanes[0]))
    lanes += [jnp.zeros_like(lanes[0])] * (-heads % 8)
    token_gate = jnp.transpose(jnp.concatenate(lanes, axis=0))

    for hop in range(1, chips):
        for p in range(2):
            sums[0, hop, p].wait_recv()
    for j in range(heads):
        columns = pl.ds(j * width, width)
        value = own_sum[0, :, columns]
        for hop in range(1, chips):
            value = value + q_got[hop - 1, :, columns]
        queries[j] = value.astype(BF16)
    for copy in pair_last:
        copy.wait_recv()
    for which in range(2):
        for at in range(me.ctx_count):
            block = pl.ds(at * tokens, tokens)
            turned[which, :, block] = jnp.transpose(keys[which, block])
    for hop in range(1, chips):
        for p in range(2):
            sums[1, hop, p].wait_recv()
    for j in range(heads):
        columns = pl.ds(j * width, width)
        value = own_sum[1, :, columns]
        for hop in range(1, chips):
            value = value + da_got[hop - 1, :, columns].astype(F32)
        if j < heads - 1:
            value = value * token_gate[:, j : j + 1]
        cotans[j] = value.astype(BF16)

    late = late_heads(heads, group)
    soon = heads - late
    parts = part_count(chips)
    lines = tokens // parts
    units, late_units, soon_units, far_units = [], [], [], []
    for t in range(parts):
        late_units.append(range(len(units), len(units) + (late > 0)))
        units += [(t, 0, pl.ds(soon, late))] * (late > 0)
        soon_units.append(range(len(units), len(units) + 1))
        units.append((t, 0, pl.ds(0, soon)))
        far_units.append(range(len(units), len(units) + chips - 1))
        units += [(t, hop, pl.ds(0, soon)) for hop in range(1, chips)]

    def unit(n, at):
        t, hop, which = units[n]
        return every.at[me.source(hop), at, which, pl.ds(t * lines, lines)]

    dq_spread = Spread(
        me, unit, (dq_direct_send, dq_direct_recv, dq_relay_send, dq_relay_recv)
    )
    block_rows = min(part_rows, max(16, 256 * 1024 // window))
    scale = width ** (-0.5)
    turned_grads[...] = jnp.zeros(turned_grads.shape, F32)

    def attend(t, j):
        def body(i, carry):
            i = t * (part_rows // block_rows) + i
            block = span(i * block_rows, block_rows)
            query, cotan = queries[j, block], cotans[j, block]
            scores = jnp.dot(query, turned[0], preferred_element_type=F32) * scale
            first = me.ctx * tokens + i * block_rows
            place = first + lax.broadcasted_iota(jnp.int32, scores.shape, 0)
            scores = jnp.where(
                lax.broadcasted_iota(jnp.int32, scores.shape, 1) <= place, scores, -1e30
            )
            raised = jnp.exp(scores - jnp.max(scores, axis=1, keepdims=True))
            shares = raised / jnp.sum(raised, axis=1, keepdims=True)
            low = shares.astype(BF16)
            outputs = jnp.dot(low, keys[1], preferred_element_type=F32)
            share_grad = jnp.dot(cotan, turned[1], preferred_element_type=F32)
            delta = jnp.sum(cotan.astype(F32) * outputs, axis=1, keepdims=True)
            score_grad = (shares * (share_grad - delta) * scale).astype(BF16)
            every[chip, seat, j, block] = jnp.dot(
                score_grad, keys[0], preferred_element_type=F32
            ).astype(BF16)
            turned_grads[0] += jnp.dot(
                jnp.transpose(query), score_grad, preferred_element_type=F32
            )
            turned_grads[1] += jnp.dot(jnp.transpose(cotan), low, preferred_element_type=F32)
            return carry

        lax.fori_loop(0, part_rows // block_rows, body, 0)

    dq_copies, late_copies = {}, []

    def late_send_on(n, k):
        for hop in range(1, chips):
            block = unit(n, seats[k])
            m = len(late_copies)
            copy = remote(block, block, late_send.at[m], late_recv.at[m], me.across(hop))
            copy.start()
            late_copies.append((units[n][0], copy))

    def start_rest(t):
        for n in soon_units[t]:
            dq_spread.start(n)
        for n in far_units[t]:
            dq_copies[n].wait_recv()
            dq_spread.start(n)

    def start_late(t):
        if t < parts:
            for n in late_units[t]:
                dq_spread.start(n)

    def pass_late(t):
        if t < parts:
            for n in late_units[t]:
                dq_spread.pass_on(n)

    for p in range(2):
        these = range(p * parts // 2, (p + 1) * parts // 2)
        for j in range(soon, heads):
            attend(p, j)
        if p == 1:
            for n in far_units[0]:
                dq_copies[n].wait_recv()
                dq_spread.start(n)
            trade_rest()
        for t in these:
            for n in late_units[t]:
                late_send_on(n, 0)
        start_late(0) if p == 0 else pass_late(0)
        for j in range(soon):
            attend(p, j)
            if p == 1 and j == 0:
                start_late(1)
        for t in these:
            for n in soon_units[t]:
                for hop in range(1, chips):
                    m = far_units[t][hop - 1]
                    block = unit(n, seat)
                    k = t * (chips - 1) + hop - 1
                    copy = remote(block, block, dq_send.at[k], dq_recv.at[k], me.across(hop))
                    copy.start()
                    dq_copies[m] = copy
        if p == 0:
            for n in soon_units[0]:
                dq_spread.start(n)

    def column(at):
        return span(at * tokens, tokens)

    core_copies = []
    for hop in range(chips):
        spot = me.source(hop) * 2
        copy = remote(
            turned_grads.at[:, :, column(spot + 1 - core)],
            core_got.at[me.source(hop)],
            core_send.at[hop],
            core_recv.at[hop],
            me.sibling,
        )
        copy.start()
        core_copies.append(copy)
    kept_out[...] = jnp.zeros(kept_out.shape, F32)
    pair_low[...] = jnp.zeros(pair_low.shape, F32)
    for hop in range(chips):
        core_copies[hop].wait_recv()
        for which in range(2):
            both = (
                turned_grads[which, :, column(me.source(hop) * 2 + core)]
                + core_got[me.source(hop), which]
            )
            if hop:
                grads_low[hop - 1, which] = jnp.transpose(both).astype(BF16)
            else:
                kept_out[0] = jnp.where(row == which, jnp.transpose(both), kept_out[0])
                pair_low[...] = jnp.where(row == which, pair_low[...], jnp.transpose(both))
    chip_copies = []
    for hop in range(1, chips):
        copy = remote(
            grads_low.at[hop - 1],
            chip_got.at[hop - 1],
            chip_send.at[hop - 1],
            chip_recv.at[hop - 1],
            (me.source(hop) * 2 + core, me.head),
        )
        copy.start()
        chip_copies.append(copy)

    shares = []

    def share_trades(some):
        for j, later, copy in some:
            copy.wait_recv()
            block = group_mats.at[seat_of(j), later, ours]
            k = len(shares)
            share = remote(block, block, share_send.at[k], share_recv.at[k], me.sibling)
            share.start()
            shares.append(share)

    share_trades(trades[: group - 1])
    if early:

        @pl.when(holder)
        def _():
            for bit in (1, 2):
                came_ahead(bit).wait_recv()
                share_ahead(bit).start()

    def hand_round(t):
        if t + 1 < parts:
            start_rest(t + 1)
        for n in list(soon_units[t]) + list(far_units[t]):
            dq_spread.pass_on(n)
        start_late(t + 2)
        pass_late(t + 1)
        for n in late_units[t]:
            dq_spread.arrive(n)
            for k in range(1, group):
                late_send_on(n, k)

    hand_round(0)
    share_trades(trades[group - 1 :])

    store.wait()
    for copy in shares:
        copy.wait_recv()
    if early:

        @pl.when(jnp.logical_not(holder))
        def _():
            for bit in (1, 2):
                share_ahead(bit).wait_recv()

    step = min(512, piece) if chips <= 2 else min(256, piece)
    flat = [(m, j) for m in range(group) for j in range(heads)]

    def made_copy(hop, i):
        return remote(
            made.at[hop - 1, i],
            hub.at[chips - hop, i],
            made_send.at[hop - 1, i],
            made_recv.at[chips - hop - 1, i],
            (me.source(hop) * 2 + core, me.head),
        )

    def land_copy(hop, i):
        return remote(
            hub.at[hop, i],
            land.at[family, i],
            land_send.at[hop, i],
            land_recv.at[family, i],
            (me.ctx, me.source(hop) * group + seat),
        )

    def moves(hop):
        return me.source(hop) != family

    def multiply(t):
        block = pl.ds(t * lines, lines)

        def body(i, carry):
            part = span(i * step, step)
            total = jnp.zeros((chips * lines, step), F32)
            for k in range(0, len(flat), 2):
                both = flat[k : k + 2]
                left = jnp.concatenate(
                    [
                        jnp.concatenate([every[me.source(hop), m, j, block] for m, j in both], axis=1)
                        for hop in range(chips)
                    ],
                    axis=0,
                )
                right = jnp.concatenate([group_mats[m, j, part] for m, j in both], axis=1)
                total += lax.dot_general(
                    left, right, (((1,), (1,)), ((), ())), preferred_element_type=F32
                )
            for hop in range(chips):
                result = made.at[hop - 1] if hop else hub.at[0]
                result[t, :, part] = total[hop * lines : (hop + 1) * lines].astype(BF16)
            return carry

        lax.fori_loop(0, piece // step, body, 0)
        for hop in range(1, chips):
            made_copy(hop, t).start()
        pl.when(moves(0))(land_copy(0, t).start)

    def pass_made(t):
        for hop in range(1, chips):
            made_copy(chips - hop, t).wait_recv()
            pl.when(moves(hop))(land_copy(hop, t).start)

    def finish_part(t):
        for n in list(soon_units[t]) + list(far_units[t]):
            dq_spread.arrive(n)
        for when, copy in late_copies:
            if when == t:
                copy.wait_recv()
        multiply(t)

    hand_round(1)
    finish_part(0)
    for hop in range(1, chips):
        chip_copies[hop - 1].wait_recv()
        for which in range(2):
            value = chip_got[hop - 1, which].astype(F32)
            kept_out[0] += jnp.where(row == which, value, 0.0)
            pair_low[...] += jnp.where(row == which, 0.0, value)
    last_low = grads_low.at[chips - 1, 0]
    last_low[...] = pair_low[...].astype(BF16)
    last = remote(last_low, pair_got, last_send.at[0], last_recv.at[0], me.beside(1))

    last.start()
    for t in range(2, parts):
        hand_round(t)
        finish_part(t - 1)
        pass_made(t - 2)
    finish_part(parts - 1)
    pass_made(parts - 2)
    pass_made(parts - 1)

    last.wait()
    kept_out[0] += pair_got[...].astype(F32)

    stay = lax.rem(chip - family + chips, chips)
    for t in range(parts):
        total = hub[stay, t].astype(F32)
        for home in homes:
            arrival = remote(
                hub.at[0, t], land.at[home, t], land_send.at[0, t], land_recv.at[home, t], me.sibling
            )
            arrival.wait_recv()
            total = total + land[home, t].astype(F32)
        input_grad_out[pl.ds(t * lines, lines)] = total.astype(BF16)

    for hop in range(chips):
        for i in range(parts):
            if hop:
                made_copy(hop, i).wait_send()
            pl.when(moves(hop))(land_copy(hop, i).wait_send)
    for copy in crossing + swaps + pair_copies + pair_next + pair_last + shares:
        copy.wait_send()
    for copy in core_copies + chip_copies + list(straight.values()):
        copy.wait_send()
    for copy in list(sums.values()) + list(dq_copies.values()):
        copy.wait_send()
    for _, copy in late_copies:
        copy.wait_send()
    for _, _, copy in trades:
        copy.wait_send()
    when_ahead(lambda bit: ahead(bit).wait_send())
    if early:

        @pl.when(holder)
        def _():
            for bit in (1, 2):
                share_ahead(bit).wait_send()

    spread.finish()
    dq_spread.finish()


def per_device(
    layer_input, output_grad, routes, route_gates, query_weight, output_weight, key_values
):
    ctx_count, head_count = lax.axis_size("ctx"), lax.axis_size("head")
    chips = ctx_count // 2
    group, hops = head_count // chips, chips - 1
    heads, depth, width = query_weight.shape
    tokens = layer_input.shape[0]
    half = 2 * depth
    piece = half // group
    window = tokens * ctx_count
    count = 2 * hops * SUBS
    parts = part_count(chips)
    late = late_heads(heads, group)
    units, lines = parts * (chips + (late > 0)), tokens // parts
    return pl.pallas_call(
        layer_kernel,
        out_shape=(
            jax.ShapeDtypeStruct((tokens, piece), BF16),
            jax.ShapeDtypeStruct((1, tokens, width), F32),
        ),
        in_specs=[ANY, ANY, VMEM, VMEM, ANY, ANY, VMEM],
        out_specs=(VMEM, VMEM),
        scratch_shapes=[
            pltpu.VMEM((2, heads, half, width), BF16),
            pltpu.VMEM((2, tokens, half), BF16),
            pltpu.VMEM((hops, 2, group, tokens, piece), BF16),
            pltpu.VMEM((2, tokens, heads * width), F32),
            pltpu.VMEM((hops, 2, tokens, heads * width), F32),
            pltpu.VMEM((hops, tokens, heads * width), F32),
            pltpu.VMEM((hops, tokens, heads * width), BF16),
            pltpu.VMEM((hops, tokens, heads * width), BF16),
            pltpu.VMEM((heads, tokens, width), BF16),
            pltpu.VMEM((heads, tokens, width), BF16),
            pltpu.VMEM((group, heads, piece, width), BF16),
            pltpu.VMEM((2, window, width), BF16),
            pltpu.VMEM((2, width, window), BF16),
            pltpu.VMEM((2, width, window), F32),
            pltpu.VMEM((chips, 2, width, tokens), F32),
            pltpu.VMEM((chips, 2, tokens, width), BF16),
            pltpu.VMEM((hops, 2, tokens, width), BF16),
            pltpu.VMEM((tokens, width), F32),
            pltpu.VMEM((tokens, width), BF16),
            pltpu.VMEM((chips, group, heads, tokens, width), BF16),
            pltpu.VMEM((hops, parts, lines, piece), BF16),
            pltpu.VMEM((chips, parts, lines, piece), BF16),
            pltpu.VMEM((chips, parts, lines, piece), BF16),
            DMA((6,)),
            DMA((4,)),
        ]
        + [DMA((count,))] * 2
        + [DMA((hops * STRAIGHT,))] * 2
        + Spread.sems(count)
        + [DMA((2, hops, 2))] * 2
        + [DMA((4 * chips,))] * 2
        + [DMA((group,))] * 2
        + [DMA((5,))] * 2
        + [DMA((group,))] * 2
        + [DMA((parts * hops,))] * 2
        + Spread.sems(units)
        + [DMA((max(1, hops * parts * group * (late > 0)),))] * 2
        + [DMA((chips,))] * 2
        + [DMA((hops,))] * 2
        + [DMA((1,))] * 2
        + [DMA((hops, parts))] * 2
        + [DMA((chips, parts))] * 2,
        compiler_params=pltpu.CompilerParams(
            collective_id=0, has_side_effects=True, vmem_limit_bytes=VMEM_BYTES
        ),
    )(
        layer_input,
        output_grad,
        routes.T,
        route_gates.T,
        query_weight,
        output_weight,
        key_values,
    )


def solution(mesh):
    in_specs = (
        P("ctx", None),
        P("ctx", None),
        P("ctx", None),
        P("ctx", None),
        P("head", "ctx", None),
        P("head", "ctx", None),
        P("head", "ctx", None),
    )
    out_specs = (P("ctx", "head"), P("head", "ctx", None))
    return jax.shard_map(
        per_device, mesh=mesh, in_specs=in_specs, out_specs=out_specs, check_vma=False
    )
```

```python
import functools

import jax
import jax.numpy as jnp
from jax import lax
from jax.experimental import pallas as pl
from jax.experimental.pallas import tpu as pltpu
from jax.sharding import PartitionSpec as P

MESH = pl.DeviceIdType.MESH
ANY = pl.BlockSpec(memory_space=pl.ANY)
VMEM = pl.BlockSpec(memory_space=pltpu.VMEM)
DMA = pltpu.SemaphoreType.DMA
F32, BF16 = jnp.float32, jnp.bfloat16
SUBS = 4
STRAIGHT = 2
VMEM_BYTES = 67_043_328


def remote(source, target, send, recv, place):
    return pltpu.make_async_remote_copy(
        src_ref=source,
        dst_ref=target,
        send_sem=send,
        recv_sem=recv,
        device_id=place,
        device_id_type=MESH,
    )


def local(source, target, sem):
    return pltpu.make_async_copy(source, target, sem)


def greet(places):
    barrier = pltpu.get_barrier_semaphore()
    for place in places:
        pl.semaphore_signal(barrier, inc=1, device_id=place, device_id_type=MESH)
    pl.semaphore_wait(barrier, len(places))


def flip(index, bit):
    return index + bit - 2 * bit * ((index // bit) % 2)


def span(start, size):
    return pl.ds(pl.multiple_of(start, size), size)


def late_heads(heads, group):
    return 2 * heads // 5 if group == 4 else 0


def part_count(chips):
    return 4 if chips <= 2 else 2


def pairs(count):
    return [tuple(range(j, min(j + 2, count))) for j in range(0, count, 2)]


class Place:
    def __init__(self):
        self.ctx_count, self.head_count = lax.axis_size("ctx"), lax.axis_size("head")
        self.ctx, self.head = lax.axis_index("ctx"), lax.axis_index("head")
        self.chips = self.ctx_count // 2
        self.chip, self.core = self.ctx // 2, self.ctx % 2
        self.group = self.head_count // self.chips
        self.seat = self.head % self.group
        self.bits = [bit for bit in (1, 2) if bit < self.group]
        self.sibling = (self.ctx + 1 - 2 * self.core, self.head)

    def other(self, hop):
        return lax.rem(self.chip + hop, self.chips)

    def source(self, hop):
        return lax.rem(self.chip - hop + self.chips, self.chips)

    def across(self, hop):
        return (self.other(hop) * 2 + self.core, self.head)

    def beside(self, bit):
        return (self.ctx, flip(self.head, bit))

    def friends(self):
        hops = [self.across(hop) for hop in range(1, self.chips)]
        return hops + [self.beside(bit) for bit in self.bits] + [self.sibling]


class Spread:
    def __init__(self, place, located, sems, straight=(), onward=None):
        self.place, self.located = place, located
        self.onward = onward or (lambda n: 1 + n % 2)
        self.straight = dict(straight)
        self.direct_send, self.direct_recv, self.relay_send, self.relay_recv = sems
        self.direct, self.relay = {}, {}

    @staticmethod
    def sems(count):
        return [DMA((2, count))] * 2 + [DMA((count,))] * 2

    def start(self, n):
        for i, bit in enumerate(self.place.bits):
            block = self.located(n, self.place.seat)
            copy = remote(
                block,
                block,
                self.direct_send.at[i, n],
                self.direct_recv.at[i, n],
                self.place.beside(bit),
            )
            copy.start()
            self.direct[n, bit] = copy

    def pass_on(self, n):
        if len(self.place.bits) < 2 or n in self.straight:
            return
        onward = self.onward(n)
        came = 3 - onward
        self.direct[n, came].wait_recv()
        block = self.located(n, flip(self.place.seat, came))
        copy = remote(
            block, block, self.relay_send.at[n], self.relay_recv.at[n], self.place.beside(onward)
        )
        copy.start()
        self.relay[n] = copy

    def arrive(self, n):
        if n in self.straight:
            for bit in self.place.bits:
                self.direct[n, bit].wait_recv()
            self.straight[n].wait_recv()
        elif len(self.place.bits) == 1:
            self.direct[n, 1].wait_recv()
        elif len(self.place.bits) == 2:
            self.direct[n, self.onward(n)].wait_recv()
            self.relay[n].wait_recv()

    def finish(self):
        for copy in list(self.direct.values()) + list(self.relay.values()):
            copy.wait_send()


def contract(rows, weights, total, first):
    heads, depth, width = weights.shape
    step = min(512, depth)

    def body(i, carry):
        part = span(i * step, step)
        left = rows[:, part]
        for group in pairs(heads):
            right = jnp.concatenate([weights[j, part] for j in group], axis=1)
            columns = pl.ds(group[0] * width, len(group) * width)
            total[:, columns] += jnp.dot(left, right, preferred_element_type=F32)
        return carry

    if first:
        total[...] = jnp.zeros(total.shape, F32)
    lax.fori_loop(0, depth // step, body, 0)


def layer_kernel(
    input_ref,
    cotan_ref,
    route_ref,
    gate_ref,
    query_ref,
    output_ref,
    pair_ref,
    input_grad_out,
    kept_out,
    other_out,
    mats,
    own,
    far,
    own_sum,
    far_sum,
    q_got,
    da_low,
    da_got,
    queries,
    cotans,
    group_mats,
    keys,
    turned,
    turned_grads,
    core_got,
    grads_low,
    chip_got,
    pair_low,
    pair_got,
    every,
    made,
    hub,
    land,
    load_sem,
    weight_sem,
    x_send,
    x_recv,
    straight_send,
    straight_recv,
    direct_send,
    direct_recv,
    relay_send,
    relay_recv,
    sum_send,
    sum_recv,
    pair_send,
    pair_recv,
    trade_send,
    trade_recv,
    early_send,
    early_recv,
    share_send,
    share_recv,
    dq_send,
    dq_recv,
    dq_direct_send,
    dq_direct_recv,
    dq_relay_send,
    dq_relay_recv,
    late_send,
    late_recv,
    core_send,
    core_recv,
    chip_send,
    chip_recv,
    last_send,
    last_recv,
    made_send,
    made_recv,
    land_send,
    land_recv,
):
    me = Place()
    chips, chip, core, seat, group = me.chips, me.chip, me.core, me.seat, me.group
    heads, depth, width = query_ref.shape
    tokens = input_ref.shape[0]
    window = tokens * me.ctx_count
    half = 2 * depth
    piece = half // group
    family = me.head // group
    acts, sources = (input_ref, cotan_ref), (query_ref, output_ref)
    rows = tokens // SUBS
    part_rows = tokens // 2

    mine = span(core * depth, depth)
    loads = []
    for a in range(2):
        loads.append(local(sources[a], mats.at[a, :, mine], load_sem.at[a]))
        loads.append(local(acts[a].at[:, span(chip * half, half)], own.at[a], load_sem.at[2 + a]))

    places = me.friends()
    if group == 4:
        places.append((me.ctx, flip(flip(me.head, 1), 2)))
    homes = [lax.rem(family + i, chips) for i in range(1, chips)]
    places += [(me.ctx, home * group + seat) for home in homes]
    greet(places)

    order = [(a, hop, s) for a in range(2) for hop in range(1, chips) for s in range(SUBS)]

    def located(n, at):
        a, hop, s = order[n]
        return far.at[hop - 1, a, at, pl.ds(s * rows, rows)]

    crossing = []
    for n, (a, hop, s) in enumerate(order):
        begin = pl.multiple_of(me.other(hop) * half + seat * piece, piece)
        copy = remote(
            acts[a].at[pl.ds(s * rows, rows), pl.ds(begin, piece)],
            located(n, seat),
            x_send.at[n],
            x_recv.at[n],
            me.across(hop),
        )
        copy.start()
        crossing.append(copy)
    straight = {}
    for n, (a, hop, s) in enumerate(order):
        if group == 4 and a == 1 and s >= SUBS - STRAIGHT:
            at = flip(flip(seat, 1), 2)
            begin = pl.multiple_of(me.other(hop) * half + at * piece, piece)
            copy = remote(
                acts[a].at[pl.ds(s * rows, rows), pl.ds(begin, piece)],
                located(n, at),
                straight_send.at[len(straight)],
                straight_recv.at[len(straight)],
                me.across(hop),
            )
            copy.start()
            straight[n] = copy
    for copy in loads:
        copy.start()
    swaps = []
    for a in range(2):
        copy = remote(
            sources[a], mats.at[a, :, mine], weight_sem.at[a], weight_sem.at[2 + a], me.sibling
        )
        copy.start()
        swaps.append(copy)

    row = me.head % 2

    def key_block(which, at):
        return keys.at[which, span(at * tokens, tokens)]

    pair_copies = []
    for hop in range(1, chips):
        copy = remote(
            pair_ref.at[0],
            key_block(row, me.ctx),
            pair_send.at[hop],
            pair_recv.at[hop],
            me.across(hop),
        )
        copy.start()
        pair_copies.append(copy)
    keep = local(pair_ref.at[0], key_block(row, me.ctx), load_sem.at[4])
    keep.start()

    early = 2 if group == 4 else 0
    holder = core == seat // 2

    def ahead(bit):
        to = flip(seat, bit)
        begin = pl.multiple_of(to * piece - core * depth, piece)
        return remote(
            query_ref.at[pl.ds(0, early), pl.ds(begin, piece)],
            group_mats.at[seat, pl.ds(0, early)],
            early_send.at[bit],
            early_recv.at[bit],
            me.beside(bit),
        )

    def came_ahead(bit):
        return remote(
            group_mats.at[seat, pl.ds(0, early)],
            group_mats.at[flip(seat, bit), pl.ds(0, early)],
            early_send.at[bit],
            early_recv.at[bit],
            me.beside(bit),
        )

    def share_ahead(bit):
        block = group_mats.at[flip(seat, bit), pl.ds(0, early)]
        return remote(
            block, block, early_send.at[2 + bit], early_recv.at[2 + bit], me.sibling
        )

    def when_ahead(action):
        if early:
            pl.when(holder)(lambda: action(1))
            pl.when(jnp.logical_not(holder))(lambda: action(2))

    when_ahead(lambda bit: ahead(bit).start())

    spread = Spread(
        me, located, (direct_send, direct_recv, relay_send, relay_recv), straight.items()
    )

    def own_slice(a, i):
        part = pl.ds(i * piece, piece)
        contract(own.at[a, :, part], mats.at[a, :, part], own_sum.at[a], i == 0)

    seats = [seat] + [flip(seat, 1)] * (group > 1)
    if group == 4:
        seats += [flip(seat, 2), flip(flip(seat, 1), 2)]
    sums = {}

    def far_part(a, hop, p):
        block = pl.ds(p * part_rows, part_rows)
        for n, (b, by, s) in enumerate(order):
            if (b, by) == (a, hop) and s // (SUBS // 2) == p:
                spread.arrive(n)
        for i, at in enumerate(seats):
            part = span(at * piece, piece)
            contract(
                far.at[hop - 1, a, at, block],
                mats.at[a, :, part],
                far_sum.at[hop - 1, a, block],
                i == 0,
            )
        if a == 0:
            source, target = far_sum.at[hop - 1, 0, block], q_got.at[hop - 1, block]
        else:
            da_low[hop - 1, block] = far_sum[hop - 1, 1, block].astype(BF16)
            source, target = da_low.at[hop - 1, block], da_got.at[hop - 1, block]
        copy = remote(
            source,
            target,
            sum_send.at[a, hop - 1, p],
            sum_recv.at[a, hop - 1, p],
            (me.source(hop) * 2 + core, me.head),
        )
        copy.start()
        sums[a, hop, p] = copy

    own_work = [(a, i) for a in range(2) for i in range(group)]
    count = len(order)
    for n in range(count):
        crossing[n].wait_recv()
        spread.start(n)
        if n >= 1:
            spread.pass_on(n - 1)
        if n == 1:
            for copy in loads:
                copy.wait()
            for copy in swaps:
                copy.wait_recv()
        if n >= 2 and own_work:
            own_slice(*own_work.pop(0))
        if chips == 2 and n == count - 3:
            far_part(0, 1, 0)
        if chips == 2 and n == count - 1:
            far_part(0, 1, 1)
    spread.pass_on(count - 1)

    keep.wait()
    for copy in pair_copies:
        copy.wait_recv()
    pair_next = []
    for hop in range(chips):
        block = key_block(row, me.source(hop) * 2 + core)
        copy = remote(
            block, block, pair_send.at[chips + hop], pair_recv.at[chips + hop], me.beside(1)
        )
        copy.start()
        pair_next.append(copy)

    part_columns = piece // 2
    ours = span(core * part_columns, part_columns)
    trades = []

    def seat_of(j):
        at = seat + 0
        for bit in (1, 2):
            if j & bit:
                at = flip(at, bit)
        return at

    held_back = late_heads(heads, group)

    def trade(j, later, k):
        to = seat_of(j)
        copy = remote(
            mats.at[0, later, span(to * piece + core * part_columns, part_columns)],
            group_mats.at[seat, later, ours],
            trade_send.at[k],
            trade_recv.at[k],
            (me.ctx, me.head - seat + to),
        )
        copy.start()
        trades.append((j, later, copy))

    for j in range(1, group):
        skip = early if j < 3 else 0
        trade(j, pl.ds(skip, heads - skip - (held_back if j == 3 else 0)), j)

    def trade_rest():
        if held_back:
            trade(3, pl.ds(heads - held_back, held_back), 0)

    store = local(mats.at[0, :, span(seat * piece, piece)], group_mats.at[seat], load_sem.at[5])
    store.start()

    for work in own_work:
        own_slice(*work)
    for a in range(2):
        for p in range(2):
            for hop in range(1, chips):
                if (a, hop, p) not in sums:
                    far_part(a, hop, p)

    for copy in pair_next:
        copy.wait_recv()
    pair_last = []
    for hop in range(chips):
        for which in range(2):
            block = key_block(which, me.source(hop) * 2 + core)
            k = 2 * chips + 2 * hop + which
            copy = remote(block, block, pair_send.at[k], pair_recv.at[k], me.sibling)
            copy.start()
            pair_last.append(copy)

    lanes = []
    for j in range(heads - 1):
        named = route_ref[...] == me.head * (heads - 1) + j
        lanes.append(jnp.sum(jnp.where(named, gate_ref[...], 0.0), axis=0, keepdims=True))
    lanes.append(jnp.ones_like(lanes[0]))
    lanes += [jnp.zeros_like(lanes[0])] * (-heads % 8)
    token_gate = jnp.transpose(jnp.concatenate(lanes, axis=0))

    for hop in range(1, chips):
        for p in range(2):
            sums[0, hop, p].wait_recv()
    for j in range(heads):
        columns = pl.ds(j * width, width)
        value = own_sum[0, :, columns]
        for hop in range(1, chips):
            value = value + q_got[hop - 1, :, columns]
        queries[j] = value.astype(BF16)
    for copy in pair_last:
        copy.wait_recv()
    for which in range(2):
        for at in range(me.ctx_count):
            block = pl.ds(at * tokens, tokens)
            turned[which, :, block] = jnp.transpose(keys[which, block])
    for hop in range(1, chips):
        for p in range(2):
            sums[1, hop, p].wait_recv()
    for j in range(heads):
        columns = pl.ds(j * width, width)
        value = own_sum[1, :, columns]
        for hop in range(1, chips):
            value = value + da_got[hop - 1, :, columns].astype(F32)
        if j < heads - 1:
            value = value * token_gate[:, j : j + 1]
        cotans[j] = value.astype(BF16)

    late = late_heads(heads, group)
    soon = heads - late
    parts = part_count(chips)
    lines = tokens // parts
    units, late_units, soon_units, far_units = [], [], [], []
    for t in range(parts):
        late_units.append(range(len(units), len(units) + (late > 0)))
        units += [(t, 0, pl.ds(soon, late))] * (late > 0)
        soon_units.append(range(len(units), len(units) + 1))
        units.append((t, 0, pl.ds(0, soon)))
        far_units.append(range(len(units), len(units) + chips - 1))
        units += [(t, hop, pl.ds(0, soon)) for hop in range(1, chips)]

    def unit(n, at):
        t, hop, which = units[n]
        return every.at[me.source(hop), at, which, pl.ds(t * lines, lines)]

    def dq_onward(n):
        return 1 + n % 2 if units[n][0] < 2 else 1

    dq_spread = Spread(
        me, unit, (dq_direct_send, dq_direct_recv, dq_relay_send, dq_relay_recv), onward=dq_onward
    )
    block_rows = min(part_rows, max(16, 256 * 1024 // window))
    scale = width ** (-0.5)
    turned_grads[...] = jnp.zeros(turned_grads.shape, F32)

    def attend(t, j):
        def body(i, carry):
            i = t * (part_rows // block_rows) + i
            block = span(i * block_rows, block_rows)
            query, cotan = queries[j, block], cotans[j, block]
            scores = jnp.dot(query, turned[0], preferred_element_type=F32) * scale
            first = me.ctx * tokens + i * block_rows
            place = first + lax.broadcasted_iota(jnp.int32, scores.shape, 0)
            scores = jnp.where(
                lax.broadcasted_iota(jnp.int32, scores.shape, 1) <= place, scores, -1e30
            )
            raised = jnp.exp(scores - jnp.max(scores, axis=1, keepdims=True))
            shares = raised / jnp.sum(raised, axis=1, keepdims=True)
            low = shares.astype(BF16)
            outputs = jnp.dot(low, keys[1], preferred_element_type=F32)
            share_grad = jnp.dot(cotan, turned[1], preferred_element_type=F32)
            delta = jnp.sum(cotan.astype(F32) * outputs, axis=1, keepdims=True)
            score_grad = (shares * (share_grad - delta) * scale).astype(BF16)
            every[chip, seat, j, block] = jnp.dot(
                score_grad, keys[0], preferred_element_type=F32
            ).astype(BF16)
            turned_grads[0] += jnp.dot(
                jnp.transpose(query), score_grad, preferred_element_type=F32
            )
            turned_grads[1] += jnp.dot(jnp.transpose(cotan), low, preferred_element_type=F32)
            return carry

        lax.fori_loop(0, part_rows // block_rows, body, 0)

    dq_copies, late_copies = {}, []

    def late_send_on(n, k):
        for hop in range(1, chips):
            block = unit(n, seats[k])
            m = len(late_copies)
            copy = remote(block, block, late_send.at[m], late_recv.at[m], me.across(hop))
            copy.start()
            late_copies.append((units[n][0], copy))

    def start_rest(t):
        for n in soon_units[t]:
            dq_spread.start(n)
        for n in far_units[t]:
            dq_copies[n].wait_recv()
            dq_spread.start(n)

    def start_late(t):
        if t < parts:
            for n in late_units[t]:
                dq_spread.start(n)

    def pass_late(t):
        if t < parts:
            for n in late_units[t]:
                dq_spread.pass_on(n)

    for p in range(2):
        these = range(p * parts // 2, (p + 1) * parts // 2)
        for j in range(soon, heads):
            attend(p, j)
        if p == 1:
            for n in far_units[0]:
                dq_copies[n].wait_recv()
                dq_spread.start(n)
            trade_rest()
        for t in these:
            for n in late_units[t]:
                late_send_on(n, 0)
        start_late(0) if p == 0 else pass_late(0)
        for j in range(soon):
            attend(p, j)
            if p == 1 and j == 0:
                start_late(1)
        for t in these:
            for n in soon_units[t]:
                for hop in range(1, chips):
                    m = far_units[t][hop - 1]
                    block = unit(n, seat)
                    k = t * (chips - 1) + hop - 1
                    copy = remote(block, block, dq_send.at[k], dq_recv.at[k], me.across(hop))
                    copy.start()
                    dq_copies[m] = copy
        if p == 0:
            for n in soon_units[0]:
                dq_spread.start(n)

    def column(at):
        return span(at * tokens, tokens)

    core_copies = []
    for hop in range(chips):
        spot = me.source(hop) * 2
        copy = remote(
            turned_grads.at[:, :, column(spot + 1 - core)],
            core_got.at[me.source(hop)],
            core_send.at[hop],
            core_recv.at[hop],
            me.sibling,
        )
        copy.start()
        core_copies.append(copy)
    kept_out[...] = jnp.zeros(kept_out.shape, F32)
    pair_low[...] = jnp.zeros(pair_low.shape, F32)
    for hop in range(chips):
        core_copies[hop].wait_recv()
        for which in range(2):
            both = (
                turned_grads[which, :, column(me.source(hop) * 2 + core)]
                + core_got[me.source(hop), which]
            )
            if hop:
                grads_low[hop - 1, which] = jnp.transpose(both).astype(BF16)
            else:
                kept_out[0] = jnp.where(row == which, jnp.transpose(both), kept_out[0])
                pair_low[...] = jnp.where(row == which, pair_low[...], jnp.transpose(both))
    chip_copies = []
    for hop in range(1, chips):
        copy = remote(
            grads_low.at[hop - 1],
            chip_got.at[hop - 1],
            chip_send.at[hop - 1],
            chip_recv.at[hop - 1],
            (me.source(hop) * 2 + core, me.head),
        )
        copy.start()
        chip_copies.append(copy)

    shares = []

    def share_trades(some):
        for j, later, copy in some:
            copy.wait_recv()
            block = group_mats.at[seat_of(j), later, ours]
            k = len(shares)
            share = remote(block, block, share_send.at[k], share_recv.at[k], me.sibling)
            share.start()
            shares.append(share)

    share_trades(trades[: group - 1])
    if early:

        @pl.when(holder)
        def _():
            for bit in (1, 2):
                came_ahead(bit).wait_recv()
                share_ahead(bit).start()

    def hand_round(t):
        if t + 1 < parts:
            start_rest(t + 1)
        for n in list(soon_units[t]) + list(far_units[t]):
            dq_spread.pass_on(n)
        start_late(t + 2)
        pass_late(t + 1)
        if t == 0:
            share_trades(trades[group - 1 :])
        for n in late_units[t]:
            dq_spread.arrive(n)
            for k in range(1, group):
                late_send_on(n, k)

    hand_round(0)

    step = min(512, piece) if chips <= 2 else min(256, piece)
    flat = [(m, j) for m in range(group) for j in range(heads)]

    def made_copy(hop, i):
        return remote(
            made.at[hop - 1, i],
            hub.at[chips - hop, i],
            made_send.at[hop - 1, i],
            made_recv.at[chips - hop - 1, i],
            (me.source(hop) * 2 + core, me.head),
        )

    def land_copy(hop, i):
        return remote(
            hub.at[hop, i],
            land.at[family, i],
            land_send.at[hop, i],
            land_recv.at[family, i],
            (me.ctx, me.source(hop) * group + seat),
        )

    def moves(hop):
        return me.source(hop) != family

    def multiply(t):
        block = pl.ds(t * lines, lines)

        def body(i, carry):
            part = span(i * step, step)
            total = jnp.zeros((chips * lines, step), F32)
            for k in range(0, len(flat), 2):
                both = flat[k : k + 2]
                left = jnp.concatenate(
                    [
                        jnp.concatenate([every[me.source(hop), m, j, block] for m, j in both], axis=1)
                        for hop in range(chips)
                    ],
                    axis=0,
                )
                right = jnp.concatenate([group_mats[m, j, part] for m, j in both], axis=1)
                total += lax.dot_general(
                    left, right, (((1,), (1,)), ((), ())), preferred_element_type=F32
                )
            for hop in range(chips):
                result = made.at[hop - 1] if hop else hub.at[0]
                result[t, :, part] = total[hop * lines : (hop + 1) * lines].astype(BF16)
            return carry

        lax.fori_loop(0, piece // step, body, 0)
        for hop in range(1, chips):
            made_copy(hop, t).start()
        pl.when(moves(0))(land_copy(0, t).start)

    def pass_made(t):
        for hop in range(1, chips):
            made_copy(chips - hop, t).wait_recv()
            pl.when(moves(hop))(land_copy(hop, t).start)

    def finish_part(t):
        for n in list(soon_units[t]) + list(far_units[t]):
            dq_spread.arrive(n)
        for when, copy in late_copies:
            if when == t:
                copy.wait_recv()
        multiply(t)

    hand_round(1)
    store.wait()
    for copy in shares:
        copy.wait_recv()
    if early:

        @pl.when(jnp.logical_not(holder))
        def _():
            for bit in (1, 2):
                share_ahead(bit).wait_recv()
    finish_part(0)
    for hop in range(1, chips):
        chip_copies[hop - 1].wait_recv()
        for which in range(2):
            value = chip_got[hop - 1, which].astype(F32)
            kept_out[0] += jnp.where(row == which, value, 0.0)
            pair_low[...] += jnp.where(row == which, 0.0, value)
    last_low = grads_low.at[chips - 1, 0]
    last_low[...] = pair_low[...].astype(BF16)
    last = remote(last_low, pair_got, last_send.at[0], last_recv.at[0], me.beside(1))

    last.start()
    for t in range(2, parts):
        hand_round(t)
        finish_part(t - 1)
        pass_made(t - 2)
    finish_part(parts - 1)
    pass_made(parts - 2)
    pass_made(parts - 1)

    last.wait()
    other_out[...] = pair_got[...]

    stay = lax.rem(chip - family + chips, chips)
    for t in range(parts):
        total = hub[stay, t].astype(F32)
        for home in homes:
            arrival = remote(
                hub.at[0, t], land.at[home, t], land_send.at[0, t], land_recv.at[home, t], me.sibling
            )
            arrival.wait_recv()
            total = total + land[home, t].astype(F32)
        input_grad_out[pl.ds(t * lines, lines)] = total.astype(BF16)

    for hop in range(chips):
        for i in range(parts):
            if hop:
                made_copy(hop, i).wait_send()
            pl.when(moves(hop))(land_copy(hop, i).wait_send)
    for copy in crossing + swaps + pair_copies + pair_next + pair_last + shares:
        copy.wait_send()
    for copy in core_copies + chip_copies + list(straight.values()):
        copy.wait_send()
    for copy in list(sums.values()) + list(dq_copies.values()):
        copy.wait_send()
    for _, copy in late_copies:
        copy.wait_send()
    for _, _, copy in trades:
        copy.wait_send()
    when_ahead(lambda bit: ahead(bit).wait_send())
    if early:

        @pl.when(holder)
        def _():
            for bit in (1, 2):
                share_ahead(bit).wait_send()

    spread.finish()
    dq_spread.finish()


def settle_kernel(grad_ref, kept_ref, rest_ref, grad_out, kept_out):
    grad_out[...] = grad_ref[...]
    kept_out[0] = kept_ref[0] + rest_ref[...].astype(F32)


def per_device(
    layer_input, output_grad, routes, route_gates, query_weight, output_weight, key_values
):
    ctx_count, head_count = lax.axis_size("ctx"), lax.axis_size("head")
    chips = ctx_count // 2
    group, hops = head_count // chips, chips - 1
    heads, depth, width = query_weight.shape
    tokens = layer_input.shape[0]
    half = 2 * depth
    piece = half // group
    window = tokens * ctx_count
    count = 2 * hops * SUBS
    parts = part_count(chips)
    late = late_heads(heads, group)
    units, lines = parts * (chips + (late > 0)), tokens // parts
    grad, kept, rest = pl.pallas_call(
        layer_kernel,
        out_shape=(
            jax.ShapeDtypeStruct((tokens, piece), BF16),
            jax.ShapeDtypeStruct((1, tokens, width), F32),
            jax.ShapeDtypeStruct((tokens, width), BF16),
        ),
        in_specs=[ANY, ANY, VMEM, VMEM, ANY, ANY, VMEM],
        out_specs=(VMEM, VMEM, VMEM),
        scratch_shapes=[
            pltpu.VMEM((2, heads, half, width), BF16),
            pltpu.VMEM((2, tokens, half), BF16),
            pltpu.VMEM((hops, 2, group, tokens, piece), BF16),
            pltpu.VMEM((2, tokens, heads * width), F32),
            pltpu.VMEM((hops, 2, tokens, heads * width), F32),
            pltpu.VMEM((hops, tokens, heads * width), F32),
            pltpu.VMEM((hops, tokens, heads * width), BF16),
            pltpu.VMEM((hops, tokens, heads * width), BF16),
            pltpu.VMEM((heads, tokens, width), BF16),
            pltpu.VMEM((heads, tokens, width), BF16),
            pltpu.VMEM((group, heads, piece, width), BF16),
            pltpu.VMEM((2, window, width), BF16),
            pltpu.VMEM((2, width, window), BF16),
            pltpu.VMEM((2, width, window), F32),
            pltpu.VMEM((chips, 2, width, tokens), F32),
            pltpu.VMEM((chips, 2, tokens, width), BF16),
            pltpu.VMEM((hops, 2, tokens, width), BF16),
            pltpu.VMEM((tokens, width), F32),
            pltpu.VMEM((tokens, width), BF16),
            pltpu.VMEM((chips, group, heads, tokens, width), BF16),
            pltpu.VMEM((hops, parts, lines, piece), BF16),
            pltpu.VMEM((chips, parts, lines, piece), BF16),
            pltpu.VMEM((chips, parts, lines, piece), BF16),
            DMA((6,)),
            DMA((4,)),
        ]
        + [DMA((count,))] * 2
        + [DMA((hops * STRAIGHT,))] * 2
        + Spread.sems(count)
        + [DMA((2, hops, 2))] * 2
        + [DMA((4 * chips,))] * 2
        + [DMA((group,))] * 2
        + [DMA((5,))] * 2
        + [DMA((group,))] * 2
        + [DMA((parts * hops,))] * 2
        + Spread.sems(units)
        + [DMA((max(1, hops * parts * group * (late > 0)),))] * 2
        + [DMA((chips,))] * 2
        + [DMA((hops,))] * 2
        + [DMA((1,))] * 2
        + [DMA((hops, parts))] * 2
        + [DMA((chips, parts))] * 2,
        compiler_params=pltpu.CompilerParams(
            collective_id=0, has_side_effects=True, vmem_limit_bytes=VMEM_BYTES
        ),
    )(
        layer_input,
        output_grad,
        routes.T,
        route_gates.T,
        query_weight,
        output_weight,
        key_values,
    )
    return pl.pallas_call(
        settle_kernel,
        out_shape=(
            jax.ShapeDtypeStruct(grad.shape, grad.dtype),
            jax.ShapeDtypeStruct(kept.shape, kept.dtype),
        ),
        in_specs=[VMEM] * 3,
        out_specs=(VMEM, VMEM),
    )(grad, kept, rest)


def solution(mesh):
    in_specs = (
        P("ctx", None),
        P("ctx", None),
        P("ctx", None),
        P("ctx", None),
        P("head", "ctx", None),
        P("head", "ctx", None),
        P("head", "ctx", None),
    )
    out_specs = (P("ctx", "head"), P("head", "ctx", None))
    return jax.shard_map(
        per_device, mesh=mesh, in_specs=in_specs, out_specs=out_specs, check_vma=False
    )
```

```python
import functools

import jax
import jax.numpy as jnp
from jax import lax
from jax.experimental import pallas as pl
from jax.experimental.pallas import tpu as pltpu
from jax.sharding import PartitionSpec as P

MESH = pl.DeviceIdType.MESH
ANY = pl.BlockSpec(memory_space=pl.ANY)
VMEM = pl.BlockSpec(memory_space=pltpu.VMEM)
DMA = pltpu.SemaphoreType.DMA
F32, BF16 = jnp.float32, jnp.bfloat16
SUBS = 4
STRAIGHT = 2
VMEM_BYTES = 67_043_328


def remote(source, target, send, recv, place):
    return pltpu.make_async_remote_copy(
        src_ref=source,
        dst_ref=target,
        send_sem=send,
        recv_sem=recv,
        device_id=place,
        device_id_type=MESH,
    )


def local(source, target, sem):
    return pltpu.make_async_copy(source, target, sem)


def greet(places):
    barrier = pltpu.get_barrier_semaphore()
    for place in places:
        pl.semaphore_signal(barrier, inc=1, device_id=place, device_id_type=MESH)
    pl.semaphore_wait(barrier, len(places))


def flip(index, bit):
    return index + bit - 2 * bit * ((index // bit) % 2)


def span(start, size):
    return pl.ds(pl.multiple_of(start, size), size)


def late_heads(heads, group):
    return 2 * heads // 5 if group == 4 else 0


def part_count(chips):
    return 4 if chips <= 2 else 2


def pairs(count):
    return [tuple(range(j, min(j + 2, count))) for j in range(0, count, 2)]


class Place:
    def __init__(self):
        self.ctx_count, self.head_count = lax.axis_size("ctx"), lax.axis_size("head")
        self.ctx, self.head = lax.axis_index("ctx"), lax.axis_index("head")
        self.chips = self.ctx_count // 2
        self.chip, self.core = self.ctx // 2, self.ctx % 2
        self.group = self.head_count // self.chips
        self.seat = self.head % self.group
        self.bits = [bit for bit in (1, 2) if bit < self.group]
        self.sibling = (self.ctx + 1 - 2 * self.core, self.head)

    def other(self, hop):
        return lax.rem(self.chip + hop, self.chips)

    def source(self, hop):
        return lax.rem(self.chip - hop + self.chips, self.chips)

    def across(self, hop):
        return (self.other(hop) * 2 + self.core, self.head)

    def beside(self, bit):
        return (self.ctx, flip(self.head, bit))

    def friends(self):
        hops = [self.across(hop) for hop in range(1, self.chips)]
        return hops + [self.beside(bit) for bit in self.bits] + [self.sibling]


class Spread:
    def __init__(self, place, located, sems, straight=(), onward=None):
        self.place, self.located = place, located
        self.onward = onward or (lambda n: 1 + n % 2)
        self.straight = dict(straight)
        self.direct_send, self.direct_recv, self.relay_send, self.relay_recv = sems
        self.direct, self.relay = {}, {}

    @staticmethod
    def sems(count):
        return [DMA((2, count))] * 2 + [DMA((count,))] * 2

    def start(self, n):
        for i, bit in enumerate(self.place.bits):
            block = self.located(n, self.place.seat)
            copy = remote(
                block,
                block,
                self.direct_send.at[i, n],
                self.direct_recv.at[i, n],
                self.place.beside(bit),
            )
            copy.start()
            self.direct[n, bit] = copy

    def pass_on(self, n):
        if len(self.place.bits) < 2 or n in self.straight:
            return
        onward = self.onward(n)
        came = 3 - onward
        self.direct[n, came].wait_recv()
        block = self.located(n, flip(self.place.seat, came))
        copy = remote(
            block, block, self.relay_send.at[n], self.relay_recv.at[n], self.place.beside(onward)
        )
        copy.start()
        self.relay[n] = copy

    def arrive(self, n):
        if n in self.straight:
            for bit in self.place.bits:
                self.direct[n, bit].wait_recv()
            self.straight[n].wait_recv()
        elif len(self.place.bits) == 1:
            self.direct[n, 1].wait_recv()
        elif len(self.place.bits) == 2:
            self.direct[n, self.onward(n)].wait_recv()
            self.relay[n].wait_recv()

    def finish(self):
        for copy in list(self.direct.values()) + list(self.relay.values()):
            copy.wait_send()


def contract(rows, weights, total, first):
    heads, depth, width = weights.shape
    step = min(512, depth)

    def body(i, carry):
        part = span(i * step, step)
        left = rows[:, part]
        for group in pairs(heads):
            right = jnp.concatenate([weights[j, part] for j in group], axis=1)
            columns = pl.ds(group[0] * width, len(group) * width)
            total[:, columns] += jnp.dot(left, right, preferred_element_type=F32)
        return carry

    if first:
        total[...] = jnp.zeros(total.shape, F32)
    lax.fori_loop(0, depth // step, body, 0)


def layer_kernel(
    input_ref,
    cotan_ref,
    route_ref,
    gate_ref,
    query_ref,
    output_ref,
    pair_ref,
    input_grad_out,
    kept_out,
    other_out,
    mats,
    own,
    far,
    own_sum,
    far_sum,
    q_got,
    da_low,
    da_got,
    queries,
    cotans,
    group_mats,
    keys,
    turned,
    turned_grads,
    core_got,
    grads_low,
    chip_got,
    pair_low,
    pair_got,
    every,
    made,
    hub,
    land,
    load_sem,
    weight_sem,
    x_send,
    x_recv,
    straight_send,
    straight_recv,
    direct_send,
    direct_recv,
    relay_send,
    relay_recv,
    sum_send,
    sum_recv,
    pair_send,
    pair_recv,
    trade_send,
    trade_recv,
    early_send,
    early_recv,
    share_send,
    share_recv,
    dq_send,
    dq_recv,
    dq_direct_send,
    dq_direct_recv,
    dq_relay_send,
    dq_relay_recv,
    late_send,
    late_recv,
    core_send,
    core_recv,
    chip_send,
    chip_recv,
    last_send,
    last_recv,
    made_send,
    made_recv,
    land_send,
    land_recv,
):
    me = Place()
    chips, chip, core, seat, group = me.chips, me.chip, me.core, me.seat, me.group
    heads, depth, width = query_ref.shape
    tokens = input_ref.shape[0]
    window = tokens * me.ctx_count
    half = 2 * depth
    piece = half // group
    family = me.head // group
    acts, sources = (input_ref, cotan_ref), (query_ref, output_ref)
    rows = tokens // SUBS
    part_rows = tokens // 2

    mine = span(core * depth, depth)
    loads = []
    for a in range(2):
        loads.append(local(sources[a], mats.at[a, :, mine], load_sem.at[a]))
        loads.append(local(acts[a].at[:, span(chip * half, half)], own.at[a], load_sem.at[2 + a]))

    places = me.friends()
    if group == 4:
        places.append((me.ctx, flip(flip(me.head, 1), 2)))
    homes = [lax.rem(family + i, chips) for i in range(1, chips)]
    places += [(me.ctx, home * group + seat) for home in homes]
    greet(places)

    order = [(a, hop, s) for a in range(2) for hop in range(1, chips) for s in range(SUBS)]

    def located(n, at):
        a, hop, s = order[n]
        return far.at[hop - 1, a, at, pl.ds(s * rows, rows)]

    crossing = []
    for n, (a, hop, s) in enumerate(order):
        begin = pl.multiple_of(me.other(hop) * half + seat * piece, piece)
        copy = remote(
            acts[a].at[pl.ds(s * rows, rows), pl.ds(begin, piece)],
            located(n, seat),
            x_send.at[n],
            x_recv.at[n],
            me.across(hop),
        )
        copy.start()
        crossing.append(copy)
    straight = {}
    for n, (a, hop, s) in enumerate(order):
        if group == 4 and a == 1 and s >= SUBS - STRAIGHT:
            at = flip(flip(seat, 1), 2)
            begin = pl.multiple_of(me.other(hop) * half + at * piece, piece)
            copy = remote(
                acts[a].at[pl.ds(s * rows, rows), pl.ds(begin, piece)],
                located(n, at),
                straight_send.at[len(straight)],
                straight_recv.at[len(straight)],
                me.across(hop),
            )
            copy.start()
            straight[n] = copy
    for copy in loads:
        copy.start()
    swaps = []
    for a in range(2):
        copy = remote(
            sources[a], mats.at[a, :, mine], weight_sem.at[a], weight_sem.at[2 + a], me.sibling
        )
        copy.start()
        swaps.append(copy)

    row = me.head % 2

    def key_block(which, at):
        return keys.at[which, span(at * tokens, tokens)]

    pair_copies = []
    for hop in range(1, chips):
        copy = remote(
            pair_ref.at[0],
            key_block(row, me.ctx),
            pair_send.at[hop],
            pair_recv.at[hop],
            me.across(hop),
        )
        copy.start()
        pair_copies.append(copy)
    keep = local(pair_ref.at[0], key_block(row, me.ctx), load_sem.at[4])
    keep.start()

    early = 2 if group == 4 else 0
    holder = core == seat // 2

    def ahead(bit):
        to = flip(seat, bit)
        begin = pl.multiple_of(to * piece - core * depth, piece)
        return remote(
            query_ref.at[pl.ds(0, early), pl.ds(begin, piece)],
            group_mats.at[seat, pl.ds(0, early)],
            early_send.at[bit],
            early_recv.at[bit],
            me.beside(bit),
        )

    def came_ahead(bit):
        return remote(
            group_mats.at[seat, pl.ds(0, early)],
            group_mats.at[flip(seat, bit), pl.ds(0, early)],
            early_send.at[bit],
            early_recv.at[bit],
            me.beside(bit),
        )

    def share_ahead(bit):
        block = group_mats.at[flip(seat, bit), pl.ds(0, early)]
        return remote(
            block, block, early_send.at[2 + bit], early_recv.at[2 + bit], me.sibling
        )

    def when_ahead(action):
        if early:
            pl.when(holder)(lambda: action(1))
            pl.when(jnp.logical_not(holder))(lambda: action(2))

    when_ahead(lambda bit: ahead(bit).start())

    spread = Spread(
        me, located, (direct_send, direct_recv, relay_send, relay_recv), straight.items()
    )

    def own_slice(a, i):
        part = pl.ds(i * piece, piece)
        contract(own.at[a, :, part], mats.at[a, :, part], own_sum.at[a], i == 0)

    seats = [seat] + [flip(seat, 1)] * (group > 1)
    if group == 4:
        seats += [flip(seat, 2), flip(flip(seat, 1), 2)]
    sums = {}

    def far_part(a, hop, p):
        block = pl.ds(p * part_rows, part_rows)
        for n, (b, by, s) in enumerate(order):
            if (b, by) == (a, hop) and s // (SUBS // 2) == p:
                spread.arrive(n)
        for i, at in enumerate(seats):
            part = span(at * piece, piece)
            contract(
                far.at[hop - 1, a, at, block],
                mats.at[a, :, part],
                far_sum.at[hop - 1, a, block],
                i == 0,
            )
        if a == 0:
            source, target = far_sum.at[hop - 1, 0, block], q_got.at[hop - 1, block]
        else:
            da_low[hop - 1, block] = far_sum[hop - 1, 1, block].astype(BF16)
            source, target = da_low.at[hop - 1, block], da_got.at[hop - 1, block]
        copy = remote(
            source,
            target,
            sum_send.at[a, hop - 1, p],
            sum_recv.at[a, hop - 1, p],
            (me.source(hop) * 2 + core, me.head),
        )
        copy.start()
        sums[a, hop, p] = copy

    own_work = [(a, i) for a in range(2) for i in range(group)]
    count = len(order)
    for n in range(count):
        crossing[n].wait_recv()
        spread.start(n)
        if n >= 1:
            spread.pass_on(n - 1)
        if n == 1:
            for copy in loads:
                copy.wait()
            for copy in swaps:
                copy.wait_recv()
        if n >= 2 and own_work:
            own_slice(*own_work.pop(0))
        if chips == 2 and n == count - 3:
            far_part(0, 1, 0)
        if chips == 2 and n == count - 1:
            far_part(0, 1, 1)
    spread.pass_on(count - 1)

    keep.wait()
    for copy in pair_copies:
        copy.wait_recv()
    pair_next = []
    for hop in range(chips):
        block = key_block(row, me.source(hop) * 2 + core)
        copy = remote(
            block, block, pair_send.at[chips + hop], pair_recv.at[chips + hop], me.beside(1)
        )
        copy.start()
        pair_next.append(copy)

    part_columns = piece // 2
    ours = span(core * part_columns, part_columns)
    trades = []

    def seat_of(j):
        at = seat + 0
        for bit in (1, 2):
            if j & bit:
                at = flip(at, bit)
        return at

    held_back = late_heads(heads, group)

    def trade(j, later, k):
        to = seat_of(j)
        copy = remote(
            mats.at[0, later, span(to * piece + core * part_columns, part_columns)],
            group_mats.at[seat, later, ours],
            trade_send.at[k],
            trade_recv.at[k],
            (me.ctx, me.head - seat + to),
        )
        copy.start()
        trades.append((j, later, copy))

    for j in range(1, group):
        skip = early if j < 3 else 0
        trade(j, pl.ds(skip, heads - skip - (held_back if j == 3 else 0)), j)

    def trade_rest():
        if held_back:
            trade(3, pl.ds(heads - held_back, held_back), 0)

    store = local(mats.at[0, :, span(seat * piece, piece)], group_mats.at[seat], load_sem.at[5])
    store.start()

    for work in own_work:
        own_slice(*work)
    for a in range(2):
        for p in range(2):
            for hop in range(1, chips):
                if (a, hop, p) not in sums:
                    far_part(a, hop, p)

    for copy in pair_next:
        copy.wait_recv()
    pair_last = []
    for hop in range(chips):
        for which in range(2):
            block = key_block(which, me.source(hop) * 2 + core)
            k = 2 * chips + 2 * hop + which
            copy = remote(block, block, pair_send.at[k], pair_recv.at[k], me.sibling)
            copy.start()
            pair_last.append(copy)

    lanes = []
    for j in range(heads - 1):
        named = route_ref[...] == me.head * (heads - 1) + j
        lanes.append(jnp.sum(jnp.where(named, gate_ref[...], 0.0), axis=0, keepdims=True))
    lanes.append(jnp.ones_like(lanes[0]))
    lanes += [jnp.zeros_like(lanes[0])] * (-heads % 8)
    token_gate = jnp.transpose(jnp.concatenate(lanes, axis=0))

    for hop in range(1, chips):
        for p in range(2):
            sums[0, hop, p].wait_recv()
    for j in range(heads):
        columns = pl.ds(j * width, width)
        value = own_sum[0, :, columns]
        for hop in range(1, chips):
            value = value + q_got[hop - 1, :, columns]
        queries[j] = value.astype(BF16)
    for copy in pair_last:
        copy.wait_recv()
    for which in range(2):
        for at in range(me.ctx_count):
            block = pl.ds(at * tokens, tokens)
            turned[which, :, block] = jnp.transpose(keys[which, block])
    for hop in range(1, chips):
        for p in range(2):
            sums[1, hop, p].wait_recv()
    for j in range(heads):
        columns = pl.ds(j * width, width)
        value = own_sum[1, :, columns]
        for hop in range(1, chips):
            value = value + da_got[hop - 1, :, columns].astype(F32)
        if j < heads - 1:
            value = value * token_gate[:, j : j + 1]
        cotans[j] = value.astype(BF16)

    late = late_heads(heads, group)
    soon = heads - late
    parts = part_count(chips)
    lines = tokens // parts
    units, late_units, soon_units, far_units = [], [], [], []
    for t in range(parts):
        late_units.append(range(len(units), len(units) + (late > 0)))
        units += [(t, 0, pl.ds(soon, late))] * (late > 0)
        soon_units.append(range(len(units), len(units) + 1))
        units.append((t, 0, pl.ds(0, soon)))
        far_units.append(range(len(units), len(units) + chips - 1))
        units += [(t, hop, pl.ds(0, soon)) for hop in range(1, chips)]

    def unit(n, at):
        t, hop, which = units[n]
        return every.at[me.source(hop), at, which, pl.ds(t * lines, lines)]

    def dq_onward(n):
        return 1 + n % 2 if units[n][0] < 2 else 1

    dq_spread = Spread(
        me, unit, (dq_direct_send, dq_direct_recv, dq_relay_send, dq_relay_recv), onward=dq_onward
    )
    block_rows = min(part_rows, max(16, 256 * 1024 // window))
    scale = width ** (-0.5)
    turned_grads[...] = jnp.zeros(turned_grads.shape, F32)

    def attend(t, j):
        def body(i, carry):
            i = t * (part_rows // block_rows) + i
            block = span(i * block_rows, block_rows)
            query, cotan = queries[j, block], cotans[j, block]
            scores = jnp.dot(query, turned[0], preferred_element_type=F32) * scale
            first = me.ctx * tokens + i * block_rows
            place = first + lax.broadcasted_iota(jnp.int32, scores.shape, 0)
            scores = jnp.where(
                lax.broadcasted_iota(jnp.int32, scores.shape, 1) <= place, scores, -1e30
            )
            raised = jnp.exp(scores - jnp.max(scores, axis=1, keepdims=True))
            shares = raised / jnp.sum(raised, axis=1, keepdims=True)
            low = shares.astype(BF16)
            outputs = jnp.dot(low, keys[1], preferred_element_type=F32)
            share_grad = jnp.dot(cotan, turned[1], preferred_element_type=F32)
            delta = jnp.sum(cotan.astype(F32) * outputs, axis=1, keepdims=True)
            score_grad = (shares * (share_grad - delta) * scale).astype(BF16)
            every[chip, seat, j, block] = jnp.dot(
                score_grad, keys[0], preferred_element_type=F32
            ).astype(BF16)
            turned_grads[0] += jnp.dot(
                jnp.transpose(query), score_grad, preferred_element_type=F32
            )
            turned_grads[1] += jnp.dot(jnp.transpose(cotan), low, preferred_element_type=F32)
            return carry

        lax.fori_loop(0, part_rows // block_rows, body, 0)

    dq_copies, late_copies = {}, []

    def late_send_on(n, k):
        for hop in range(1, chips):
            block = unit(n, seats[k])
            m = len(late_copies)
            copy = remote(block, block, late_send.at[m], late_recv.at[m], me.across(hop))
            copy.start()
            late_copies.append((units[n][0], copy))

    def start_rest(t):
        for n in soon_units[t]:
            dq_spread.start(n)
        for n in far_units[t]:
            dq_copies[n].wait_recv()
            dq_spread.start(n)

    def start_late(t):
        if t < parts:
            for n in late_units[t]:
                dq_spread.start(n)

    def pass_late(t):
        if t < parts:
            for n in late_units[t]:
                dq_spread.pass_on(n)

    for p in range(2):
        these = range(p * parts // 2, (p + 1) * parts // 2)
        for j in range(soon, heads):
            attend(p, j)
        if p == 1:
            for n in far_units[0]:
                dq_copies[n].wait_recv()
                dq_spread.start(n)
            trade_rest()
        for t in these:
            for n in late_units[t]:
                late_send_on(n, 0)
        start_late(0) if p == 0 else pass_late(0)
        for j in range(soon):
            attend(p, j)
            if p == 1 and j == 0:
                start_late(1)
        for t in these:
            for n in soon_units[t]:
                for hop in range(1, chips):
                    m = far_units[t][hop - 1]
                    block = unit(n, seat)
                    k = t * (chips - 1) + hop - 1
                    copy = remote(block, block, dq_send.at[k], dq_recv.at[k], me.across(hop))
                    copy.start()
                    dq_copies[m] = copy
        if p == 0:
            for n in soon_units[0]:
                dq_spread.start(n)

    def column(at):
        return span(at * tokens, tokens)

    core_copies = []
    for hop in range(chips):
        spot = me.source(hop) * 2
        copy = remote(
            turned_grads.at[:, :, column(spot + 1 - core)],
            core_got.at[me.source(hop)],
            core_send.at[hop],
            core_recv.at[hop],
            me.sibling,
        )
        copy.start()
        core_copies.append(copy)
    kept_out[...] = jnp.zeros(kept_out.shape, F32)
    pair_low[...] = jnp.zeros(pair_low.shape, F32)
    for hop in range(chips):
        core_copies[hop].wait_recv()
        for which in range(2):
            both = (
                turned_grads[which, :, column(me.source(hop) * 2 + core)]
                + core_got[me.source(hop), which]
            )
            if hop:
                grads_low[hop - 1, which] = jnp.transpose(both).astype(BF16)
            else:
                kept_out[0] = jnp.where(row == which, jnp.transpose(both), kept_out[0])
                pair_low[...] = jnp.where(row == which, pair_low[...], jnp.transpose(both))
    chip_copies = []
    for hop in range(1, chips):
        copy = remote(
            grads_low.at[hop - 1],
            chip_got.at[hop - 1],
            chip_send.at[hop - 1],
            chip_recv.at[hop - 1],
            (me.source(hop) * 2 + core, me.head),
        )
        copy.start()
        chip_copies.append(copy)

    shares = []

    def share_trades(some):
        for j, later, copy in some:
            copy.wait_recv()
            block = group_mats.at[seat_of(j), later, ours]
            k = len(shares)
            share = remote(block, block, share_send.at[k], share_recv.at[k], me.sibling)
            share.start()
            shares.append(share)

    share_trades(trades[: group - 1])
    if early:

        @pl.when(holder)
        def _():
            for bit in (1, 2):
                came_ahead(bit).wait_recv()
                share_ahead(bit).start()

    def hand_round(t):
        if t + 1 < parts:
            start_rest(t + 1)
        for n in list(soon_units[t]) + list(far_units[t]):
            dq_spread.pass_on(n)
        start_late(t + 2)
        pass_late(t + 1)
        if t == 0:
            share_trades(trades[group - 1 :])
        for n in late_units[t]:
            dq_spread.arrive(n)
            for k in range(1, group):
                late_send_on(n, k)

    hand_round(0)

    step = min(512, piece) if chips <= 2 else min(256, piece)
    flat = [(m, j) for m in range(group) for j in range(heads)]

    def made_copy(hop, i):
        return remote(
            made.at[hop - 1, i],
            hub.at[chips - hop, i],
            made_send.at[hop - 1, i],
            made_recv.at[chips - hop - 1, i],
            (me.source(hop) * 2 + core, me.head),
        )

    def land_copy(hop, i):
        return remote(
            hub.at[hop, i],
            land.at[family, i],
            land_send.at[hop, i],
            land_recv.at[family, i],
            (me.ctx, me.source(hop) * group + seat),
        )

    def moves(hop):
        return me.source(hop) != family

    def multiply(t):
        block = pl.ds(t * lines, lines)

        def body(i, carry):
            part = span(i * step, step)
            total = jnp.zeros((chips * lines, step), F32)
            for k in range(0, len(flat), 2):
                both = flat[k : k + 2]
                left = jnp.concatenate(
                    [
                        jnp.concatenate([every[me.source(hop), m, j, block] for m, j in both], axis=1)
                        for hop in range(chips)
                    ],
                    axis=0,
                )
                right = jnp.concatenate([group_mats[m, j, part] for m, j in both], axis=1)
                total += lax.dot_general(
                    left, right, (((1,), (1,)), ((), ())), preferred_element_type=F32
                )
            for hop in range(chips):
                result = made.at[hop - 1] if hop else hub.at[0]
                result[t, :, part] = total[hop * lines : (hop + 1) * lines].astype(BF16)
            return carry

        lax.fori_loop(0, piece // step, body, 0)
        pl.when(moves(0))(land_copy(0, t).start)
        for hop in range(1, chips):
            made_copy(hop, t).start()

    def pass_made(t):
        for hop in range(1, chips):
            made_copy(chips - hop, t).wait_recv()
            pl.when(moves(hop))(land_copy(hop, t).start)

    def finish_part(t):
        for n in list(soon_units[t]) + list(far_units[t]):
            dq_spread.arrive(n)
        for when, copy in late_copies:
            if when == t:
                copy.wait_recv()
        multiply(t)

    hand_round(1)
    store.wait()
    for copy in shares:
        copy.wait_recv()
    if early:

        @pl.when(jnp.logical_not(holder))
        def _():
            for bit in (1, 2):
                share_ahead(bit).wait_recv()
    finish_part(0)
    for hop in range(1, chips):
        chip_copies[hop - 1].wait_recv()
        for which in range(2):
            value = chip_got[hop - 1, which].astype(F32)
            kept_out[0] += jnp.where(row == which, value, 0.0)
            pair_low[...] += jnp.where(row == which, 0.0, value)
    last_low = grads_low.at[chips - 1, 0]
    last_low[...] = pair_low[...].astype(BF16)
    last = remote(last_low, pair_got, last_send.at[0], last_recv.at[0], me.beside(1))

    last.start()
    for t in range(2, parts):
        hand_round(t)
        pass_made(t - 2)
        finish_part(t - 1)
    finish_part(parts - 1)
    pass_made(parts - 2)
    pass_made(parts - 1)

    last.wait()
    other_out[...] = pair_got[...]

    stay = lax.rem(chip - family + chips, chips)
    for t in range(parts):
        total = hub[stay, t].astype(F32)
        for home in homes:
            arrival = remote(
                hub.at[0, t], land.at[home, t], land_send.at[0, t], land_recv.at[home, t], me.sibling
            )
            arrival.wait_recv()
            total = total + land[home, t].astype(F32)
        input_grad_out[pl.ds(t * lines, lines)] = total.astype(BF16)

    for hop in range(chips):
        for i in range(parts):
            if hop:
                made_copy(hop, i).wait_send()
            pl.when(moves(hop))(land_copy(hop, i).wait_send)
    for copy in crossing + swaps + pair_copies + pair_next + pair_last + shares:
        copy.wait_send()
    for copy in core_copies + chip_copies + list(straight.values()):
        copy.wait_send()
    for copy in list(sums.values()) + list(dq_copies.values()):
        copy.wait_send()
    for _, copy in late_copies:
        copy.wait_send()
    for _, _, copy in trades:
        copy.wait_send()
    when_ahead(lambda bit: ahead(bit).wait_send())
    if early:

        @pl.when(holder)
        def _():
            for bit in (1, 2):
                share_ahead(bit).wait_send()

    spread.finish()
    dq_spread.finish()


def settle_kernel(grad_ref, kept_ref, rest_ref, grad_out, kept_out):
    grad_out[...] = grad_ref[...]
    kept_out[0] = kept_ref[0] + rest_ref[...].astype(F32)


def per_device(
    layer_input, output_grad, routes, route_gates, query_weight, output_weight, key_values
):
    ctx_count, head_count = lax.axis_size("ctx"), lax.axis_size("head")
    chips = ctx_count // 2
    group, hops = head_count // chips, chips - 1
    heads, depth, width = query_weight.shape
    tokens = layer_input.shape[0]
    half = 2 * depth
    piece = half // group
    window = tokens * ctx_count
    count = 2 * hops * SUBS
    parts = part_count(chips)
    late = late_heads(heads, group)
    units, lines = parts * (chips + (late > 0)), tokens // parts
    grad, kept, rest = pl.pallas_call(
        layer_kernel,
        out_shape=(
            jax.ShapeDtypeStruct((tokens, piece), BF16),
            jax.ShapeDtypeStruct((1, tokens, width), F32),
            jax.ShapeDtypeStruct((tokens, width), BF16),
        ),
        in_specs=[ANY, ANY, VMEM, VMEM, ANY, ANY, VMEM],
        out_specs=(VMEM, VMEM, VMEM),
        scratch_shapes=[
            pltpu.VMEM((2, heads, half, width), BF16),
            pltpu.VMEM((2, tokens, half), BF16),
            pltpu.VMEM((hops, 2, group, tokens, piece), BF16),
            pltpu.VMEM((2, tokens, heads * width), F32),
            pltpu.VMEM((hops, 2, tokens, heads * width), F32),
            pltpu.VMEM((hops, tokens, heads * width), F32),
            pltpu.VMEM((hops, tokens, heads * width), BF16),
            pltpu.VMEM((hops, tokens, heads * width), BF16),
            pltpu.VMEM((heads, tokens, width), BF16),
            pltpu.VMEM((heads, tokens, width), BF16),
            pltpu.VMEM((group, heads, piece, width), BF16),
            pltpu.VMEM((2, window, width), BF16),
            pltpu.VMEM((2, width, window), BF16),
            pltpu.VMEM((2, width, window), F32),
            pltpu.VMEM((chips, 2, width, tokens), F32),
            pltpu.VMEM((chips, 2, tokens, width), BF16),
            pltpu.VMEM((hops, 2, tokens, width), BF16),
            pltpu.VMEM((tokens, width), F32),
            pltpu.VMEM((tokens, width), BF16),
            pltpu.VMEM((chips, group, heads, tokens, width), BF16),
            pltpu.VMEM((hops, parts, lines, piece), BF16),
            pltpu.VMEM((chips, parts, lines, piece), BF16),
            pltpu.VMEM((chips, parts, lines, piece), BF16),
            DMA((6,)),
            DMA((4,)),
        ]
        + [DMA((count,))] * 2
        + [DMA((hops * STRAIGHT,))] * 2
        + Spread.sems(count)
        + [DMA((2, hops, 2))] * 2
        + [DMA((4 * chips,))] * 2
        + [DMA((group,))] * 2
        + [DMA((5,))] * 2
        + [DMA((group,))] * 2
        + [DMA((parts * hops,))] * 2
        + Spread.sems(units)
        + [DMA((max(1, hops * parts * group * (late > 0)),))] * 2
        + [DMA((chips,))] * 2
        + [DMA((hops,))] * 2
        + [DMA((1,))] * 2
        + [DMA((hops, parts))] * 2
        + [DMA((chips, parts))] * 2,
        compiler_params=pltpu.CompilerParams(
            collective_id=0, has_side_effects=True, vmem_limit_bytes=VMEM_BYTES
        ),
    )(
        layer_input,
        output_grad,
        routes.T,
        route_gates.T,
        query_weight,
        output_weight,
        key_values,
    )
    return pl.pallas_call(
        settle_kernel,
        out_shape=(
            jax.ShapeDtypeStruct(grad.shape, grad.dtype),
            jax.ShapeDtypeStruct(kept.shape, kept.dtype),
        ),
        in_specs=[VMEM] * 3,
        out_specs=(VMEM, VMEM),
    )(grad, kept, rest)


def solution(mesh):
    in_specs = (
        P("ctx", None),
        P("ctx", None),
        P("ctx", None),
        P("ctx", None),
        P("head", "ctx", None),
        P("head", "ctx", None),
        P("head", "ctx", None),
    )
    out_specs = (P("ctx", "head"), P("head", "ctx", None))
    return jax.shard_map(
        per_device, mesh=mesh, in_specs=in_specs, out_specs=out_specs, check_vma=False
    )
```
